32 devices in a mesh: pipe: 4 (over z), dp: 4 (over y, x), tensor: 2 (over core).
Axes of the slice: x: 2, y: 2, z: 4, core: 2. Of those that a mesh axis runs over, the one named last changes fastest.
Arguments:
- saved_inputs: bfloat16 [3, 2, 4, 512, 4096], P(None, None, 'pipe', 'dp', 'tensor'), may hold values from -6 to 6
- proj_in: bfloat16 [2, 4, 512, 4096], P(None, 'pipe', None, 'tensor'), may hold values from -0.09375 to 0.09375
- proj_out: bfloat16 [2, 4, 512, 4096], P(None, 'pipe', None, 'tensor'), may hold values from -0.25 to 0.25
- norm_gain: float32 [2, 4, 4096], P(None, 'pipe', 'tensor'), may hold values from 0.1 to 1.9
- arriving: bfloat16 [2, 4, 512, 4096], P(None, 'pipe', 'dp', 'tensor'), may hold values from -6 to 6
- logp_grad: bfloat16 [2, 512, 4096], P(None, 'dp', 'tensor'), may hold values from -6 to 6
- rewards: float32 [2, 4, 4], P(None, 'dp'), may hold values from -4 to 4
- seq_lengths: int32 [2, 4, 4], P(None, 'dp'), may hold values from 1 to 64, 128 in all within a row
- group_ids: int32 [2, 4, 4], P(None, 'dp'), may hold values from 0 to 3
Outputs:
- grad_in: float32 [2, 4, 512, 4096], P(None, 'pipe', 'dp', 'tensor')
- grad_out: float32 [2, 4, 512, 4096], P(None, 'pipe', 'dp', 'tensor')
- leaving: bfloat16 [2, 4, 512, 4096], P(None, 'pipe', 'dp', 'tensor')
The draws below stay inside these ranges and needn't reach their ends.
Inputs may be any that keep to these rules, and one draw needn't show every extreme that they name: `seq_lengths`: the 4 lengths of one microbatch on one replica sum to 128. `group_ids`: groups take sequences from several replicas and microbatches.
All inputs are finite; a program needn't handle non-finite values.
Results may differ from the reference program's by a relative error of at most 0.023.
Values may be sent and summed in bfloat16 or wider, within the bound.
A program may use at most 128 MiB of HBM per device.

```python
import math
import jax
import jax.numpy as jnp
import numpy as np
from jax import lax

D = 4096
R = 512
ROWS = 128
SEQS = 4
STEPS = 3
NEW = 2
GROUPS = 4
MOST = 64
N_PIPE = 4
N_DP = 4
N_TENSOR = 2


def set_ends(values, stream_key, smallest, top_value):
    place = [jax.random.randint(jax.random.fold_in(stream_key, axis), (), 0, length) for axis, length in enumerate(values.shape)]
    main_axis = values.shape.index(max(values.shape))
    next_to = place[:main_axis] + [(place[main_axis] + 1) % values.shape[main_axis]] + place[main_axis + 1:]
    return values.at[tuple(place)].set(smallest).at[tuple(next_to)].set(top_value)


def block_levels(own_key, shape, split, least, largest):
    gain = 1.0
    for axis_at, blocks in split:
        heights = jax.random.uniform(jax.random.fold_in(jax.random.fold_in(own_key, 6), axis_at), (blocks,), jnp.float32, least / len(split), largest / len(split))
        gain = gain * jnp.repeat(jnp.exp(heights), shape[axis_at] // blocks).reshape((-1,) + (1,) * (len(shape) - 1 - axis_at))
    return gain


def profile(number_of, total, bound, lean):
    loads = [(1 << 20) // math.isqrt(grade ** lean) + 1 for grade in range(2, number_of + 1)]
    spare, given = total - bound - (number_of - 1), [1] * (number_of - 1)
    while spare > 0:
        movable = [i for i in range(number_of - 1) if given[i] < bound]
        pool, budget = sum([loads[i] for i in movable]), spare
        for i in movable:
            extra = min(bound - given[i], max(1, budget * loads[i] // pool), spare)
            given[i] = given[i] + extra
            spare = spare - extra
    return np.array([bound] + given)


def ragged(own_key, count, total, reach, lean):
    if count == 2:
        one = jax.random.randint(own_key, (), max(1, total - reach), min(reach, total - 1) + 1)
        return jnp.stack([one, total - one])
    lengths = jnp.asarray(profile(count, total, reach, lean), jnp.int32)
    pairs = (count - 1) // 2
    source_of, sink = lengths[1:1 + 2 * pairs:2], lengths[2:2 + 2 * pairs:2]
    slack = jnp.minimum(source_of - 1, reach - sink)
    passed = jax.random.randint(jax.random.fold_in(own_key, 1), (pairs,), 0, 1 << 20) % (slack + 1)
    lengths = lengths.at[1:1 + 2 * pairs:2].set(source_of - passed).at[2:2 + 2 * pairs:2].set(sink + passed)
    return lengths[jax.random.permutation(jax.random.fold_in(own_key, 2), count)]


def normal_values(own_key, extent, spread, reach, shards=(), kind=jnp.bfloat16):
    gain = block_levels(own_key, extent, shards, -0.22, 0.18) if shards else 1.0
    entries = jax.random.normal(own_key, extent, jnp.float32) * spread * gain
    return jnp.minimum(jnp.maximum(entries, -reach), reach).astype(kind)


def setup_inputs(seed: int = 0) -> dict:
    streams_of = jax.random.split(jax.random.key(seed), 10)
    return {
        "saved_inputs": normal_values(streams_of[0], (STEPS, 2, N_PIPE, N_DP * ROWS, D), 1.0, 6.0, ((2, 4), (3, 4), (4, 2))),
        "proj_in": normal_values(streams_of[1], (2, N_PIPE, R, D), D ** -0.5, 0.09375, ((1, 4), (3, 2))),
        "proj_out": normal_values(streams_of[2], (2, N_PIPE, R, D), R ** -0.5, 0.25, ((1, 4), (3, 2))),
        "norm_gain": jnp.clip(1.0 + 0.18 * jax.random.normal(streams_of[3], (2, N_PIPE, D), jnp.float32), 0.1, 1.9),
        "arriving": normal_values(streams_of[4], (2, N_PIPE, N_DP * ROWS, D), 1.0, 6.0, ((1, 4), (2, 4), (3, 2))),
        "logp_grad": normal_values(streams_of[5], (NEW, N_DP * ROWS, D), 1.0, 6.0, ((1, 4), (2, 2))),
        "rewards": normal_values(streams_of[6], (NEW, N_DP, SEQS), 1.0, 4.0, ((1, 4),), jnp.float32),
        "seq_lengths": jax.vmap(lambda own: ragged(own, SEQS, ROWS, MOST, 2))(jax.random.split(streams_of[7], NEW * N_DP)).reshape((NEW, N_DP, SEQS)).astype(jnp.int32),
        "group_ids": set_ends(jax.random.randint(streams_of[8], (NEW, N_DP, SEQS), 0, GROUPS), jax.random.fold_in(streams_of[8], 1), 0, GROUPS - 1).astype(jnp.int32),
    }


EPS = 1e-05

def silu_slope(values):
    sigma = jax.nn.sigmoid(values)
    return sigma * (1.0 + values * (1.0 - sigma))

def round_trip(values):
    return lax.optimization_barrier(values.astype(jnp.bfloat16)).astype(jnp.float32)

def block_product(left, right):
    count = left.shape[0]
    width = right.shape[0]
    left_blocks = left.astype(jnp.float32).reshape(count, N_TENSOR, D // N_TENSOR)
    right_blocks = right.astype(jnp.float32).reshape(width, N_TENSOR, D // N_TENSOR)
    pieces = jnp.einsum('rtd,ktd->trk', left_blocks, right_blocks)
    return lax.optimization_barrier(jnp.sum(round_trip(pieces), axis=0))

def block_back(operands):
    inputs, arrive, weight_in, weight_out, gain_row = operands
    inputs_f = inputs.astype(jnp.float32)
    squares = lax.optimization_barrier(jnp.sum(inputs_f * inputs_f, axis=-1))
    inv_rms = 1.0 / jnp.sqrt(squares / D + EPS)
    gained = (inputs_f * gain_row).astype(jnp.bfloat16)
    pre_sum = block_product(gained, weight_in)
    back_sum = block_product(arrive, weight_out)
    pre_act = inv_rms[:, None] * pre_sum
    hidden = jax.nn.silu(pre_act).astype(jnp.bfloat16)
    grad_pre = back_sum * silu_slope(pre_act)
    grad_scaled = (inv_rms[:, None] * grad_pre).astype(jnp.bfloat16)
    grad_gained = jnp.dot(grad_scaled, weight_in, preferred_element_type=jnp.float32)
    radial_sum = lax.optimization_barrier(jnp.sum(grad_pre * pre_sum, axis=-1))
    out_cot = arrive.astype(jnp.float32) + gain_row * grad_gained - inputs_f * (inv_rms ** 3 * radial_sum / D)[:, None]
    return (out_cot.astype(jnp.bfloat16), grad_scaled, hidden)

def top_cotangent(logp_grad, rewards, seq_lengths, group_ids):
    groups = jnp.arange(GROUPS, dtype=jnp.int32)
    member = (group_ids[..., None] == groups).astype(jnp.float32)
    sums = lax.optimization_barrier(jnp.sum(member * rewards[..., None], axis=(0, 1, 2)))
    counts = lax.optimization_barrier(jnp.sum(member, axis=(0, 1, 2)))
    means = sums / jnp.maximum(counts, 1.0)
    advantage = rewards - lax.optimization_barrier(jnp.sum(member * means, axis=-1))
    ends = jnp.cumsum(seq_lengths, axis=-1).astype(jnp.int32)
    position = jnp.arange(ROWS, dtype=jnp.int32)
    segment = lax.optimization_barrier(jnp.sum((position[:, None] >= ends[..., None, :]).astype(jnp.int32), axis=-1))
    pick = (segment[..., None] == jnp.arange(SEQS, dtype=jnp.int32)).astype(jnp.float32)
    weights = lax.optimization_barrier(jnp.sum(pick * advantage[..., None, :], axis=-1)).reshape(NEW, N_DP * ROWS)
    return (-weights[..., None] * logp_grad.astype(jnp.float32)).astype(jnp.bfloat16)

def reference(saved_inputs, proj_in, proj_out, norm_gain, arriving, logp_grad, rewards, seq_lengths, group_ids):
    entering = top_cotangent(logp_grad, rewards, seq_lengths, group_ids)
    slots = 2 * N_PIPE
    tokens = N_DP * ROWS
    weights_in = proj_in.reshape(slots, R, D)
    weights_out = proj_out.reshape(slots, R, D)
    gains = norm_gain.reshape(slots, D)
    current = arriving
    cot_list = []
    scaled_list = []
    hidden_list = []
    out_cot = arriving
    for step_index in range(STEPS):
        inputs = saved_inputs[step_index].reshape(slots, tokens, D)
        flat_cot = current.reshape(slots, tokens, D)
        out_flat, grad_scaled, hidden = lax.map(block_back, (inputs, flat_cot, weights_in, weights_out, gains))
        cot_list.append(flat_cot)
        scaled_list.append(grad_scaled)
        hidden_list.append(hidden)
        out_cot = out_flat.reshape(2, N_PIPE, tokens, D)
        if step_index + 1 < STEPS:
            lower = jnp.concatenate([out_cot[0, 1:], out_cot[1, :1]], axis=0)
            upper = jnp.concatenate([out_cot[1, 1:], entering[step_index][None]], axis=0)
            current = jnp.stack([lower, upper])
    cot_all = jnp.stack(cot_list)
    scaled_all = jnp.stack(scaled_list)
    hidden_all = jnp.stack(hidden_list)
    saved_all = saved_inputs.reshape(STEPS, slots, tokens, D)
    scale = 1.0 / (N_DP * ROWS)

    def slot_grads(slot):
        slot = slot.astype(jnp.int32)
        inputs = lax.dynamic_index_in_dim(saved_all, slot, 1, keepdims=False)
        arrive = lax.dynamic_index_in_dim(cot_all, slot, 1, keepdims=False)
        grad_scaled = lax.dynamic_index_in_dim(scaled_all, slot, 1, keepdims=False)
        hidden = lax.dynamic_index_in_dim(hidden_all, slot, 1, keepdims=False)
        gain_row = lax.dynamic_index_in_dim(gains, slot, 0, keepdims=False)
        gained = (inputs.astype(jnp.float32) * gain_row).astype(jnp.bfloat16)
        left_in = grad_scaled.astype(jnp.float32).reshape(STEPS, N_DP, ROWS, R)
        right_in = gained.astype(jnp.float32).reshape(STEPS, N_DP, ROWS, D)
        per_in = jnp.einsum('snrk,snrd->nkd', left_in, right_in)
        left_out = hidden.astype(jnp.float32).reshape(STEPS, N_DP, ROWS, R)
        right_out = arrive.astype(jnp.float32).reshape(STEPS, N_DP, ROWS, D)
        per_out = jnp.einsum('snrk,snrd->nkd', left_out, right_out)
        total_in = lax.optimization_barrier(jnp.sum(round_trip(per_in), axis=0)) * scale
        total_out = lax.optimization_barrier(jnp.sum(round_trip(per_out), axis=0)) * scale
        return (total_in, total_out)
    grad_in, grad_out = lax.map(slot_grads, jnp.arange(slots, dtype=jnp.int32))
    return (grad_in.reshape(2, N_PIPE, R, D), grad_out.reshape(2, N_PIPE, R, D), out_cot)
```

```python
import functools

import jax
import jax.numpy as jnp
from jax import lax
from jax.experimental import pallas as pl
from jax.experimental.pallas import tpu as pltpu
from jax.sharding import PartitionSpec as P

EPS = 1e-05
MESH = pl.DeviceIdType.MESH
F32 = jnp.float32
BF16 = jnp.bfloat16


def dot_nt(a, b):
    return lax.dot_general(a, b, (((1,), (1,)), ((), ())), preferred_element_type=F32)


def factors(n):
    low = 1
    for k in range(1, n + 1):
        if n % k == 0 and k * k <= n:
            low = k
    return low, n // low


CHUNKS = 4
GATHERED = (4, 4)
PARTS = 2
scope = jax.named_scope


def reductions():
    jobs = [("out", v, j) for v in (1, 0) for j in range(CHUNKS)]
    jobs += [("in", v, j) for v in (1, 0) for j in range(GATHERED[v], CHUNKS)]
    return {job: e for e, job in enumerate(jobs)}


def kernel(
    dims,
    x_hbm, wi_hbm, wo_hbm, gn_hbm, ar_hbm, lp_hbm, rew_hbm, len_hbm, ids_hbm,
    fi, fo, lv,
    xs, gd, ca, wi, wo, lp, ps, pr, presum, slope, hid_t, gs, gs_t, gsr0, gsr1, xr0, xr1, bs, br, ob,
    sqs, sqr, inv_t, stl, str_, gb, r1, p2, r2, p2i, r2i,
    gn_ref, rew_ref, len_ref, ids_ref, str2,
    in_sem, sq_sem, st_sem, pre_sem, back_sem, pipe_s, pipe_r, xg_s, xg_r, gt_s, gt_r,
    r1_s, r1_r, r2_s, r2_r, ri_s, ri_r,
):
    steps, vs, tok, wid, rank, nt, npipe, ndp = dims
    na, nb = factors(ndp)
    rc = rank // ndp
    full = wid * nt
    tile = min(512, wid // 2)
    rtile = min(512, rank)
    cc = wid // CHUNKS
    part_tok = tok // PARTS
    lanes = stl.shape[2]
    new_count, _, seq_count = rew_ref.shape
    unit_lane = new_count * ndp * seq_count // 8
    me_t = lax.axis_index("tensor")
    me_p = lax.axis_index("pipe")
    me_d = lax.axis_index("dp")
    me_h = me_d // nb
    me_l = me_d % nb
    prev_p = lax.rem(me_p + npipe - 1, npipe)
    next_p = lax.rem(me_p + 1, npipe)

    def load(src, dst, k):
        return pltpu.make_async_copy(src, dst, in_sem.at[k])

    loads = [
        load(ar_hbm.at[1], ca.at[1, 0], 0),
        load(wo_hbm.at[1], wo.at[1], 1),
        load(x_hbm.at[:, 1], xs.at[:, 1], 2),
        load(wi_hbm.at[1], wi.at[1], 3),
        load(x_hbm.at[:, 0], xs.at[:, 0], 4),
        load(ar_hbm.at[0], ca.at[0, 0], 5),
        load(wo_hbm.at[0], wo.at[0], 6),
        load(wi_hbm.at[0], wi.at[0], 7),
        load(lp_hbm, lp, 8),
    ]
    small = [
        load(gn_hbm, gn_ref, 9),
        load(rew_hbm, rew_ref, 10),
        load(len_hbm, len_ref, 11),
        load(ids_hbm, ids_ref, 12),
    ]

    barrier = pltpu.get_barrier_semaphore()
    for k in range(1, nt):
        pl.semaphore_signal(barrier, inc=1, device_id={"tensor": lax.rem(me_t + k, nt)}, device_id_type=MESH)
    for k in range(1, na):
        peer = lax.rem(me_h + k, na) * nb + me_l
        pl.semaphore_signal(barrier, inc=1, device_id={"dp": peer}, device_id_type=MESH)
    for k in range(1, nb):
        peer = me_h * nb + lax.rem(me_l + k, nb)
        pl.semaphore_signal(barrier, inc=1, device_id={"dp": peer}, device_id_type=MESH)
    for other in (prev_p, next_p):
        pl.semaphore_signal(barrier, inc=1, device_id={"pipe": other}, device_id_type=MESH)

    for item in small + loads:
        item.start()

    with scope("barrier"):
        pl.semaphore_wait(barrier, nt - 1 + na - 1 + nb - 1 + 2)

    def to_tensor(src, dst_of, send_of, recv_of):
        return [
            pltpu.make_async_remote_copy(
                src_ref=src, dst_ref=dst_of(k - 1), send_sem=send_of(k - 1), recv_sem=recv_of(k - 1),
                device_id={"tensor": lax.rem(me_t + k, nt)}, device_id_type=MESH,
            )
            for k in range(1, nt)
        ]

    def to_dp(src_of, dst_of, send_of, recv_of, kind):
        out = []
        count = {"h": na, "l": nb}[kind]
        for k in range(1, count):
            if kind == "h":
                part = lax.rem(me_h + k, na)
                who = part * nb + me_l
            else:
                part = lax.rem(me_l + k, nb)
                who = me_h * nb + part
            out.append(
                pltpu.make_async_remote_copy(
                    src_ref=src_of(part), dst_ref=dst_of(k - 1), send_sem=send_of(k - 1), recv_sem=recv_of(k - 1),
                    device_id={"dp": who}, device_id_type=MESH,
                )
            )
        return out

    gather_kind = ("h", "l")
    split_kind = ("l", "h")
    count_of = {"h": na, "l": nb}
    xr = (xr0, xr1)
    gsr = (gsr0, gsr1)

    def x_copies(t, v):
        base = v * steps + t
        cols = pl.ds(0, GATHERED[v] * cc)
        return to_dp(
            lambda part: x_hbm.at[t, v, :, cols], lambda k: xr[v].at[k, t],
            lambda k: xg_s.at[base, k], lambda k: xg_r.at[base, k], gather_kind[v],
        )


    def stat_copies(kind):
        if kind == "l":
            return to_dp(lambda part: stl.at[0], lambda k: str_.at[k], lambda k: st_sem.at[0, k], lambda k: st_sem.at[1, k], kind)
        return to_dp(lambda part: stl.at[1], lambda k: str2.at[k], lambda k: st_sem.at[2, k], lambda k: st_sem.at[3, k], kind)

    def stats_first():
        lane8 = lax.broadcasted_iota(jnp.int32, (8, lanes), 1)
        row8 = lax.broadcasted_iota(jnp.int32, (8, lanes), 0)
        stats_own = jnp.where((row8 == 2) & (lane8 == unit_lane), 1.0, 0.0)
        for n in range(new_count):
            for k in range(seq_count):
                value = jnp.where(row8 == 0, rew_ref[n, 0, k], jnp.where(row8 == 1, 1.0, 0.0))
                stats_own = stats_own + jnp.where(lane8 == ids_ref[n, 0, k], value, 0.0)
        stl[0] = stats_own
        for item in stat_copies("l"):
            item.start()

    def stats_second():
        for item in stat_copies("l"):
            item.wait_recv()
        total = stl[0]
        for k in range(nb - 1):
            total = total + str_[k]
        stl[1] = total
        for item in stat_copies("h"):
            item.start()

    def start_gather(v, which):
        for t in which:
            for item in x_copies(t, v):
                item.start()

    lane = lax.broadcasted_iota(jnp.int32, (tok, 128), 1)

    def sq_copies(v):
        return to_tensor(
            sqs.at[v], lambda k: sqr.at[k, v], lambda k: sq_sem.at[0, v, k], lambda k: sq_sem.at[1, v, k]
        )

    def prep(v):
        def body(t, squares_all):
            row = xs[t, v].astype(F32)
            gd[v, pl.ds(pl.multiple_of(t * tok, tok), tok), :] = (row * gn_ref[v]).astype(BF16)
            squares = jnp.sum(row * row, axis=-1, keepdims=True)
            return jnp.where(lane == t, squares, squares_all)

        sqs[v] = lax.fori_loop(0, steps, body, jnp.zeros((tok, 128), F32))
        for item in sq_copies(v):
            item.start()

    def finish_sq(v):
        for item in sq_copies(v):
            item.wait_recv()
        total = sqs[v]
        for k in range(nt - 1):
            total = total + sqr[k, v]
        inv_t[v] = 1.0 / jnp.sqrt(total * (1.0 / full) + EPS)

    def gs_copies(t, v):
        cols = pl.ds(t * tok, tok)
        base = v * steps + t
        source = (lambda part: gs_t.at[v, part, :, :, cols]) if v == 0 else (lambda part: gs_t.at[v, :, part, :, cols])
        return to_dp(
            source, lambda k: gsr[v].at[k, :, :, cols],
            lambda k: gt_s.at[base, k], lambda k: gt_r.at[base, k], gather_kind[v],
        )

    pre_copies = {}
    back_copies = {}

    def pre_part(v):
        def body(j, carry):
            cols = pl.ds(pl.multiple_of(j * rtile, rtile), rtile)
            ps[v, :, cols] = dot_nt(gd[v], wi[v, cols, :]).astype(BF16)
            return carry

        lax.fori_loop(0, rank // rtile, body, 0)
        pre_copies[v] = to_tensor(
            ps.at[v], lambda k: pr.at[k, v], lambda k: pre_sem.at[0, v, k], lambda k: pre_sem.at[1, v, k]
        )
        for item in pre_copies[v]:
            item.start()

    def rows_of(h):
        return pl.ds(h * part_tok, part_tok)

    def back_part(t, v, h=None):
        rows = pl.ds(0, tok) if h is None else rows_of(h)

        def body(j, carry):
            cols = pl.ds(pl.multiple_of(j * rtile, rtile), rtile)
            bs[v, t, rows, cols] = dot_nt(ca[v, t, rows, :], wo[v, cols, :]).astype(BF16)
            return carry

        lax.fori_loop(0, rank // rtile, body, 0)
        base = (v * steps + t) * PARTS + (h or 0)
        back_copies[t, v, h] = to_tensor(
            bs.at[v, t, rows], lambda k: br.at[k, v, t, rows],
            lambda k: back_sem.at[0, base, k], lambda k: back_sem.at[1, base, k],
        )
        for item in back_copies[t, v, h]:
            item.start()

    def finish_pre(v, which_steps):
        for t in which_steps:
            rows = pl.ds(t * tok, tok)
            total = ps[v, rows, :].astype(F32)
            for k in range(nt - 1):
                total = total + pr[k, v, rows, :].astype(F32)
            pre = inv_t[v, :, t:t + 1] * total
            sigma = jax.nn.sigmoid(pre)
            presum[v, rows, :] = total
            hid_t[v, :, rows] = jnp.transpose(pre * sigma).astype(BF16)
            slope[v, rows, :] = sigma * (1.0 + pre * (1.0 - sigma))

    def wait_back(t, v, h=None):
        for item in back_copies[t, v, h]:
            item.wait_recv()

    def finish_back(t, v, h):
        own = rows_of(h)
        rows = pl.ds(t * tok + h * part_tok, part_tok)
        inv = inv_t[v, own, t:t + 1]
        total = bs[v, t, own, :].astype(F32)
        for k in range(nt - 1):
            total = total + br[k, v, t, own, :].astype(F32)
        grad_pre = total * slope[v, rows, :]
        gs[v, rows, :] = (inv * grad_pre).astype(BF16)
        radial = jnp.sum(grad_pre * presum[v, rows, :], axis=-1, keepdims=True)
        coef = inv * inv * inv * radial * (1.0 / full)

        def body(j, carry):
            cols = pl.ds(pl.multiple_of(j * tile, tile), tile)
            lifted = jnp.dot(gs[v, rows, :], wi[v, :, cols], preferred_element_type=F32)
            out = (
                ca[v, t, own, cols].astype(F32)
                + gn_ref[v, :, cols] * lifted
                - xs[t, v, own, cols].astype(F32) * coef
            ).astype(BF16)
            if t < steps - 1:
                ob[t, v, own, cols] = out
            else:
                lv[v, own, cols] = out
            return carry

        lax.fori_loop(0, wid // tile, body, 0)

    def finish_gs(t, v):
        rows = pl.ds(t * tok, tok)
        flipped = jnp.transpose(gs[v, rows, :].astype(F32)).astype(BF16)
        gs_t[v, :, :, :, rows] = flipped.reshape(na, nb, rc, tok)
        for item in gs_copies(t, v):
            item.start()

    def pipe_copy(t, v, slot, h):
        return pltpu.make_async_remote_copy(
            src_ref=ob.at[t, v, rows_of(h)], dst_ref=ca.at[slot, t + 1, rows_of(h)],
            send_sem=pipe_s.at[t, v, h], recv_sem=pipe_r.at[t, slot, h],
            device_id={"pipe": prev_p}, device_id_type=MESH,
        )

    def send_on(t, v, h):
        @pl.when(me_p > 0)
        def _():
            pipe_copy(t, v, v, h).start()

        if v == 1:
            @pl.when(me_p == 0)
            def _():
                pipe_copy(t, 1, 0, h).start()

    def sent_on(t, v, h):
        @pl.when(me_p > 0)
        def _():
            pipe_copy(t, v, v, h).wait_send()

        if v == 1:
            @pl.when(me_p == 0)
            def _():
                pipe_copy(t, 1, 0, h).wait_send()

    def take(t, v, h):
        if v == 0:
            pipe_copy(t - 1, v, v, h).wait_recv()
        else:
            @pl.when(me_p < npipe - 1)
            def _():
                pipe_copy(t - 1, v, v, h).wait_recv()

            @pl.when(me_p == npipe - 1)
            def _():
                stats = stl[1]
                for k in range(na - 1):
                    stats = stats + str2[k]
                means = stats[0:1] / jnp.maximum(stats[1:2], 1.0) + stats[2:3] * (1.0 / ndp)
                tok_row = lax.broadcasted_iota(jnp.int32, (part_tok, lanes), 0) + h * part_tok
                tok_lane = lax.broadcasted_iota(jnp.int32, (part_tok, lanes), 1)
                hot = jnp.zeros((part_tok, lanes), F32)
                begin = 0
                for k in range(seq_count):
                    finish = begin + len_ref[t - 1, 0, k]
                    inside = (tok_row >= begin) & (tok_row < finish)
                    value = jnp.where(tok_lane == ids_ref[t - 1, 0, k], 1.0, 0.0)
                    value = value - jnp.where(tok_lane == unit_lane, rew_ref[t - 1, 0, k], 0.0)
                    hot = hot + jnp.where(inside, value, 0.0)
                    begin = finish
                weight = jnp.sum(hot * means, axis=-1, keepdims=True)
                ca[1, t, rows_of(h), :] = (weight * lp[t - 1, rows_of(h), :].astype(F32)).astype(BF16)

    jobs = reductions()

    def axes_of(job):
        return ("l", "h") if job[2] % 2 == 0 else ("h", "l")

    def cols_of(j):
        return pl.ds(j * cc, cc)

    def split_copies(job):
        e = jobs[job]
        first, second = axes_of(job)
        count = count_of[second]
        source = (lambda part: gb.at[e, :, part]) if first == "l" else (lambda part: gb.at[e, part])
        return to_dp(
            source, lambda k: r1.at[e, k, pl.ds(0, count)], lambda k: r1_s.at[e, k], lambda k: r1_r.at[e, k], first
        )

    def join_copies(job):
        e = jobs[job]
        return to_dp(
            lambda part: p2.at[e, part], lambda k: r2.at[e, k], lambda k: r2_s.at[e, k], lambda k: r2_r.at[e, k],
            axes_of(job)[1],
        )

    def product(job):
        what, v, j = job
        e = jobs[job]
        if what == "out":
            value = jnp.dot(
                hid_t[v], ca[v, :, :, cols_of(j)].reshape(steps * tok, cc), preferred_element_type=F32
            )
        else:
            value = jnp.dot(
                gs_t[v].reshape(rank, steps * tok), xs[:, v, :, cols_of(j)].reshape(steps * tok, cc),
                preferred_element_type=F32,
            ) * gn_ref[v, :, cols_of(j)]
        gb[e] = value.astype(BF16).reshape(na, nb, rc, cc)
        for item in split_copies(job):
            item.start()

    def middle(job):
        e = jobs[job]
        first, second = axes_of(job)
        count = count_of[second]
        for item in split_copies(job):
            item.wait_recv()
        own = gb[e, :, me_l] if first == "l" else gb[e, me_h]
        total = own.astype(F32)
        for k in range(count_of[first] - 1):
            total = total + r1[e, k, :count].astype(F32)
        p2[e, :count] = total.astype(BF16)
        for item in join_copies(job):
            item.start()

    scale = 1.0 / (ndp * tok)

    def final(job):
        what, v, j = job
        e = jobs[job]
        kind = axes_of(job)[1]
        for item in join_copies(job):
            item.wait_recv()
        total = p2[e, me_h if kind == "h" else me_l].astype(F32)
        for k in range(count_of[kind] - 1):
            total = total + r2[e, k].astype(F32)
        dest = fo if what == "out" else fi
        dest[v, :, cols_of(j)] = total * scale

    def in_copies(v, j):
        base = v * CHUNKS + j
        return to_dp(
            lambda part: p2i.at[v, j, part], lambda k: r2i.at[v, j, k],
            lambda k: ri_s.at[base, k], lambda k: ri_r.at[base, k], split_kind[v],
        )

    def wait_gathered(v):
        for t in range(steps):
            for item in x_copies(t, v) + gs_copies(t, v):
                item.wait_recv()

    def grad_in(v, which):
        width = count_of[split_kind[v]]
        own = gs_t[v, me_h] if v == 0 else gs_t[v, :, me_l]
        own = own.reshape(width * rc, steps * tok)
        for j in which:
            value = jnp.dot(
                own, xs[:, v, :, cols_of(j)].reshape(steps * tok, cc), preferred_element_type=F32
            )
            for k in range(count_of[gather_kind[v]] - 1):
                left = gsr[v][k].reshape(width * rc, steps * tok)
                value = value + jnp.dot(
                    left, xr[v][k, :, :, cols_of(j)].reshape(steps * tok, cc), preferred_element_type=F32
                )
            value = value * gn_ref[v, :, cols_of(j)]
            p2i[v, j, :width] = value.astype(BF16).reshape(width, rc, cc)
            for item in in_copies(v, j):
                item.start()

    def final_in(v, j):
        for item in in_copies(v, j):
            item.wait_recv()
        along_h = split_kind[v] == "h"
        total = p2i[v, j, me_h if along_h else me_l].astype(F32)
        for k in range(count_of[split_kind[v]] - 1):
            total = total + r2i[v, j, k].astype(F32)
        fi[v, :, cols_of(j)] = total * scale

    def step(t, v, h):
        with scope(f"take_{t}{v}{h}"):
            take(t, v, h)
        with scope(f"back_{t}{v}{h}"):
            back_part(t, v, h)
            wait_back(t, v, h)
        with scope(f"fin_{t}{v}{h}"):
            finish_back(t, v, h)
        if t < steps - 1 and v == 1:
            send_on(t, v, h)

    halves = range(PARTS)
    with scope("stats"):
        for item in small:
            item.wait()
        start_gather(0, [0])
        stats_first()
        start_gather(1, range(steps))
    with scope("ld01"):
        loads[0].wait()
        loads[1].wait()
    with scope("first1"):
        back_part(0, 1)
        loads[2].wait()
        prep(1)
        loads[3].wait()
        pre_part(1)
        loads[4].wait()
        prep(0)
    with scope("wpre1"):
        finish_sq(1)
        for item in pre_copies[1]:
            item.wait_recv()
    with scope("fin1"):
        finish_pre(1, [0])
        wait_back(0, 1)
        for h in halves:
            finish_back(0, 1, h)
            send_on(0, 1, h)
        finish_gs(0, 1)
    with scope("first0"):
        stats_second()
        start_gather(0, range(1, steps))
        loads[5].wait()
        loads[6].wait()
        back_part(0, 0)
        loads[7].wait()
        pre_part(0)
        finish_pre(1, range(1, steps))
    with scope("wpre0"):
        finish_sq(0)
        for item in pre_copies[0]:
            item.wait_recv()
    with scope("fin0"):
        finish_pre(0, [0])
        wait_back(0, 0)
        for h in halves:
            finish_back(0, 0, h)
        finish_gs(0, 0)
        finish_pre(0, range(1, steps))
        loads[8].wait()
        for item in stat_copies("h"):
            item.wait_recv()

    for t in range(1, steps):
        for h in halves:
            step(t, 1, h)
        if t < steps - 1:
            if t == 1:
                for h in halves:
                    send_on(0, 0, h)
            finish_gs(t, 1)
    with scope("gout1"):
        finish_gs(steps - 1, 1)
        for j in range(CHUNKS):
            product(("out", 1, j))
    for t in range(1, steps - 1):
        for h in halves:
            step(t, 0, h)
            send_on(t, 0, h)
        finish_gs(t, 0)
    with scope("wgat1"):
        wait_gathered(1)
    with scope("gin1"):
        grad_in(1, range(GATHERED[1]))
    for j in range(GATHERED[1], CHUNKS):
        product(("in", 1, j))
    t = steps - 1
    step(t, 0, 0)
    with scope("mid1a"):
        for j in range(CHUNKS):
            middle(("out", 1, j))
    for h in halves[1:]:
        step(t, 0, h)
    with scope("gout0"):
        finish_gs(t, 0)
        for j in range(CHUNKS):
            product(("out", 0, j))
    with scope("mid1b"):
        for j in range(GATHERED[1], CHUNKS):
            middle(("in", 1, j))
    with scope("wgat0"):
        wait_gathered(0)
    with scope("gin0"):
        grad_in(0, range(GATHERED[0]))
        for j in range(GATHERED[0], CHUNKS):
            product(("in", 0, j))
    with scope("final1i"):
        for j in range(GATHERED[1]):
            final_in(1, j)
    for j in range(CHUNKS):
        with scope(f"mid0_{j}"):
            middle(("out", 0, j))
    for j in range(GATHERED[0], CHUNKS):
        middle(("in", 0, j))
    with scope("final1"):
        for job in jobs:
            if job[1] == 1:
                final(job)
    with scope("final0i"):
        for j in range(GATHERED[0]):
            final_in(0, j)
    for job in jobs:
        if job[1] == 0:
            with scope(f"fin0_{job[2]}"):
                final(job)
    for item in stat_copies("l") + stat_copies("h") + sq_copies(0) + sq_copies(1):
        item.wait_send()
    for items in back_copies.values():
        for item in items:
            item.wait_send()
    for v in range(vs):
        for item in pre_copies[v]:
            item.wait_send()
        for t in range(steps):
            for item in x_copies(t, v) + gs_copies(t, v):
                item.wait_send()
            if t < steps - 1:
                for h in halves:
                    sent_on(t, v, h)
        for j in range(GATHERED[v]):
            for item in in_copies(v, j):
                item.wait_send()
    for job in jobs:
        for item in split_copies(job) + join_copies(job):
            item.wait_send()


def shards(
    saved_inputs, proj_in, proj_out, norm_gain, arriving, logp_grad, rewards, seq_lengths, group_ids
):
    nt = lax.axis_size("tensor")
    npipe = lax.axis_size("pipe")
    ndp = lax.axis_size("dp")
    steps, vs, _, tok, wid = saved_inputs.shape
    rank = proj_in.shape[2]
    new_count = logp_grad.shape[0]
    group_count = new_count * ndp * rewards.shape[2] // 8
    lanes = -(-(group_count + 1) // 128) * 128
    na, nb = factors(ndp)
    rc = rank // ndp
    cc = wid // CHUNKS
    jobs = len(reductions())
    hm, lm = max(na - 1, 1), max(nb - 1, 1)
    dims = (steps, vs, tok, wid, rank, nt, npipe, ndp)
    peers = max(nt - 1, 1)
    any_spec = pl.BlockSpec(memory_space=pl.ANY)
    vmem = pl.BlockSpec(memory_space=pltpu.VMEM)
    V = pltpu.VMEM
    DMA = pltpu.SemaphoreType.DMA
    pmax = max(na, nb)
    less = max(pmax - 1, 1)
    scratch = [
        V((steps, vs, tok, wid), BF16),
        V((vs, steps * tok, wid), BF16),
        V((vs, steps, tok, wid), BF16),
        V((vs, rank, wid), BF16),
        V((vs, rank, wid), BF16),
        V((new_count, tok, wid), BF16),
        V((vs, steps * tok, rank), BF16),
        V((peers, vs, steps * tok, rank), BF16),
        V((vs, steps * tok, rank), F32),
        V((vs, steps * tok, rank), F32),
        V((vs, rank, steps * tok), BF16),
        V((vs, steps * tok, rank), BF16),
        V((vs, na, nb, rc, steps * tok), BF16),
        V((hm, nb, rc, steps * tok), BF16),
        V((lm, na, rc, steps * tok), BF16),
        V((hm, steps, tok, GATHERED[0] * cc), BF16),
        V((lm, steps, tok, GATHERED[1] * cc), BF16),
        V((vs, steps, tok, rank), BF16),
        V((peers, vs, steps, tok, rank), BF16),
        V((steps - 1, vs, tok, wid), BF16),
        V((vs, tok, 128), F32),
        V((peers, vs, tok, 128), F32),
        V((vs, tok, 128), F32),
        V((2, 8, lanes), F32),
        V((lm, 8, lanes), F32),
        V((jobs, na, nb, rc, cc), BF16),
        V((jobs, less, pmax, rc, cc), BF16),
        V((jobs, pmax, rc, cc), BF16),
        V((jobs, less, rc, cc), BF16),
        V((vs, CHUNKS, pmax, rc, cc), BF16),
        V((vs, CHUNKS, less, rc, cc), BF16),
        V(norm_gain.shape, F32),
        pltpu.SMEM(rewards.shape, F32),
        pltpu.SMEM(seq_lengths.shape, jnp.int32),
        pltpu.SMEM(group_ids.shape, jnp.int32),
        V((hm, 8, lanes), F32),
        DMA((13,)),
        DMA((2, vs, peers)),
        DMA((4, less)),
        DMA((2, vs, peers)),
        DMA((2, vs * steps * PARTS, peers)),
        DMA((steps - 1, vs, PARTS)),
        DMA((steps - 1, vs, PARTS)),
        DMA((vs * steps, less)),
        DMA((vs * steps, less)),
        DMA((vs * steps, less)),
        DMA((vs * steps, less)),
        DMA((jobs, less)),
        DMA((jobs, less)),
        DMA((jobs, less)),
        DMA((jobs, less)),
        DMA((vs * CHUNKS, less)),
        DMA((vs * CHUNKS, less)),
    ]
    grad_in, grad_out, leaving = pl.pallas_call(
        functools.partial(kernel, dims),
        out_shape=(
            V((vs, rc, wid), F32),
            V((vs, rc, wid), F32),
            V((vs, tok, wid), BF16),
        ),
        in_specs=[any_spec] * 9,
        out_specs=(vmem, vmem, vmem),
        scratch_shapes=scratch,
        compiler_params=pltpu.CompilerParams(
            collective_id=0, has_side_effects=True, vmem_limit_bytes=58 * 1024 * 1024
        ),
    )(
        saved_inputs[:, :, 0], proj_in[:, 0], proj_out[:, 0], norm_gain, arriving[:, 0], logp_grad,
        rewards, seq_lengths, group_ids,
    )
    return grad_in[:, None], grad_out[:, None], leaving[:, None]


def solution(mesh):
    return jax.shard_map(
        shards,
        mesh=mesh,
        in_specs=(
            P(None, None, "pipe", "dp", "tensor"),
            P(None, "pipe", None, "tensor"),
            P(None, "pipe", None, "tensor"),
            P(None, "pipe", "tensor"),
            P(None, "pipe", "dp", "tensor"),
            P(None, "dp", "tensor"),
            P(None, "dp", None),
            P(None, "dp", None),
            P(None, "dp", None),
        ),
        out_specs=(
            P(None, "pipe", "dp", "tensor"),
            P(None, "pipe", "dp", "tensor"),
            P(None, "pipe", "dp", "tensor"),
        ),
        check_vma=False,
    )
```

```python
import functools

import jax
import jax.numpy as jnp
from jax import lax
from jax.experimental import pallas as pl
from jax.experimental.pallas import tpu as pltpu
from jax.sharding import PartitionSpec as P

EPS = 1e-05
MESH = pl.DeviceIdType.MESH
F32 = jnp.float32
BF16 = jnp.bfloat16


def dot_nt(a, b):
    return lax.dot_general(a, b, (((1,), (1,)), ((), ())), preferred_element_type=F32)


def factors(n):
    low = 1
    for k in range(1, n + 1):
        if n % k == 0 and k * k <= n:
            low = k
    return low, n // low


CHUNKS = 4
GATHERED = (4, 4)
PARTS = 2
FIRST_AXIS = ("hhhl", "lllh")
scope = jax.named_scope


def reductions():
    jobs = [("out", v, j) for v in (1, 0) for j in range(CHUNKS)]
    jobs += [("in", v, j) for v in (1, 0) for j in range(GATHERED[v], CHUNKS)]
    return {job: e for e, job in enumerate(jobs)}


def kernel(
    dims,
    x_hbm, wi_hbm, wo_hbm, gn_hbm, ar_hbm, lp_hbm, rew_hbm, len_hbm, ids_hbm,
    fi, fo, lv,
    xs, gd, ca, wi, wo, lp, ps, pr, presum, slope, hid_t, gs, gs_t, gsr0, gsr1, xr0, xr1, bs, br, ob,
    sqs, sqr, inv_t, stl, str_, gb, r1, p2, r2, p2i, r2i,
    gn_ref, rew_ref, len_ref, ids_ref, str2, wrap_sem,
    in_sem, sq_sem, st_sem, pre_sem, back_sem, pipe_s, pipe_r, xg_s, xg_r, gt_s, gt_r, gf_s, gf_r,
    r1_s, r1_r, r2_s, r2_r, ri_s, ri_r,
):
    steps, vs, tok, wid, rank, nt, npipe, ndp = dims
    na, nb = factors(ndp)
    rc = rank // ndp
    full = wid * nt
    tile = min(512, wid // 2)
    rtile = min(512, rank)
    cc = wid // CHUNKS
    part_tok = tok // PARTS
    lanes = stl.shape[2]
    new_count, _, seq_count = rew_ref.shape
    unit_lane = new_count * ndp * seq_count // 8
    me_t = lax.axis_index("tensor")
    me_p = lax.axis_index("pipe")
    me_d = lax.axis_index("dp")
    me_h = me_d // nb
    me_l = me_d % nb
    prev_p = lax.rem(me_p + npipe - 1, npipe)
    next_p = lax.rem(me_p + 1, npipe)

    def load(src, dst, k):
        return pltpu.make_async_copy(src, dst, in_sem.at[k])

    loads = [
        load(ar_hbm.at[1], ca.at[1, 0], 0),
        load(wo_hbm.at[1], wo.at[1], 1),
        load(x_hbm.at[:, 1], xs.at[:, 1], 2),
        load(wi_hbm.at[1], wi.at[1], 3),
        load(x_hbm.at[:, 0], xs.at[:, 0], 4),
        load(ar_hbm.at[0], ca.at[0, 0], 5),
        load(wo_hbm.at[0], wo.at[0], 6),
        load(wi_hbm.at[0], wi.at[0], 7),
        load(lp_hbm, lp, 8),
    ]
    small = [
        load(gn_hbm, gn_ref, 9),
        load(rew_hbm, rew_ref, 10),
        load(len_hbm, len_ref, 11),
        load(ids_hbm, ids_ref, 12),
    ]

    barrier = pltpu.get_barrier_semaphore()
    for k in range(1, nt):
        pl.semaphore_signal(barrier, inc=1, device_id={"tensor": lax.rem(me_t + k, nt)}, device_id_type=MESH)
    for k in range(1, na):
        peer = lax.rem(me_h + k, na) * nb + me_l
        pl.semaphore_signal(barrier, inc=1, device_id={"dp": peer}, device_id_type=MESH)
    for k in range(1, nb):
        peer = me_h * nb + lax.rem(me_l + k, nb)
        pl.semaphore_signal(barrier, inc=1, device_id={"dp": peer}, device_id_type=MESH)

    @pl.when(me_p < npipe - 1)
    def _():
        pl.semaphore_signal(barrier, inc=1, device_id={"pipe": next_p}, device_id_type=MESH)

    @pl.when(me_p == 0)
    def _():
        pl.semaphore_signal(barrier, inc=1, device_id={"pipe": prev_p}, device_id_type=MESH)


    for item in small + loads:
        item.start()

    with scope("barrier"):
        along_pipe = jnp.where(me_p == 0, 0, jnp.where(me_p == npipe - 1, 2, 1))
        pl.semaphore_wait(barrier, nt - 1 + na - 1 + nb - 1 + along_pipe)

    @pl.when(me_p == npipe - 1)
    def _():
        pl.semaphore_signal(wrap_sem, inc=1, device_id={"pipe": next_p}, device_id_type=MESH)

    def to_tensor(src, dst_of, send_of, recv_of):
        return [
            pltpu.make_async_remote_copy(
                src_ref=src, dst_ref=dst_of(k - 1), send_sem=send_of(k - 1), recv_sem=recv_of(k - 1),
                device_id={"tensor": lax.rem(me_t + k, nt)}, device_id_type=MESH,
            )
            for k in range(1, nt)
        ]

    def to_dp(src_of, dst_of, send_of, recv_of, kind):
        out = []
        count = {"h": na, "l": nb}[kind]
        for k in range(1, count):
            if kind == "h":
                part = lax.rem(me_h + k, na)
                who = part * nb + me_l
            else:
                part = lax.rem(me_l + k, nb)
                who = me_h * nb + part
            out.append(
                pltpu.make_async_remote_copy(
                    src_ref=src_of(part), dst_ref=dst_of(k - 1), send_sem=send_of(k - 1), recv_sem=recv_of(k - 1),
                    device_id={"dp": who}, device_id_type=MESH,
                )
            )
        return out

    gather_kind = ("h", "l")
    split_kind = ("l", "h")
    count_of = {"h": na, "l": nb}
    xr = (xr0, xr1)
    gsr = (gsr0, gsr1)

    def x_copies(t, v):
        base = v * steps + t
        cols = pl.ds(0, GATHERED[v] * cc)
        return to_dp(
            lambda part: x_hbm.at[t, v, :, cols], lambda k: xr[v].at[k, t],
            lambda k: xg_s.at[base, k], lambda k: xg_r.at[base, k], gather_kind[v],
        )


    def stat_copies(kind):
        if kind == "l":
            return to_dp(lambda part: stl.at[0], lambda k: str_.at[k], lambda k: st_sem.at[0, k], lambda k: st_sem.at[1, k], kind)
        return to_dp(lambda part: stl.at[1], lambda k: str2.at[k], lambda k: st_sem.at[2, k], lambda k: st_sem.at[3, k], kind)

    def stats_first():
        lane8 = lax.broadcasted_iota(jnp.int32, (8, lanes), 1)
        row8 = lax.broadcasted_iota(jnp.int32, (8, lanes), 0)
        stats_own = jnp.where((row8 == 2) & (lane8 == unit_lane), 1.0, 0.0)
        for n in range(new_count):
            for k in range(seq_count):
                value = jnp.where(row8 == 0, rew_ref[n, 0, k], jnp.where(row8 == 1, 1.0, 0.0))
                stats_own = stats_own + jnp.where(lane8 == ids_ref[n, 0, k], value, 0.0)
        stl[0] = stats_own
        for item in stat_copies("l"):
            item.start()

    def stats_second():
        for item in stat_copies("l"):
            item.wait_recv()
        total = stl[0]
        for k in range(nb - 1):
            total = total + str_[k]
        stl[1] = total
        for item in stat_copies("h"):
            item.start()

    def start_gather(v, which):
        for t in which:
            for item in x_copies(t, v):
                item.start()

    lane = lax.broadcasted_iota(jnp.int32, (tok, 128), 1)

    def sq_copies(v):
        return to_tensor(
            sqs.at[v], lambda k: sqr.at[k, v], lambda k: sq_sem.at[0, v, k], lambda k: sq_sem.at[1, v, k]
        )

    def prep(v):
        def body(t, squares_all):
            row = xs[t, v].astype(F32)
            gd[v, pl.ds(pl.multiple_of(t * tok, tok), tok), :] = (row * gn_ref[v]).astype(BF16)
            squares = jnp.sum(row * row, axis=-1, keepdims=True)
            return jnp.where(lane == t, squares, squares_all)

        sqs[v] = lax.fori_loop(0, steps, body, jnp.zeros((tok, 128), F32))
        for item in sq_copies(v):
            item.start()

    def finish_sq(v):
        for item in sq_copies(v):
            item.wait_recv()
        total = sqs[v]
        for k in range(nt - 1):
            total = total + sqr[k, v]
        inv_t[v] = 1.0 / jnp.sqrt(total * (1.0 / full) + EPS)

    def share_of(v):
        count = count_of[split_kind[v]]
        if count % nt:
            return pl.ds(0, count)
        return pl.ds(me_t * (count // nt), count // nt)

    def gs_copies(t, v):
        cols = pl.ds(t * tok, tok)
        base = v * steps + t
        mine = share_of(v)
        source = (lambda part: gs_t.at[v, part, mine, :, cols]) if v == 0 else (lambda part: gs_t.at[v, mine, part, :, cols])
        return to_dp(
            source, lambda k: gsr[v].at[k, mine, :, cols],
            lambda k: gt_s.at[base, k], lambda k: gt_r.at[base, k], gather_kind[v],
        )

    def pass_copies(t, v):
        if count_of[split_kind[v]] % nt:
            return []
        cols = pl.ds(t * tok, tok)
        base = v * steps + t
        out = []
        for k in range(count_of[gather_kind[v]] - 1):
            piece = gsr[v].at[k, share_of(v), :, cols]
            out += to_tensor(piece, lambda i: piece, lambda i: gf_s.at[base, k, i], lambda i: gf_r.at[base, k, i])
        return out

    pre_copies = {}
    back_copies = {}

    def pre_part(v):
        def body(j, carry):
            cols = pl.ds(pl.multiple_of(j * rtile, rtile), rtile)
            ps[v, :, cols] = dot_nt(gd[v], wi[v, cols, :]).astype(BF16)
            return carry

        lax.fori_loop(0, rank // rtile, body, 0)
        pre_copies[v] = to_tensor(
            ps.at[v], lambda k: pr.at[k, v], lambda k: pre_sem.at[0, v, k], lambda k: pre_sem.at[1, v, k]
        )
        for item in pre_copies[v]:
            item.start()

    def rows_of(h):
        return pl.ds(h * part_tok, part_tok)

    def back_part(t, v, h=None):
        rows = pl.ds(0, tok) if h is None else rows_of(h)

        def body(j, carry):
            cols = pl.ds(pl.multiple_of(j * rtile, rtile), rtile)
            bs[v, t, rows, cols] = dot_nt(ca[v, t, rows, :], wo[v, cols, :]).astype(BF16)
            return carry

        lax.fori_loop(0, rank // rtile, body, 0)
        base = (v * steps + t) * PARTS + (h or 0)
        back_copies[t, v, h] = to_tensor(
            bs.at[v, t, rows], lambda k: br.at[k, v, t, rows],
            lambda k: back_sem.at[0, base, k], lambda k: back_sem.at[1, base, k],
        )
        for item in back_copies[t, v, h]:
            item.start()

    def finish_pre(v, which_steps):
        for t in which_steps:
            rows = pl.ds(t * tok, tok)
            total = ps[v, rows, :].astype(F32)
            for k in range(nt - 1):
                total = total + pr[k, v, rows, :].astype(F32)
            pre = inv_t[v, :, t:t + 1] * total
            sigma = jax.nn.sigmoid(pre)
            presum[v, rows, :] = total
            hid_t[v, :, rows] = jnp.transpose(pre * sigma).astype(BF16)
            slope[v, rows, :] = sigma * (1.0 + pre * (1.0 - sigma))

    def wait_back(t, v, h=None):
        for item in back_copies[t, v, h]:
            item.wait_recv()

    def finish_back(t, v, h):
        own = rows_of(h)
        rows = pl.ds(t * tok + h * part_tok, part_tok)
        inv = inv_t[v, own, t:t + 1]
        total = bs[v, t, own, :].astype(F32)
        for k in range(nt - 1):
            total = total + br[k, v, t, own, :].astype(F32)
        grad_pre = total * slope[v, rows, :]
        gs[v, rows, :] = (inv * grad_pre).astype(BF16)
        radial = jnp.sum(grad_pre * presum[v, rows, :], axis=-1, keepdims=True)
        coef = inv * inv * inv * radial * (1.0 / full)

        def body(j, carry):
            cols = pl.ds(pl.multiple_of(j * tile, tile), tile)
            lifted = jnp.dot(gs[v, rows, :], wi[v, :, cols], preferred_element_type=F32)
            out = (
                ca[v, t, own, cols].astype(F32)
                + gn_ref[v, :, cols] * lifted
                - xs[t, v, own, cols].astype(F32) * coef
            ).astype(BF16)
            if t < steps - 1:
                ob[t, v, own, cols] = out
            else:
                lv[v, own, cols] = out
            return carry

        lax.fori_loop(0, wid // tile, body, 0)

    def finish_gs(t, v):
        rows = pl.ds(t * tok, tok)
        flipped = jnp.transpose(gs[v, rows, :].astype(F32)).astype(BF16)
        gs_t[v, :, :, :, rows] = flipped.reshape(na, nb, rc, tok)
        for item in gs_copies(t, v):
            item.start()

    def pipe_copy(t, v, slot, h):
        return pltpu.make_async_remote_copy(
            src_ref=ob.at[t, v, rows_of(h)], dst_ref=ca.at[slot, t + 1, rows_of(h)],
            send_sem=pipe_s.at[t, v, h], recv_sem=pipe_r.at[t, slot, h],
            device_id={"pipe": prev_p}, device_id_type=MESH,
        )

    def send_on(t, v, h):
        @pl.when(me_p > 0)
        def _():
            pipe_copy(t, v, v, h).start()

        if v == 1:
            @pl.when(me_p == 0)
            def _():
                if t == 0 and h == 0:
                    pl.semaphore_wait(wrap_sem, 1)
                pipe_copy(t, 1, 0, h).start()

    def sent_on(t, v, h):
        @pl.when(me_p > 0)
        def _():
            pipe_copy(t, v, v, h).wait_send()

        if v == 1:
            @pl.when(me_p == 0)
            def _():
                pipe_copy(t, 1, 0, h).wait_send()

    def take(t, v, h):
        if v == 0:
            pipe_copy(t - 1, v, v, h).wait_recv()
        else:
            @pl.when(me_p < npipe - 1)
            def _():
                pipe_copy(t - 1, v, v, h).wait_recv()

            @pl.when(me_p == npipe - 1)
            def _():
                if t == 1 and h == 0:
                    for item in stat_copies("h"):
                        item.wait_recv()
                stats = stl[1]
                for k in range(na - 1):
                    stats = stats + str2[k]
                means = stats[0:1] / jnp.maximum(stats[1:2], 1.0) + stats[2:3] * (1.0 / ndp)
                tok_row = lax.broadcasted_iota(jnp.int32, (part_tok, lanes), 0) + h * part_tok
                tok_lane = lax.broadcasted_iota(jnp.int32, (part_tok, lanes), 1)
                hot = jnp.zeros((part_tok, lanes), F32)
                begin = 0
                for k in range(seq_count):
                    finish = begin + len_ref[t - 1, 0, k]
                    inside = (tok_row >= begin) & (tok_row < finish)
                    value = jnp.where(tok_lane == ids_ref[t - 1, 0, k], 1.0, 0.0)
                    value = value - jnp.where(tok_lane == unit_lane, rew_ref[t - 1, 0, k], 0.0)
                    hot = hot + jnp.where(inside, value, 0.0)
                    begin = finish
                weight = jnp.sum(hot * means, axis=-1, keepdims=True)
                ca[1, t, rows_of(h), :] = (weight * lp[t - 1, rows_of(h), :].astype(F32)).astype(BF16)

    jobs = reductions()

    def axes_of(job):
        return ("l", "h") if FIRST_AXIS[job[1]][job[2]] == "l" else ("h", "l")

    def cols_of(j):
        return pl.ds(j * cc, cc)

    def split_copies(job):
        e = jobs[job]
        first, second = axes_of(job)
        count = count_of[second]
        source = (lambda part: gb.at[e, :, part]) if first == "l" else (lambda part: gb.at[e, part])
        return to_dp(
            source, lambda k: r1.at[e, k, pl.ds(0, count)], lambda k: r1_s.at[e, k], lambda k: r1_r.at[e, k], first
        )

    def join_copies(job):
        e = jobs[job]
        return to_dp(
            lambda part: p2.at[e, part], lambda k: r2.at[e, k], lambda k: r2_s.at[e, k], lambda k: r2_r.at[e, k],
            axes_of(job)[1],
        )

    def product(job):
        what, v, j = job
        e = jobs[job]
        if what == "out":
            value = jnp.dot(
                hid_t[v], ca[v, :, :, cols_of(j)].reshape(steps * tok, cc), preferred_element_type=F32
            )
        else:
            value = jnp.dot(
                gs_t[v].reshape(rank, steps * tok), xs[:, v, :, cols_of(j)].reshape(steps * tok, cc),
                preferred_element_type=F32,
            ) * gn_ref[v, :, cols_of(j)]
        gb[e] = value.astype(BF16).reshape(na, nb, rc, cc)
        for item in split_copies(job):
            item.start()

    def middle(job):
        e = jobs[job]
        first, second = axes_of(job)
        count = count_of[second]
        for item in split_copies(job):
            item.wait_recv()
        own = gb[e, :, me_l] if first == "l" else gb[e, me_h]
        total = own.astype(F32)
        for k in range(count_of[first] - 1):
            total = total + r1[e, k, :count].astype(F32)
        p2[e, :count] = total.astype(BF16)
        for item in join_copies(job):
            item.start()

    scale = 1.0 / (ndp * tok)

    def final(job):
        what, v, j = job
        e = jobs[job]
        kind = axes_of(job)[1]
        for item in join_copies(job):
            item.wait_recv()
        total = p2[e, me_h if kind == "h" else me_l].astype(F32)
        for k in range(count_of[kind] - 1):
            total = total + r2[e, k].astype(F32)
        dest = fo if what == "out" else fi
        dest[v, :, cols_of(j)] = total * scale

    def in_copies(v, j):
        base = v * CHUNKS + j
        return to_dp(
            lambda part: p2i.at[v, j, part], lambda k: r2i.at[v, j, k],
            lambda k: ri_s.at[base, k], lambda k: ri_r.at[base, k], split_kind[v],
        )

    def wait_gathered(v):
        for t in range(steps):
            for item in gs_copies(t, v):
                item.wait_recv()
            for item in pass_copies(t, v):
                item.start()
        for t in range(steps):
            for item in x_copies(t, v) + pass_copies(t, v):
                item.wait_recv()

    def grad_in(v, which):
        width = count_of[split_kind[v]]
        own = gs_t[v, me_h] if v == 0 else gs_t[v, :, me_l]
        own = own.reshape(width * rc, steps * tok)
        for j in which:
            value = jnp.dot(
                own, xs[:, v, :, cols_of(j)].reshape(steps * tok, cc), preferred_element_type=F32
            )
            for k in range(count_of[gather_kind[v]] - 1):
                left = gsr[v][k].reshape(width * rc, steps * tok)
                value = value + jnp.dot(
                    left, xr[v][k, :, :, cols_of(j)].reshape(steps * tok, cc), preferred_element_type=F32
                )
            value = value * gn_ref[v, :, cols_of(j)]
            p2i[v, j, :width] = value.astype(BF16).reshape(width, rc, cc)
            for item in in_copies(v, j):
                item.start()

    def final_in(v, j):
        for item in in_copies(v, j):
            item.wait_recv()
        along_h = split_kind[v] == "h"
        total = p2i[v, j, me_h if along_h else me_l].astype(F32)
        for k in range(count_of[split_kind[v]] - 1):
            total = total + r2i[v, j, k].astype(F32)
        fi[v, :, cols_of(j)] = total * scale

    def step(t, v, h):
        with scope(f"take_{t}{v}{h}"):
            take(t, v, h)
        with scope(f"back_{t}{v}{h}"):
            back_part(t, v, h)
            wait_back(t, v, h)
        with scope(f"fin_{t}{v}{h}"):
            finish_back(t, v, h)
        if t < steps - 1 and v == 1:
            send_on(t, v, h)

    halves = range(PARTS)
    with scope("stats"):
        for item in small:
            item.wait()
        start_gather(0, [0])
        stats_first()
        start_gather(1, range(steps))
    with scope("ld01"):
        loads[0].wait()
        loads[1].wait()
    with scope("first1"):
        back_part(0, 1)
        loads[2].wait()
        prep(1)
        loads[3].wait()
        pre_part(1)
        loads[4].wait()
        prep(0)
    with scope("wpre1"):
        finish_sq(1)
        for item in pre_copies[1]:
            item.wait_recv()
    with scope("fin1"):
        finish_pre(1, [0])
        wait_back(0, 1)
        for h in halves:
            finish_back(0, 1, h)
            send_on(0, 1, h)
        finish_gs(0, 1)
    with scope("first0"):
        stats_second()
        start_gather(0, range(1, steps))
        loads[5].wait()
        loads[6].wait()
        back_part(0, 0)
        loads[7].wait()
        pre_part(0)
        finish_pre(1, range(1, steps))
    with scope("wpre0"):
        finish_sq(0)
        for item in pre_copies[0]:
            item.wait_recv()
    with scope("fin0"):
        finish_pre(0, [0])
        wait_back(0, 0)
        for h in halves:
            finish_back(0, 0, h)
        finish_gs(0, 0)
        finish_pre(0, range(1, steps))
        loads[8].wait()

    for t in range(1, steps):
        for h in halves:
            step(t, 1, h)
        if t < steps - 1:
            if t == 1:
                for h in halves:
                    send_on(0, 0, h)
            finish_gs(t, 1)
    last = steps - 1
    early = min(3, GATHERED[1])
    with scope("gout1"):
        finish_gs(last, 1)
        for j in (0, 3, 1, 2):
            product(("out", 1, j))
        for j in range(GATHERED[1], CHUNKS):
            product(("in", 1, j))

    def gather_in_1():
        with scope("wgat1"):
            wait_gathered(1)
        with scope("gin1"):
            grad_in(1, range(early))

    for t in range(1, last):
        for h in halves:
            step(t, 0, h)
            send_on(t, 0, h)
            if t == last - 1 and h == 0:
                gather_in_1()
        finish_gs(t, 0)
    with scope("mid1a"):
        middle(("out", 1, 3))
        middle(("out", 1, 0))
    step(last, 0, 0)
    with scope("mid1b"):
        middle(("out", 1, 1))
    for h in halves[1:]:
        step(last, 0, h)
    with scope("gout0"):
        finish_gs(last, 0)
        for j in (3, 0, 1, 2):
            product(("out", 0, j))
    with scope("gin1b"):
        middle(("out", 1, 2))
        grad_in(1, range(early, GATHERED[1]))
        for j in range(GATHERED[1], CHUNKS):
            middle(("in", 1, j))
    with scope("wgat0"):
        wait_gathered(0)
    with scope("gin0"):
        grad_in(0, range(GATHERED[0]))
        for j in range(GATHERED[0], CHUNKS):
            product(("in", 0, j))
    with scope("mid0_3"):
        middle(("out", 0, 3))
    with scope("mid0_0"):
        middle(("out", 0, 0))
    with scope("final1a"):
        for j in (0, 1, 3):
            final(("out", 1, j))
        for j in range(early):
            final_in(1, j)
    @pl.when(me_p < npipe - 1)
    def _():
        for item in stat_copies("h"):
            item.wait_recv()

    with scope("drain"):
        for item in stat_copies("l") + stat_copies("h") + sq_copies(0) + sq_copies(1):
            item.wait_send()
        for items in back_copies.values():
            for item in items:
                item.wait_send()
        for v in range(vs):
            for item in pre_copies[v]:
                item.wait_send()
            for t in range(steps):
                for item in x_copies(t, v) + gs_copies(t, v) + pass_copies(t, v):
                    item.wait_send()
                if t < steps - 1:
                    for h in halves:
                        sent_on(t, v, h)
    for j in (1, 2):
        with scope(f"mid0_{j}"):
            middle(("out", 0, j))
    for j in range(GATHERED[0], CHUNKS):
        middle(("in", 0, j))
    with scope("final0i"):
        for j in range(GATHERED[0]):
            final_in(0, j)
    with scope("final1b"):
        for j in range(early, GATHERED[1]):
            final_in(1, j)
        for j in range(GATHERED[1], CHUNKS):
            final(("in", 1, j))
        final(("out", 1, 2))
    for v in range(vs):
        for j in range(GATHERED[v]):
            for item in in_copies(v, j):
                item.wait_send()
    for job in jobs:
        for item in split_copies(job):
            item.wait_send()
    for j in (0, 1, 3, 2):
        with scope(f"fin0_{j}"):
            final(("out", 0, j))
    for j in range(GATHERED[0], CHUNKS):
        final(("in", 0, j))
    with scope("tail"):
        for job in jobs:
            for item in join_copies(job):
                item.wait_send()


def store(a, b, c, a_out, b_out, c_out, sem):
    copies = [pltpu.make_async_copy(*pair, sem.at[k]) for k, pair in enumerate(((a, a_out), (b, b_out), (c, c_out)))]
    for item in copies:
        item.start()
    for item in copies:
        item.wait()


def shards(
    saved_inputs, proj_in, proj_out, norm_gain, arriving, logp_grad, rewards, seq_lengths, group_ids
):
    nt = lax.axis_size("tensor")
    npipe = lax.axis_size("pipe")
    ndp = lax.axis_size("dp")
    steps, vs, _, tok, wid = saved_inputs.shape
    rank = proj_in.shape[2]
    new_count = logp_grad.shape[0]
    group_count = new_count * ndp * rewards.shape[2] // 8
    lanes = -(-(group_count + 1) // 128) * 128
    na, nb = factors(ndp)
    rc = rank // ndp
    cc = wid // CHUNKS
    jobs = len(reductions())
    hm, lm = max(na - 1, 1), max(nb - 1, 1)
    dims = (steps, vs, tok, wid, rank, nt, npipe, ndp)
    peers = max(nt - 1, 1)
    any_spec = pl.BlockSpec(memory_space=pl.ANY)
    vmem = pl.BlockSpec(memory_space=pltpu.VMEM)
    V = pltpu.VMEM
    DMA = pltpu.SemaphoreType.DMA
    pmax = max(na, nb)
    less = max(pmax - 1, 1)
    scratch = [
        V((steps, vs, tok, wid), BF16),
        V((vs, steps * tok, wid), BF16),
        V((vs, steps, tok, wid), BF16),
        V((vs, rank, wid), BF16),
        V((vs, rank, wid), BF16),
        V((new_count, tok, wid), BF16),
        V((vs, steps * tok, rank), BF16),
        V((peers, vs, steps * tok, rank), BF16),
        V((vs, steps * tok, rank), F32),
        V((vs, steps * tok, rank), F32),
        V((vs, rank, steps * tok), BF16),
        V((vs, steps * tok, rank), BF16),
        V((vs, na, nb, rc, steps * tok), BF16),
        V((hm, nb, rc, steps * tok), BF16),
        V((lm, na, rc, steps * tok), BF16),
        V((hm, steps, tok, GATHERED[0] * cc), BF16),
        V((lm, steps, tok, GATHERED[1] * cc), BF16),
        V((vs, steps, tok, rank), BF16),
        V((peers, vs, steps, tok, rank), BF16),
        V((steps - 1, vs, tok, wid), BF16),
        V((vs, tok, 128), F32),
        V((peers, vs, tok, 128), F32),
        V((vs, tok, 128), F32),
        V((2, 8, lanes), F32),
        V((lm, 8, lanes), F32),
        V((jobs, na, nb, rc, cc), BF16),
        V((jobs, less, pmax, rc, cc), BF16),
        V((jobs, pmax, rc, cc), BF16),
        V((jobs, less, rc, cc), BF16),
        V((vs, CHUNKS, pmax, rc, cc), BF16),
        V((vs, CHUNKS, less, rc, cc), BF16),
        V(norm_gain.shape, F32),
        pltpu.SMEM(rewards.shape, F32),
        pltpu.SMEM(seq_lengths.shape, jnp.int32),
        pltpu.SMEM(group_ids.shape, jnp.int32),
        V((hm, 8, lanes), F32),
        pltpu.SemaphoreType.REGULAR,
        DMA((13,)),
        DMA((2, vs, peers)),
        DMA((4, less)),
        DMA((2, vs, peers)),
        DMA((2, vs * steps * PARTS, peers)),
        DMA((steps - 1, vs, PARTS)),
        DMA((steps - 1, vs, PARTS)),
        DMA((vs * steps, less)),
        DMA((vs * steps, less)),
        DMA((vs * steps, less)),
        DMA((vs * steps, less)),
        DMA((vs * steps, less, peers)),
        DMA((vs * steps, less, peers)),
        DMA((jobs, less)),
        DMA((jobs, less)),
        DMA((jobs, less)),
        DMA((jobs, less)),
        DMA((vs * CHUNKS, less)),
        DMA((vs * CHUNKS, less)),
    ]
    grad_in, grad_out, leaving = pl.pallas_call(
        functools.partial(kernel, dims),
        out_shape=(
            V((vs, rc, wid), F32),
            V((vs, rc, wid), F32),
            V((vs, tok, wid), BF16),
        ),
        in_specs=[any_spec] * 9,
        out_specs=(vmem, vmem, vmem),
        scratch_shapes=scratch,
        compiler_params=pltpu.CompilerParams(
            collective_id=0, has_side_effects=True, vmem_limit_bytes=58 * 1024 * 1024
        ),
    )(
        saved_inputs[:, :, 0], proj_in[:, 0], proj_out[:, 0], norm_gain, arriving[:, 0], logp_grad,
        rewards, seq_lengths, group_ids,
    )
    grad_in, grad_out, leaving = pl.pallas_call(
        store,
        out_shape=tuple(jax.ShapeDtypeStruct(a.shape, a.dtype) for a in (grad_in, grad_out, leaving)),
        in_specs=[vmem] * 3,
        out_specs=[any_spec] * 3,
        scratch_shapes=[DMA((3,))],
        compiler_params=pltpu.CompilerParams(vmem_limit_bytes=1024 * 1024),
    )(grad_in, grad_out, leaving)
    return grad_in[:, None], grad_out[:, None], leaving[:, None]


def solution(mesh):
    return jax.shard_map(
        shards,
        mesh=mesh,
        in_specs=(
            P(None, None, "pipe", "dp", "tensor"),
            P(None, "pipe", None, "tensor"),
            P(None, "pipe", None, "tensor"),
            P(None, "pipe", "tensor"),
            P(None, "pipe", "dp", "tensor"),
            P(None, "dp", "tensor"),
            P(None, "dp", None),
            P(None, "dp", None),
            P(None, "dp", None),
        ),
        out_specs=(
            P(None, "pipe", "dp", "tensor"),
            P(None, "pipe", "dp", "tensor"),
            P(None, "pipe", "dp", "tensor"),
        ),
        check_vma=False,
    )
```

```python
import functools

import jax
import jax.numpy as jnp
from jax import lax
from jax.experimental import pallas as pl
from jax.experimental.pallas import tpu as pltpu
from jax.sharding import PartitionSpec as P

EPS = 1e-05
MESH = pl.DeviceIdType.MESH
F32 = jnp.float32
BF16 = jnp.bfloat16


def dot_nt(a, b):
    return lax.dot_general(a, b, (((1,), (1,)), ((), ())), preferred_element_type=F32)


def factors(n):
    low = 1
    for k in range(1, n + 1):
        if n % k == 0 and k * k <= n:
            low = k
    return low, n // low


CHUNKS = 4
GATHERED = (4, 3)
PARTS = 2
FIRST_AXIS = ("hhhl", "lllh")
IN_AXIS = ("h", "l")
ORDER = ((3, 0, 1, 2), (3, 0, 1, 2))
scope = jax.named_scope


def reductions():
    jobs = [("out", v, j) for v in (1, 0) for j in range(CHUNKS)]
    jobs += [("in", v, j) for v in (1, 0) for j in range(GATHERED[v], CHUNKS)]
    return {job: e for e, job in enumerate(jobs)}


def pieces(steps, t, h):
    return ORDER[0] if t == steps - 2 and h == PARTS - 1 else (None,)


def pipe_slots(steps, vs):
    keys = [(t, v, h, c) for t in range(steps - 1) for v in range(vs) for h in range(PARTS) for c in pieces(steps, t, h)]
    return {key: k for k, key in enumerate(keys)}


def kernel(
    dims,
    x_hbm, wi_hbm, wo_hbm, gn_hbm, ar_hbm, lp_hbm, rew_hbm, len_hbm, ids_hbm,
    fi, fo, lv,
    xs, gd, ca, wi, wo, lp, ps, pr, presum, slope, hid_t, gs, gs_t, gsr0, gsr1, xr0, xr1, bs, br, ob,
    sqs, sqr, inv_t, stl, str_, gb, r1, p2, r2, p2i, r2i,
    gn_ref, rew_ref, len_ref, ids_ref, str2, wrap_sem,
    in_sem, sq_sem, st_sem, pre_sem, back_sem, pipe_s, pipe_r, xg_s, xg_r, gt_s, gt_r, gf_s, gf_r,
    r1_s, r1_r, r2_s, r2_r, ri_s, ri_r,
):
    steps, vs, tok, wid, rank, nt, npipe, ndp = dims
    na, nb = factors(ndp)
    rc = rank // ndp
    full = wid * nt
    tile = min(512, wid // 2)
    rtile = min(512, rank)
    cc = wid // CHUNKS
    part_tok = tok // PARTS
    lanes = stl.shape[2]
    new_count, _, seq_count = rew_ref.shape
    unit_lane = new_count * ndp * seq_count // 8
    me_t = lax.axis_index("tensor")
    me_p = lax.axis_index("pipe")
    me_d = lax.axis_index("dp")
    me_h = me_d // nb
    me_l = me_d % nb
    prev_p = lax.rem(me_p + npipe - 1, npipe)
    next_p = lax.rem(me_p + 1, npipe)

    def load(src, dst, k):
        return pltpu.make_async_copy(src, dst, in_sem.at[k])

    loads = [
        load(ar_hbm.at[1], ca.at[1, 0], 0),
        load(wo_hbm.at[1], wo.at[1], 1),
        load(x_hbm.at[:, 1], xs.at[:, 1], 2),
        load(wi_hbm.at[1], wi.at[1], 3),
        load(x_hbm.at[:, 0], xs.at[:, 0], 4),
        load(ar_hbm.at[0], ca.at[0, 0], 5),
        load(wo_hbm.at[0], wo.at[0], 6),
        load(wi_hbm.at[0], wi.at[0], 7),
        load(lp_hbm, lp, 8),
    ]
    small = [
        load(gn_hbm, gn_ref, 9),
        load(rew_hbm, rew_ref, 10),
        load(len_hbm, len_ref, 11),
        load(ids_hbm, ids_ref, 12),
    ]

    barrier = pltpu.get_barrier_semaphore()
    for k in range(1, nt):
        pl.semaphore_signal(barrier, inc=1, device_id={"tensor": lax.rem(me_t + k, nt)}, device_id_type=MESH)
    for k in range(1, na):
        peer = lax.rem(me_h + k, na) * nb + me_l
        pl.semaphore_signal(barrier, inc=1, device_id={"dp": peer}, device_id_type=MESH)
    for k in range(1, nb):
        peer = me_h * nb + lax.rem(me_l + k, nb)
        pl.semaphore_signal(barrier, inc=1, device_id={"dp": peer}, device_id_type=MESH)

    @pl.when(me_p < npipe - 1)
    def _():
        pl.semaphore_signal(barrier, inc=1, device_id={"pipe": next_p}, device_id_type=MESH)

    @pl.when(me_p == 0)
    def _():
        pl.semaphore_signal(barrier, inc=1, device_id={"pipe": prev_p}, device_id_type=MESH)


    for item in small + loads:
        item.start()

    with scope("barrier"):
        along_pipe = jnp.where(me_p == 0, 0, jnp.where(me_p == npipe - 1, 2, 1))
        pl.semaphore_wait(barrier, nt - 1 + na - 1 + nb - 1 + along_pipe)

    @pl.when(me_p == npipe - 1)
    def _():
        pl.semaphore_signal(wrap_sem, inc=1, device_id={"pipe": next_p}, device_id_type=MESH)

    def to_tensor(src, dst_of, send_of, recv_of):
        return [
            pltpu.make_async_remote_copy(
                src_ref=src, dst_ref=dst_of(k - 1), send_sem=send_of(k - 1), recv_sem=recv_of(k - 1),
                device_id={"tensor": lax.rem(me_t + k, nt)}, device_id_type=MESH,
            )
            for k in range(1, nt)
        ]

    def to_dp(src_of, dst_of, send_of, recv_of, kind):
        out = []
        count = {"h": na, "l": nb}[kind]
        for k in range(1, count):
            if kind == "h":
                part = lax.rem(me_h + k, na)
                who = part * nb + me_l
            else:
                part = lax.rem(me_l + k, nb)
                who = me_h * nb + part
            out.append(
                pltpu.make_async_remote_copy(
                    src_ref=src_of(part), dst_ref=dst_of(k - 1), send_sem=send_of(k - 1), recv_sem=recv_of(k - 1),
                    device_id={"dp": who}, device_id_type=MESH,
                )
            )
        return out

    gather_kind = ("h", "l")
    split_kind = ("l", "h")
    count_of = {"h": na, "l": nb}
    xr = (xr0, xr1)
    gsr = (gsr0, gsr1)

    def x_copies(t, v):
        base = v * steps + t
        cols = pl.ds(0, GATHERED[v] * cc)
        return to_dp(
            lambda part: x_hbm.at[t, v, :, cols], lambda k: xr[v].at[k, t],
            lambda k: xg_s.at[base, k], lambda k: xg_r.at[base, k], gather_kind[v],
        )


    def stat_copies(kind):
        if kind == "l":
            return to_dp(lambda part: stl.at[0], lambda k: str_.at[k], lambda k: st_sem.at[0, k], lambda k: st_sem.at[1, k], kind)
        return to_dp(lambda part: stl.at[1], lambda k: str2.at[k], lambda k: st_sem.at[2, k], lambda k: st_sem.at[3, k], kind)

    def stats_first():
        lane8 = lax.broadcasted_iota(jnp.int32, (8, lanes), 1)
        row8 = lax.broadcasted_iota(jnp.int32, (8, lanes), 0)
        stats_own = jnp.where((row8 == 2) & (lane8 == unit_lane), 1.0, 0.0)
        for n in range(new_count):
            for k in range(seq_count):
                value = jnp.where(row8 == 0, rew_ref[n, 0, k], jnp.where(row8 == 1, 1.0, 0.0))
                stats_own = stats_own + jnp.where(lane8 == ids_ref[n, 0, k], value, 0.0)
        stl[0] = stats_own
        for item in stat_copies("l"):
            item.start()

    def stats_second():
        for item in stat_copies("l"):
            item.wait_recv()
        total = stl[0]
        for k in range(nb - 1):
            total = total + str_[k]
        stl[1] = total
        for item in stat_copies("h"):
            item.start()

    def start_gather(v, which):
        for t in which:
            for item in x_copies(t, v):
                item.start()

    lane = lax.broadcasted_iota(jnp.int32, (tok, 128), 1)

    groups = ((0, 1), (1, steps))

    def group_of(t):
        return 0 if t == 0 else 1

    def sq_copies(v, g):
        base = 2 * v + g
        return to_tensor(
            sqs.at[v, g], lambda k: sqr.at[k, v, g], lambda k: sq_sem.at[0, base, k], lambda k: sq_sem.at[1, base, k]
        )

    def prep(v, g):
        def body(t, squares_all):
            row = xs[t, v].astype(F32)
            gd[v, pl.ds(pl.multiple_of(t * tok, tok), tok), :] = (row * gn_ref[v]).astype(BF16)
            squares = jnp.sum(row * row, axis=-1, keepdims=True)
            return jnp.where(lane == t, squares, squares_all)

        sqs[v, g] = lax.fori_loop(*groups[g], body, jnp.zeros((tok, 128), F32))
        for item in sq_copies(v, g):
            item.start()

    def finish_sq(v, g):
        for item in sq_copies(v, g):
            item.wait_recv()
        total = sqs[v, g]
        for k in range(nt - 1):
            total = total + sqr[k, v, g]
        inv_t[v, g] = 1.0 / jnp.sqrt(total * (1.0 / full) + EPS)

    def share_of(v):
        count = count_of[split_kind[v]]
        if count % nt:
            return pl.ds(0, count)
        return pl.ds(me_t * (count // nt), count // nt)

    def gs_copies(t, v):
        cols = pl.ds(t * tok, tok)
        base = v * steps + t
        mine = share_of(v)
        source = (lambda part: gs_t.at[v, part, mine, :, cols]) if v == 0 else (lambda part: gs_t.at[v, mine, part, :, cols])
        return to_dp(
            source, lambda k: gsr[v].at[k, mine, :, cols],
            lambda k: gt_s.at[base, k], lambda k: gt_r.at[base, k], gather_kind[v],
        )

    def pass_copies(t, v):
        if count_of[split_kind[v]] % nt:
            return []
        cols = pl.ds(t * tok, tok)
        base = v * steps + t
        out = []
        for k in range(count_of[gather_kind[v]] - 1):
            piece = gsr[v].at[k, share_of(v), :, cols]
            out += to_tensor(piece, lambda i: piece, lambda i: gf_s.at[base, k, i], lambda i: gf_r.at[base, k, i])
        return out

    pre_copies = {}
    back_copies = {}

    def pre_part(v, g):
        low, high = groups[g]
        rows = pl.ds(low * tok, (high - low) * tok)

        def body(j, carry):
            cols = pl.ds(pl.multiple_of(j * rtile, rtile), rtile)
            ps[v, rows, cols] = dot_nt(gd[v, rows, :], wi[v, cols, :]).astype(BF16)
            return carry

        lax.fori_loop(0, rank // rtile, body, 0)
        base = 2 * v + g
        pre_copies[v, g] = to_tensor(
            ps.at[v, rows], lambda k: pr.at[k, v, rows], lambda k: pre_sem.at[0, base, k], lambda k: pre_sem.at[1, base, k]
        )
        for item in pre_copies[v, g]:
            item.start()

    def wait_pre(v, g):
        finish_sq(v, g)
        for item in pre_copies[v, g]:
            item.wait_recv()

    def cols_of(j):
        return pl.ds(j * cc, cc)

    def rows_of(h):
        return pl.ds(h * part_tok, part_tok)

    def back_part(t, v, h=None):
        rows = pl.ds(0, tok) if h is None else rows_of(h)

        def body(j, carry):
            cols = pl.ds(pl.multiple_of(j * rtile, rtile), rtile)
            bs[v, t, rows, cols] = dot_nt(ca[v, t, rows, :], wo[v, cols, :]).astype(BF16)
            return carry

        lax.fori_loop(0, rank // rtile, body, 0)
        base = (v * steps + t) * PARTS + (h or 0)
        back_copies[t, v, h] = to_tensor(
            bs.at[v, t, rows], lambda k: br.at[k, v, t, rows],
            lambda k: back_sem.at[0, base, k], lambda k: back_sem.at[1, base, k],
        )
        for item in back_copies[t, v, h]:
            item.start()

    def finish_pre(v, which_steps):
        for t in which_steps:
            rows = pl.ds(t * tok, tok)
            total = ps[v, rows, :].astype(F32)
            for k in range(nt - 1):
                total = total + pr[k, v, rows, :].astype(F32)
            pre = inv_t[v, group_of(t), :, t:t + 1] * total
            sigma = jax.nn.sigmoid(pre)
            presum[v, rows, :] = total
            hid_t[v, :, rows] = jnp.transpose(pre * sigma).astype(BF16)
            slope[v, rows, :] = sigma * (1.0 + pre * (1.0 - sigma))

    def wait_back(t, v, h=None):
        for item in back_copies[t, v, h]:
            item.wait_recv()

    def finish_back(t, v, h, send=True):
        own = rows_of(h)
        rows = pl.ds(t * tok + h * part_tok, part_tok)
        inv = inv_t[v, group_of(t), own, t:t + 1]
        total = bs[v, t, own, :].astype(F32)
        for k in range(nt - 1):
            total = total + br[k, v, t, own, :].astype(F32)
        grad_pre = total * slope[v, rows, :]
        gs[v, rows, :] = (inv * grad_pre).astype(BF16)
        radial = jnp.sum(grad_pre * presum[v, rows, :], axis=-1, keepdims=True)
        coef = inv * inv * inv * radial * (1.0 / full)

        def part(cols):
            lifted = jnp.dot(gs[v, rows, :], wi[v, :, cols], preferred_element_type=F32)
            out = (
                ca[v, t, own, cols].astype(F32)
                + gn_ref[v, :, cols] * lifted
                - xs[t, v, own, cols].astype(F32) * coef
            ).astype(BF16)
            if t < steps - 1:
                ob[t, v, own, cols] = out
            else:
                lv[v, own, cols] = out

        def body(j, carry):
            part(pl.ds(pl.multiple_of(j * tile, tile), tile))
            return carry

        if t < steps - 1 and len(pieces(steps, t, h)) > 1:
            for c in pieces(steps, t, h):
                part(cols_of(c))
                send_on(t, v, h, c)
        else:
            lax.fori_loop(0, wid // tile, body, 0)
            if t < steps - 1 and send:
                send_on(t, v, h, None)

    halves = range(PARTS)
    slots = pipe_slots(steps, vs)

    def finish_gs(t, v):
        rows = pl.ds(t * tok, tok)
        flipped = jnp.transpose(gs[v, rows, :].astype(F32)).astype(BF16)
        gs_t[v, :, :, :, rows] = flipped.reshape(na, nb, rc, tok)
        for item in gs_copies(t, v):
            item.start()

    def pipe_copy(t, v, slot, h, c):
        where = (rows_of(h),) if c is None else (rows_of(h), cols_of(c))
        return pltpu.make_async_remote_copy(
            src_ref=ob.at[(t, v) + where], dst_ref=ca.at[(slot, t + 1) + where],
            send_sem=pipe_s.at[slots[t, v, h, c]], recv_sem=pipe_r.at[slots[t, slot, h, c]],
            device_id={"pipe": prev_p}, device_id_type=MESH,
        )

    def send_on(t, v, h, c):
        @pl.when(me_p > 0)
        def _():
            pipe_copy(t, v, v, h, c).start()

        if v == 1:
            @pl.when(me_p == 0)
            def _():
                if t == 0 and h == 0:
                    pl.semaphore_wait(wrap_sem, 1)
                pipe_copy(t, 1, 0, h, c).start()

    def sent_on(t, v, h):
        for c in pieces(steps, t, h):
            @pl.when(me_p > 0)
            def _():
                pipe_copy(t, v, v, h, c).wait_send()

            if v == 1:
                @pl.when(me_p == 0)
                def _():
                    pipe_copy(t, 1, 0, h, c).wait_send()

    def take(t, v, h, only=None):
        want = pieces(steps, t - 1, h)
        first = only is None or only == want[0]
        if only is not None:
            want = (only,)
        if v == 0:
            for c in want:
                pipe_copy(t - 1, v, v, h, c).wait_recv()
            return

        @pl.when(me_p < npipe - 1)
        def _():
            for c in want:
                pipe_copy(t - 1, v, v, h, c).wait_recv()

        if first:
            @pl.when(me_p == npipe - 1)
            def _():
                if t == 1 and h == 0:
                    for item in stat_copies("h"):
                        item.wait_recv()
                stats = stl[1]
                for k in range(na - 1):
                    stats = stats + str2[k]
                means = stats[0:1] / jnp.maximum(stats[1:2], 1.0) + stats[2:3] * (1.0 / ndp)
                tok_row = lax.broadcasted_iota(jnp.int32, (part_tok, lanes), 0) + h * part_tok
                tok_lane = lax.broadcasted_iota(jnp.int32, (part_tok, lanes), 1)
                hot = jnp.zeros((part_tok, lanes), F32)
                begin = 0
                for k in range(seq_count):
                    finish = begin + len_ref[t - 1, 0, k]
                    inside = (tok_row >= begin) & (tok_row < finish)
                    value = jnp.where(tok_lane == ids_ref[t - 1, 0, k], 1.0, 0.0)
                    value = value - jnp.where(tok_lane == unit_lane, rew_ref[t - 1, 0, k], 0.0)
                    hot = hot + jnp.where(inside, value, 0.0)
                    begin = finish
                weight = jnp.sum(hot * means, axis=-1, keepdims=True)
                ca[1, t, rows_of(h), :] = (weight * lp[t - 1, rows_of(h), :].astype(F32)).astype(BF16)

    jobs = reductions()

    def axes_of(job):
        what, v, j = job
        first = FIRST_AXIS[v][j] if what == "out" else IN_AXIS[v]
        return ("l", "h") if first == "l" else ("h", "l")

    def split_copies(job):
        e = jobs[job]
        first, second = axes_of(job)
        count = count_of[second]
        source = (lambda part: gb.at[e, :, part]) if first == "l" else (lambda part: gb.at[e, part])
        return to_dp(
            source, lambda k: r1.at[e, k, pl.ds(0, count)], lambda k: r1_s.at[e, k], lambda k: r1_r.at[e, k], first
        )

    def join_copies(job):
        e = jobs[job]
        return to_dp(
            lambda part: p2.at[e, part], lambda k: r2.at[e, k], lambda k: r2_s.at[e, k], lambda k: r2_r.at[e, k],
            axes_of(job)[1],
        )

    def product(job):
        what, v, j = job
        e = jobs[job]
        if what == "out":
            value = jnp.dot(
                hid_t[v], ca[v, :, :, cols_of(j)].reshape(steps * tok, cc), preferred_element_type=F32
            )
        else:
            value = jnp.dot(
                gs_t[v].reshape(rank, steps * tok), xs[:, v, :, cols_of(j)].reshape(steps * tok, cc),
                preferred_element_type=F32,
            ) * gn_ref[v, :, cols_of(j)]
        gb[e] = value.astype(BF16).reshape(na, nb, rc, cc)
        for item in split_copies(job):
            item.start()

    def middle(job):
        e = jobs[job]
        first, second = axes_of(job)
        count = count_of[second]
        for item in split_copies(job):
            item.wait_recv()
        own = gb[e, :, me_l] if first == "l" else gb[e, me_h]
        total = own.astype(F32)
        for k in range(count_of[first] - 1):
            total = total + r1[e, k, :count].astype(F32)
        p2[e, :count] = total.astype(BF16)
        for item in join_copies(job):
            item.start()

    scale = 1.0 / (ndp * tok)

    def final(job):
        what, v, j = job
        e = jobs[job]
        kind = axes_of(job)[1]
        for item in join_copies(job):
            item.wait_recv()
        total = p2[e, me_h if kind == "h" else me_l].astype(F32)
        for k in range(count_of[kind] - 1):
            total = total + r2[e, k].astype(F32)
        dest = fo if what == "out" else fi
        dest[v, :, cols_of(j)] = total * scale

    def in_copies(v, j):
        base = v * CHUNKS + j
        return to_dp(
            lambda part: p2i.at[v, j, part], lambda k: r2i.at[v, j, k],
            lambda k: ri_s.at[base, k], lambda k: ri_r.at[base, k], split_kind[v],
        )

    def wait_gathered(v):
        for t in range(steps):
            for item in gs_copies(t, v):
                item.wait_recv()
            for item in pass_copies(t, v):
                item.start()
        for t in range(steps):
            for item in x_copies(t, v) + pass_copies(t, v):
                item.wait_recv()

    def grad_in(v, which):
        width = count_of[split_kind[v]]
        own = gs_t[v, me_h] if v == 0 else gs_t[v, :, me_l]
        own = own.reshape(width * rc, steps * tok)
        for j in which:
            value = jnp.dot(
                own, xs[:, v, :, cols_of(j)].reshape(steps * tok, cc), preferred_element_type=F32
            )
            for k in range(count_of[gather_kind[v]] - 1):
                left = gsr[v][k].reshape(width * rc, steps * tok)
                value = value + jnp.dot(
                    left, xr[v][k, :, :, cols_of(j)].reshape(steps * tok, cc), preferred_element_type=F32
                )
            value = value * gn_ref[v, :, cols_of(j)]
            p2i[v, j, :width] = value.astype(BF16).reshape(width, rc, cc)
            for item in in_copies(v, j):
                item.start()

    def final_in(v, j):
        for item in in_copies(v, j):
            item.wait_recv()
        along_h = split_kind[v] == "h"
        total = p2i[v, j, me_h if along_h else me_l].astype(F32)
        for k in range(count_of[split_kind[v]] - 1):
            total = total + r2i[v, j, k].astype(F32)
        fi[v, :, cols_of(j)] = total * scale

    last = steps - 1

    def back(t, v, h, during=None):
        with scope(f"back_{t}{v}{h}"):
            back_part(t, v, h)
            if during is not None:
                during()
            wait_back(t, v, h)
        with scope(f"fin_{t}{v}{h}"):
            finish_back(t, v, h)

    def step(t, v, h, during=None):
        with scope(f"take_{t}{v}{h}"):
            take(t, v, h)
        back(t, v, h, during)

    def products(v, which):
        for j in which:
            with scope(f"prod_{v}{j}"):
                take(last, v, PARTS - 1, j)
                product(("out", v, j))

    def rest(what, v):
        return range(GATHERED[v], CHUNKS) if what == "in" else range(GATHERED[v])

    with scope("stats"):
        for item in small:
            item.wait()
        start_gather(0, [0])
        stats_first()
        start_gather(1, range(steps))
    with scope("ld01"):
        loads[0].wait()
        loads[1].wait()
    with scope("first1"):
        back_part(0, 1)
        loads[2].wait()
        prep(1, 0)
        loads[3].wait()
        pre_part(1, 0)
        prep(1, 1)
        loads[4].wait()
        prep(0, 0)
    with scope("wpre1"):
        wait_pre(1, 0)
    with scope("fin1"):
        finish_pre(1, [0])
        wait_back(0, 1)
        for h in halves:
            finish_back(0, 1, h)
    with scope("first0"):
        finish_gs(0, 1)
        stats_second()
        start_gather(0, range(1, steps))
        pre_part(1, 1)
        prep(0, 1)
        loads[5].wait()
        loads[6].wait()
        back_part(0, 0)
        loads[7].wait()
        pre_part(0, 0)
        pre_part(0, 1)
        wait_pre(1, 1)
        finish_pre(1, range(1, steps))
    with scope("wpre0"):
        wait_pre(0, 0)
    with scope("fin0"):
        finish_pre(0, [0])
        wait_back(0, 0)
        for h in halves:
            finish_back(0, 0, h, send=False)
        finish_gs(0, 0)
        wait_pre(0, 1)
        finish_pre(0, range(1, steps))
        loads[8].wait()

    for t in range(1, last):
        for h in halves:
            step(t, 1, h)
        if t == 1:
            for h in halves:
                send_on(0, 0, h, None)
        finish_gs(t, 1)
    for h in halves[:-1]:
        step(last, 1, h)
    products(1, ORDER[1][:2])
    for j in ORDER[1][2:]:
        take(last, 1, PARTS - 1, j)
    back(last, 1, PARTS - 1)
    with scope("gout1"):
        finish_gs(last, 1)
        for j in ORDER[1][2:]:
            product(("out", 1, j))
        for j in rest("in", 1):
            product(("in", 1, j))

    def first_middles():
        middle(("out", 1, 0))

    for t in range(1, last):
        for h in halves:
            ending = t == last - 1
            step(t, 0, h, first_middles if ending and h == 0 else None)
            if ending and h == 0:
                with scope("wgat1"):
                    wait_gathered(1)
                with scope("gin1"):
                    grad_in(1, rest("out", 1)[:1])
        finish_gs(t, 0)
    with scope("mid11"):
        middle(("out", 1, 1))
        middle(("out", 1, 3))
    for h in halves[:-1]:
        step(last, 0, h)
    with scope("mid12"):
        middle(("out", 1, 2))
    products(0, ORDER[0][:2])
    for j in ORDER[0][2:]:
        take(last, 0, PARTS - 1, j)
    back(last, 0, PARTS - 1)
    with scope("gout0"):
        finish_gs(last, 0)
        for j in ORDER[0][2:]:
            product(("out", 0, j))
        for j in rest("in", 0):
            product(("in", 0, j))
    with scope("gin1b"):
        grad_in(1, rest("out", 1)[1:])
    with scope("midi1"):
        for j in rest("in", 1):
            middle(("in", 1, j))
    with scope("mid0_0"):
        middle(("out", 0, 0))
    with scope("wgat0"):
        wait_gathered(0)
    with scope("gin0"):
        grad_in(0, rest("out", 0))
    with scope("mid0_3"):
        middle(("out", 0, 3))
    with scope("final1a"):
        for j in (0, 1, 3):
            final(("out", 1, j))
        for j in rest("out", 1)[:1]:
            final_in(1, j)

    @pl.when(me_p < npipe - 1)
    def _():
        for item in stat_copies("h"):
            item.wait_recv()

    with scope("drain"):
        for item in stat_copies("l") + stat_copies("h") + sum([sq_copies(v, g) for v in range(vs) for g in range(2)], []):
            item.wait_send()
        for items in back_copies.values():
            for item in items:
                item.wait_send()
        for v in range(vs):
            for g in range(2):
                for item in pre_copies[v, g]:
                    item.wait_send()
            for t in range(steps):
                for item in x_copies(t, v) + gs_copies(t, v) + pass_copies(t, v):
                    item.wait_send()
                if t < steps - 1:
                    for h in halves:
                        sent_on(t, v, h)
    for j in (1, 2):
        with scope(f"mid0_{j}"):
            middle(("out", 0, j))
    with scope("midi0"):
        for j in rest("in", 0):
            middle(("in", 0, j))
    with scope("final0i"):
        for j in rest("out", 0):
            final_in(0, j)
    with scope("final1b"):
        for j in rest("out", 1)[1:]:
            final_in(1, j)
        for j in rest("in", 1):
            final(("in", 1, j))
        final(("out", 1, 2))
    for v in range(vs):
        for j in range(GATHERED[v]):
            for item in in_copies(v, j):
                item.wait_send()
    for job in jobs:
        for item in split_copies(job):
            item.wait_send()
    for j in (0, 1, 3, 2):
        with scope(f"fin0_{j}"):
            final(("out", 0, j))
    with scope("fini0"):
        for j in rest("in", 0):
            final(("in", 0, j))
    with scope("tail"):
        for job in jobs:
            for item in join_copies(job):
                item.wait_send()


def store(a, b, c, a_out, b_out, c_out, sem):
    copies = [pltpu.make_async_copy(*pair, sem.at[k]) for k, pair in enumerate(((a, a_out), (b, b_out), (c, c_out)))]
    for item in copies:
        item.start()
    for item in copies:
        item.wait()


def shards(
    saved_inputs, proj_in, proj_out, norm_gain, arriving, logp_grad, rewards, seq_lengths, group_ids
):
    nt = lax.axis_size("tensor")
    npipe = lax.axis_size("pipe")
    ndp = lax.axis_size("dp")
    steps, vs, _, tok, wid = saved_inputs.shape
    rank = proj_in.shape[2]
    new_count = logp_grad.shape[0]
    group_count = new_count * ndp * rewards.shape[2] // 8
    lanes = -(-(group_count + 1) // 128) * 128
    na, nb = factors(ndp)
    rc = rank // ndp
    cc = wid // CHUNKS
    jobs = len(reductions())
    pipe_count = len(pipe_slots(steps, vs))
    hm, lm = max(na - 1, 1), max(nb - 1, 1)
    dims = (steps, vs, tok, wid, rank, nt, npipe, ndp)
    peers = max(nt - 1, 1)
    any_spec = pl.BlockSpec(memory_space=pl.ANY)
    vmem = pl.BlockSpec(memory_space=pltpu.VMEM)
    V = pltpu.VMEM
    DMA = pltpu.SemaphoreType.DMA
    pmax = max(na, nb)
    less = max(pmax - 1, 1)
    scratch = [
        V((steps, vs, tok, wid), BF16),
        V((vs, steps * tok, wid), BF16),
        V((vs, steps, tok, wid), BF16),
        V((vs, rank, wid), BF16),
        V((vs, rank, wid), BF16),
        V((new_count, tok, wid), BF16),
        V((vs, steps * tok, rank), BF16),
        V((peers, vs, steps * tok, rank), BF16),
        V((vs, steps * tok, rank), F32),
        V((vs, steps * tok, rank), F32),
        V((vs, rank, steps * tok), BF16),
        V((vs, steps * tok, rank), BF16),
        V((vs, na, nb, rc, steps * tok), BF16),
        V((hm, nb, rc, steps * tok), BF16),
        V((lm, na, rc, steps * tok), BF16),
        V((hm, steps, tok, GATHERED[0] * cc), BF16),
        V((lm, steps, tok, GATHERED[1] * cc), BF16),
        V((vs, steps, tok, rank), BF16),
        V((peers, vs, steps, tok, rank), BF16),
        V((steps - 1, vs, tok, wid), BF16),
        V((vs, 2, tok, 128), F32),
        V((peers, vs, 2, tok, 128), F32),
        V((vs, 2, tok, 128), F32),
        V((2, 8, lanes), F32),
        V((lm, 8, lanes), F32),
        V((jobs, na, nb, rc, cc), BF16),
        V((jobs, less, pmax, rc, cc), BF16),
        V((jobs, pmax, rc, cc), BF16),
        V((jobs, less, rc, cc), BF16),
        V((vs, CHUNKS, pmax, rc, cc), BF16),
        V((vs, CHUNKS, less, rc, cc), BF16),
        V(norm_gain.shape, F32),
        pltpu.SMEM(rewards.shape, F32),
        pltpu.SMEM(seq_lengths.shape, jnp.int32),
        pltpu.SMEM(group_ids.shape, jnp.int32),
        V((hm, 8, lanes), F32),
        pltpu.SemaphoreType.REGULAR,
        DMA((13,)),
        DMA((2, 2 * vs, peers)),
        DMA((4, less)),
        DMA((2, 2 * vs, peers)),
        DMA((2, vs * steps * PARTS, peers)),
        DMA((pipe_count,)),
        DMA((pipe_count,)),
        DMA((vs * steps, less)),
        DMA((vs * steps, less)),
        DMA((vs * steps, less)),
        DMA((vs * steps, less)),
        DMA((vs * steps, less, peers)),
        DMA((vs * steps, less, peers)),
        DMA((jobs, less)),
        DMA((jobs, less)),
        DMA((jobs, less)),
        DMA((jobs, less)),
        DMA((vs * CHUNKS, less)),
        DMA((vs * CHUNKS, less)),
    ]
    grad_in, grad_out, leaving = pl.pallas_call(
        functools.partial(kernel, dims),
        out_shape=(
            V((vs, rc, wid), F32),
            V((vs, rc, wid), F32),
            V((vs, tok, wid), BF16),
        ),
        in_specs=[any_spec] * 9,
        out_specs=(vmem, vmem, vmem),
        scratch_shapes=scratch,
        compiler_params=pltpu.CompilerParams(
            collective_id=0, has_side_effects=True, vmem_limit_bytes=58 * 1024 * 1024
        ),
    )(
        saved_inputs[:, :, 0], proj_in[:, 0], proj_out[:, 0], norm_gain, arriving[:, 0], logp_grad,
        rewards, seq_lengths, group_ids,
    )
    grad_in, grad_out, leaving = pl.pallas_call(
        store,
        out_shape=tuple(jax.ShapeDtypeStruct(a.shape, a.dtype) for a in (grad_in, grad_out, leaving)),
        in_specs=[vmem] * 3,
        out_specs=[any_spec] * 3,
        scratch_shapes=[DMA((3,))],
        compiler_params=pltpu.CompilerParams(vmem_limit_bytes=1024 * 1024),
    )(grad_in, grad_out, leaving)
    return grad_in[:, None], grad_out[:, None], leaving[:, None]


def solution(mesh):
    return jax.shard_map(
        shards,
        mesh=mesh,
        in_specs=(
            P(None, None, "pipe", "dp", "tensor"),
            P(None, "pipe", None, "tensor"),
            P(None, "pipe", None, "tensor"),
            P(None, "pipe", "tensor"),
            P(None, "pipe", "dp", "tensor"),
            P(None, "dp", "tensor"),
            P(None, "dp", None),
            P(None, "dp", None),
            P(None, "dp", None),
        ),
        out_specs=(
            P(None, "pipe", "dp", "tensor"),
            P(None, "pipe", "dp", "tensor"),
            P(None, "pipe", "dp", "tensor"),
        ),
        check_vma=False,
    )
```

```python
import functools

import jax
import jax.numpy as jnp
from jax import lax
from jax.experimental import pallas as pl
from jax.experimental.pallas import tpu as pltpu
from jax.sharding import PartitionSpec as P

EPS = 1e-05
MESH = pl.DeviceIdType.MESH
F32 = jnp.float32
BF16 = jnp.bfloat16


def dot_nt(a, b):
    return lax.dot_general(a, b, (((1,), (1,)), ((), ())), preferred_element_type=F32)


def factors(n):
    low = 1
    for k in range(1, n + 1):
        if n % k == 0 and k * k <= n:
            low = k
    return low, n // low


CHUNKS = 4
GATHERED = (3, 3)
PARTS = 2
FIRST_AXIS = ("hhll", "hllh")
IN_AXIS = ("h", "l")
ORDER = (3, 2, 0, 1)
scope = jax.named_scope


def reductions():
    jobs = [("out", v, j) for v in (1, 0) for j in range(CHUNKS)]
    jobs += [("in", v, j) for v in (1, 0) for j in range(GATHERED[v], CHUNKS)]
    return {job: e for e, job in enumerate(jobs)}


def pieces(steps, t, h):
    return ORDER if (t, h) in ((0, 0), (steps - 2, PARTS - 1)) else (None,)


def pipe_slots(steps, vs):
    keys = [(t, v, h, c) for t in range(steps - 1) for v in range(vs) for h in range(PARTS) for c in pieces(steps, t, h)]
    return {key: k for k, key in enumerate(keys)}


def kernel(
    dims,
    x_hbm, wi_hbm, wo_hbm, gn_hbm, ar_hbm, lp_hbm, rew_hbm, len_hbm, ids_hbm,
    fi, fo, lv,
    xs, gd, ca, wi, wo, lp, ps, pr, presum, slope, hid_t, gs, gs_t, gsr0, gsr1, xr0, xr1, bs, br, ob,
    sqs, sqr, inv_t, stl, str_, gb, r1, p2, r2, p2i, r2i,
    gn_ref, rew_ref, len_ref, ids_ref, str2, wrap_sem,
    in_sem, sq_s, sq_r, st_sem, pre_s, pre_r, back_s, back_r, pipe_s, pipe_r, xg_s, xg_r, gt_s, gt_r, gf_s, gf_r,
    r1_s, r1_r, r2_s, r2_r, ri_s, ri_r,
):
    steps, vs, tok, wid, rank, nt, npipe, ndp = dims
    na, nb = factors(ndp)
    rc = rank // ndp
    full = wid * nt
    tile = min(512, wid // 2)
    rtile = min(512, rank)
    cc = wid // CHUNKS
    part_tok = tok // PARTS
    lanes = stl.shape[2]
    new_count, _, seq_count = rew_ref.shape
    unit_lane = new_count * ndp * seq_count // 8
    me_t = lax.axis_index("tensor")
    me_p = lax.axis_index("pipe")
    me_d = lax.axis_index("dp")
    me_h = me_d // nb
    me_l = me_d % nb
    prev_p = lax.rem(me_p + npipe - 1, npipe)
    next_p = lax.rem(me_p + 1, npipe)

    def load(src, dst, k):
        return pltpu.make_async_copy(src, dst, in_sem.at[k])

    loads = [
        load(ar_hbm.at[1], ca.at[1, 0], 0),
        load(wo_hbm.at[1], wo.at[1], 1),
        load(x_hbm.at[:, 1], xs.at[:, 1], 2),
        load(wi_hbm.at[1], wi.at[1], 3),
        load(x_hbm.at[:, 0], xs.at[:, 0], 4),
        load(ar_hbm.at[0], ca.at[0, 0], 5),
        load(wo_hbm.at[0], wo.at[0], 6),
        load(wi_hbm.at[0], wi.at[0], 7),
        load(lp_hbm, lp, 8),
    ]
    small = [
        load(gn_hbm, gn_ref, 9),
        load(rew_hbm, rew_ref, 10),
        load(len_hbm, len_ref, 11),
        load(ids_hbm, ids_ref, 12),
    ]

    barrier = pltpu.get_barrier_semaphore()
    for k in range(1, nt):
        pl.semaphore_signal(barrier, inc=1, device_id={"tensor": lax.rem(me_t + k, nt)}, device_id_type=MESH)
    for k in range(1, na):
        peer = lax.rem(me_h + k, na) * nb + me_l
        pl.semaphore_signal(barrier, inc=1, device_id={"dp": peer}, device_id_type=MESH)
    for k in range(1, nb):
        peer = me_h * nb + lax.rem(me_l + k, nb)
        pl.semaphore_signal(barrier, inc=1, device_id={"dp": peer}, device_id_type=MESH)

    @pl.when(me_p < npipe - 1)
    def _():
        pl.semaphore_signal(barrier, inc=1, device_id={"pipe": next_p}, device_id_type=MESH)

    @pl.when(me_p == 0)
    def _():
        pl.semaphore_signal(barrier, inc=1, device_id={"pipe": prev_p}, device_id_type=MESH)


    for item in small + loads:
        item.start()

    with scope("barrier"):
        along_pipe = jnp.where(me_p == 0, 0, jnp.where(me_p == npipe - 1, 2, 1))
        pl.semaphore_wait(barrier, nt - 1 + na - 1 + nb - 1 + along_pipe)

    @pl.when(me_p == npipe - 1)
    def _():
        pl.semaphore_signal(wrap_sem, inc=1, device_id={"pipe": next_p}, device_id_type=MESH)

    def to_tensor(src, dst_of, send_of, recv_of):
        return [
            pltpu.make_async_remote_copy(
                src_ref=src, dst_ref=dst_of(k - 1), send_sem=send_of(k - 1), recv_sem=recv_of(k - 1),
                device_id={"tensor": lax.rem(me_t + k, nt)}, device_id_type=MESH,
            )
            for k in range(1, nt)
        ]

    def to_dp(src_of, dst_of, send_of, recv_of, kind):
        out = []
        count = {"h": na, "l": nb}[kind]
        for k in range(1, count):
            if kind == "h":
                part = lax.rem(me_h + k, na)
                who = part * nb + me_l
            else:
                part = lax.rem(me_l + k, nb)
                who = me_h * nb + part
            out.append(
                pltpu.make_async_remote_copy(
                    src_ref=src_of(part), dst_ref=dst_of(k - 1), send_sem=send_of(k - 1), recv_sem=recv_of(k - 1),
                    device_id={"dp": who}, device_id_type=MESH,
                )
            )
        return out

    gather_kind = ("h", "l")
    split_kind = ("l", "h")
    count_of = {"h": na, "l": nb}
    xr = (xr0, xr1)
    gsr = (gsr0, gsr1)

    def x_copies(t, v):
        cols = pl.ds(0, GATHERED[v] * cc)
        return to_dp(
            lambda part: x_hbm.at[t, v, :, cols], lambda k: xr[v].at[k, t],
            lambda k: xg_s.at[v], lambda k: xg_r.at[v], gather_kind[v],
        )


    def stat_copies(kind):
        if kind == "l":
            return to_dp(lambda part: stl.at[0], lambda k: str_.at[k], lambda k: st_sem.at[0, k], lambda k: st_sem.at[1, k], kind)
        return to_dp(lambda part: stl.at[1], lambda k: str2.at[k], lambda k: st_sem.at[2, k], lambda k: st_sem.at[3, k], kind)

    def stats_first():
        lane8 = lax.broadcasted_iota(jnp.int32, (8, lanes), 1)
        row8 = lax.broadcasted_iota(jnp.int32, (8, lanes), 0)
        stats_own = jnp.where((row8 == 2) & (lane8 == unit_lane), 1.0, 0.0)
        for n in range(new_count):
            for k in range(seq_count):
                value = jnp.where(row8 == 0, rew_ref[n, 0, k], jnp.where(row8 == 1, 1.0, 0.0))
                stats_own = stats_own + jnp.where(lane8 == ids_ref[n, 0, k], value, 0.0)
        stl[0] = stats_own
        for item in stat_copies("l"):
            item.start()

    def stats_second():
        for item in stat_copies("l"):
            item.wait_recv()
        total = stl[0]
        for k in range(nb - 1):
            total = total + str_[k]
        stl[1] = total
        for item in stat_copies("h"):
            item.start()

    def start_gather(v, which):
        for t in which:
            for item in x_copies(t, v):
                item.start()

    lane = lax.broadcasted_iota(jnp.int32, (tok, 128), 1)

    groups = ((0, 1), (1, steps))

    def group_of(t):
        return 0 if t == 0 else 1

    def sq_copies(v, g):
        base = 2 * v + g
        return to_tensor(
            sqs.at[v, g], lambda k: sqr.at[k, v, g], lambda k: sq_s, lambda k: sq_r.at[base, k]
        )

    def prep(v, g):
        def body(t, squares_all):
            row = xs[t, v].astype(F32)
            gd[v, pl.ds(pl.multiple_of(t * tok, tok), tok), :] = (row * gn_ref[v]).astype(BF16)
            squares = jnp.sum(row * row, axis=-1, keepdims=True)
            return jnp.where(lane == t, squares, squares_all)

        sqs[v, g] = lax.fori_loop(*groups[g], body, jnp.zeros((tok, 128), F32))
        for item in sq_copies(v, g):
            item.start()

    def finish_sq(v, g):
        for item in sq_copies(v, g):
            item.wait_recv()
        total = sqs[v, g]
        for k in range(nt - 1):
            total = total + sqr[k, v, g]
        inv_t[v, g] = 1.0 / jnp.sqrt(total * (1.0 / full) + EPS)

    def share_of(v):
        count = count_of[split_kind[v]]
        if count % nt:
            return pl.ds(0, count)
        return pl.ds(me_t * (count // nt), count // nt)

    def gs_copies(t, v):
        cols = pl.ds(t * tok, tok)
        mine = share_of(v)
        source = (lambda part: gs_t.at[v, part, mine, :, cols]) if v == 0 else (lambda part: gs_t.at[v, mine, part, :, cols])
        return to_dp(
            source, lambda k: gsr[v].at[k, mine, :, cols],
            lambda k: gt_s.at[v], lambda k: gt_r.at[v], gather_kind[v],
        )

    def pass_copies(v):
        if count_of[split_kind[v]] % nt:
            return []
        out = []
        for k in range(count_of[gather_kind[v]] - 1):
            piece = gsr[v].at[k, share_of(v)]
            out += to_tensor(piece, lambda i: piece, lambda i: gf_s.at[v, k, i], lambda i: gf_r.at[v, k, i])
        return out

    def take_bytes(ref, sem):
        pltpu.make_async_copy(ref, ref, sem).wait()

    pre_copies = {}
    back_copies = {}

    def pre_part(v, g):
        low, high = groups[g]
        rows = pl.ds(low * tok, (high - low) * tok)

        def body(j, carry):
            cols = pl.ds(pl.multiple_of(j * rtile, rtile), rtile)
            ps[v, rows, cols] = dot_nt(gd[v, rows, :], wi[v, cols, :]).astype(BF16)
            return carry

        lax.fori_loop(0, rank // rtile, body, 0)
        base = 2 * v + g
        pre_copies[v, g] = to_tensor(
            ps.at[v, rows], lambda k: pr.at[k, v, rows], lambda k: pre_s, lambda k: pre_r.at[base, k]
        )
        for item in pre_copies[v, g]:
            item.start()

    def wait_pre(v, g):
        finish_sq(v, g)
        for item in pre_copies[v, g]:
            item.wait_recv()

    def cols_of(j):
        return pl.ds(j * cc, cc)

    def rows_of(h):
        return pl.ds(h * part_tok, part_tok)

    def back_part(t, v, h=None):
        rows = pl.ds(0, tok) if h is None else rows_of(h)

        def body(j, carry):
            cols = pl.ds(pl.multiple_of(j * rtile, rtile), rtile)
            bs[v, t, rows, cols] = dot_nt(ca[v, t, rows, :], wo[v, cols, :]).astype(BF16)
            return carry

        lax.fori_loop(0, rank // rtile, body, 0)
        base = v * (1 + (steps - 1) * PARTS) + (0 if h is None else 1 + (t - 1) * PARTS + h)
        back_copies[t, v, h] = to_tensor(
            bs.at[v, t, rows], lambda k: br.at[k, v, t, rows],
            lambda k: back_s, lambda k: back_r.at[base, k],
        )
        for item in back_copies[t, v, h]:
            item.start()

    def finish_pre(v, which_steps):
        for t in which_steps:
            rows = pl.ds(t * tok, tok)
            total = ps[v, rows, :].astype(F32)
            for k in range(nt - 1):
                total = total + pr[k, v, rows, :].astype(F32)
            pre = inv_t[v, group_of(t), :, t:t + 1] * total
            sigma = jax.nn.sigmoid(pre)
            presum[v, rows, :] = total
            hid_t[v, :, rows] = jnp.transpose(pre * sigma).astype(BF16)
            slope[v, rows, :] = sigma * (1.0 + pre * (1.0 - sigma))

    def wait_back(t, v, h=None):
        for item in back_copies[t, v, h]:
            item.wait_recv()

    def finish_back(t, v, h, send=True):
        own = rows_of(h)
        rows = pl.ds(t * tok + h * part_tok, part_tok)
        inv = inv_t[v, group_of(t), own, t:t + 1]
        total = bs[v, t, own, :].astype(F32)
        for k in range(nt - 1):
            total = total + br[k, v, t, own, :].astype(F32)
        grad_pre = total * slope[v, rows, :]
        gs[v, rows, :] = (inv * grad_pre).astype(BF16)
        radial = jnp.sum(grad_pre * presum[v, rows, :], axis=-1, keepdims=True)
        coef = inv * inv * inv * radial * (1.0 / full)

        def part(cols):
            lifted = jnp.dot(gs[v, rows, :], wi[v, :, cols], preferred_element_type=F32)
            out = (
                ca[v, t, own, cols].astype(F32)
                + gn_ref[v, :, cols] * lifted
                - xs[t, v, own, cols].astype(F32) * coef
            ).astype(BF16)
            if t < steps - 1:
                ob[t, v, own, cols] = out
            else:
                lv[v, own, cols] = out

        def body(j, carry):
            part(pl.ds(pl.multiple_of(j * tile, tile), tile))
            return carry

        if t < steps - 1 and len(pieces(steps, t, h)) > 1:
            for c in pieces(steps, t, h):
                part(cols_of(c))
                if send:
                    send_on(t, v, h, c)
        else:
            lax.fori_loop(0, wid // tile, body, 0)
            if t < steps - 1 and send:
                send_on(t, v, h, None)

    halves = range(PARTS)
    slots = pipe_slots(steps, vs)

    def finish_gs(t, v):
        rows = pl.ds(t * tok, tok)
        flipped = jnp.transpose(gs[v, rows, :].astype(F32)).astype(BF16)
        gs_t[v, :, :, :, rows] = flipped.reshape(na, nb, rc, tok)
        for item in gs_copies(t, v):
            item.start()

    def pipe_copy(t, v, slot, h, c):
        where = (rows_of(h),) if c is None else (rows_of(h), cols_of(c))
        return pltpu.make_async_remote_copy(
            src_ref=ob.at[(t, v) + where], dst_ref=ca.at[(slot, t + 1) + where],
            send_sem=pipe_s, recv_sem=pipe_r.at[slots[t, slot, h, c]],
            device_id={"pipe": prev_p}, device_id_type=MESH,
        )

    def send_on(t, v, h, c):
        @pl.when(me_p > 0)
        def _():
            pipe_copy(t, v, v, h, c).start()

        if v == 1:
            @pl.when(me_p == 0)
            def _():
                if t == 0 and h == 0 and c == pieces(steps, t, h)[0]:
                    pl.semaphore_wait(wrap_sem, 1)
                pipe_copy(t, 1, 0, h, c).start()

    def take(t, v, h, only=None):
        want = pieces(steps, t - 1, h)
        first = only is None or only == want[0]
        if only is not None:
            want = (only,)
        if v == 0:
            for c in want:
                pipe_copy(t - 1, v, v, h, c).wait_recv()
            return

        @pl.when(me_p < npipe - 1)
        def _():
            for c in want:
                pipe_copy(t - 1, v, v, h, c).wait_recv()

        if first:
            @pl.when(me_p == npipe - 1)
            def _():
                if t == 1 and h == 0:
                    for item in stat_copies("h"):
                        item.wait_recv()
                stats = stl[1]
                for k in range(na - 1):
                    stats = stats + str2[k]
                means = stats[0:1] / jnp.maximum(stats[1:2], 1.0) + stats[2:3] * (1.0 / ndp)
                tok_row = lax.broadcasted_iota(jnp.int32, (part_tok, lanes), 0) + h * part_tok
                tok_lane = lax.broadcasted_iota(jnp.int32, (part_tok, lanes), 1)
                hot = jnp.zeros((part_tok, lanes), F32)
                begin = 0
                for k in range(seq_count):
                    finish = begin + len_ref[t - 1, 0, k]
                    inside = (tok_row >= begin) & (tok_row < finish)
                    value = jnp.where(tok_lane == ids_ref[t - 1, 0, k], 1.0, 0.0)
                    value = value - jnp.where(tok_lane == unit_lane, rew_ref[t - 1, 0, k], 0.0)
                    hot = hot + jnp.where(inside, value, 0.0)
                    begin = finish
                weight = jnp.sum(hot * means, axis=-1, keepdims=True)
                ca[1, t, rows_of(h), :] = (weight * lp[t - 1, rows_of(h), :].astype(F32)).astype(BF16)

    jobs = reductions()

    def axes_of(job):
        what, v, j = job
        first = FIRST_AXIS[v][j] if what == "out" else IN_AXIS[v]
        return ("l", "h") if first == "l" else ("h", "l")

    def split_copies(job):
        e = jobs[job]
        first, second = axes_of(job)
        count = count_of[second]
        source = (lambda part: gb.at[e, :, part]) if first == "l" else (lambda part: gb.at[e, part])
        return to_dp(
            source, lambda k: r1.at[e, k, pl.ds(0, count)], lambda k: r1_s, lambda k: r1_r.at[e, k], first
        )

    def join_copies(job):
        e = jobs[job]
        return to_dp(
            lambda part: p2.at[e, part], lambda k: r2.at[e, k], lambda k: r2_s, lambda k: r2_r.at[e, k],
            axes_of(job)[1],
        )

    def product(job):
        what, v, j = job
        e = jobs[job]
        if what == "out":
            value = jnp.dot(
                hid_t[v], ca[v, :, :, cols_of(j)].reshape(steps * tok, cc), preferred_element_type=F32
            )
        else:
            value = jnp.dot(
                gs_t[v].reshape(rank, steps * tok), xs[:, v, :, cols_of(j)].reshape(steps * tok, cc),
                preferred_element_type=F32,
            ) * gn_ref[v, :, cols_of(j)]
        gb[e] = value.astype(BF16).reshape(na, nb, rc, cc)
        for item in split_copies(job):
            item.start()

    def middle(job):
        e = jobs[job]
        first, second = axes_of(job)
        count = count_of[second]
        for item in split_copies(job):
            item.wait_recv()
        own = gb[e, :, me_l] if first == "l" else gb[e, me_h]
        total = own.astype(F32)
        for k in range(count_of[first] - 1):
            total = total + r1[e, k, :count].astype(F32)
        p2[e, :count] = total.astype(BF16)
        for item in join_copies(job):
            item.start()

    scale = 1.0 / (ndp * tok)

    def final(job):
        what, v, j = job
        e = jobs[job]
        kind = axes_of(job)[1]
        for item in join_copies(job):
            item.wait_recv()
        total = p2[e, me_h if kind == "h" else me_l].astype(F32)
        for k in range(count_of[kind] - 1):
            total = total + r2[e, k].astype(F32)
        dest = fo if what == "out" else fi
        dest[v, :, cols_of(j)] = total * scale

    def in_copies(v, j):
        base = v * CHUNKS + j
        return to_dp(
            lambda part: p2i.at[v, j, part], lambda k: r2i.at[v, j, k],
            lambda k: ri_s.at[v], lambda k: ri_r.at[base, k], split_kind[v],
        )

    def wait_gathered(v):
        take_bytes(gsr[v].at[:, share_of(v)], gt_r.at[v])
        for item in pass_copies(v):
            item.start()
        take_bytes(xr[v], xg_r.at[v])
        for item in pass_copies(v):
            item.wait_recv()

    def grad_in(v, which):
        width = count_of[split_kind[v]]
        own = gs_t[v, me_h] if v == 0 else gs_t[v, :, me_l]
        own = own.reshape(width * rc, steps * tok)
        for j in which:
            value = jnp.dot(
                own, xs[:, v, :, cols_of(j)].reshape(steps * tok, cc), preferred_element_type=F32
            )
            for k in range(count_of[gather_kind[v]] - 1):
                left = gsr[v][k].reshape(width * rc, steps * tok)
                value = value + jnp.dot(
                    left, xr[v][k, :, :, cols_of(j)].reshape(steps * tok, cc), preferred_element_type=F32
                )
            value = value * gn_ref[v, :, cols_of(j)]
            p2i[v, j, :width] = value.astype(BF16).reshape(width, rc, cc)
            for item in in_copies(v, j):
                item.start()

    def final_in(v, j):
        for item in in_copies(v, j):
            item.wait_recv()
        along_h = split_kind[v] == "h"
        total = p2i[v, j, me_h if along_h else me_l].astype(F32)
        for k in range(count_of[split_kind[v]] - 1):
            total = total + r2i[v, j, k].astype(F32)
        fi[v, :, cols_of(j)] = total * scale

    last = steps - 1

    def back(t, v, h, during=None):
        with scope(f"back_{t}{v}{h}"):
            back_part(t, v, h)
            if during is not None:
                during()
            wait_back(t, v, h)
        with scope(f"fin_{t}{v}{h}"):
            finish_back(t, v, h)

    def step(t, v, h, during=None):
        with scope(f"take_{t}{v}{h}"):
            take(t, v, h)
        back(t, v, h, during)

    def products(v, which):
        for j in which:
            with scope(f"prod_{v}{j}"):
                take(last, v, PARTS - 1, j)
                product(("out", v, j))

    def rest(what, v):
        return range(GATHERED[v], CHUNKS) if what == "in" else range(GATHERED[v])

    with scope("stats"):
        for item in small:
            item.wait()
        start_gather(0, [0])
        stats_first()
        start_gather(1, range(steps))
    with scope("ld01"):
        loads[0].wait()
        loads[1].wait()
    with scope("first1"):
        back_part(0, 1)
        loads[2].wait()
        prep(1, 0)
        loads[3].wait()
        pre_part(1, 0)
        prep(1, 1)
        loads[4].wait()
        prep(0, 0)
    with scope("wpre1"):
        wait_pre(1, 0)
    with scope("fin1"):
        finish_pre(1, [0])
        wait_back(0, 1)
        for h in halves:
            finish_back(0, 1, h)
    with scope("first0"):
        finish_gs(0, 1)
        stats_second()
        start_gather(0, range(1, steps))
        pre_part(1, 1)
        prep(0, 1)
        loads[5].wait()
        loads[6].wait()
        back_part(0, 0)
        loads[7].wait()
        pre_part(0, 0)
        pre_part(0, 1)
        wait_pre(1, 1)
        finish_pre(1, range(1, steps))
    with scope("wpre0"):
        wait_pre(0, 0)
    with scope("fin0"):
        finish_pre(0, [0])
        wait_back(0, 0)
        for h in halves:
            finish_back(0, 0, h, send=False)
        finish_gs(0, 0)
        wait_pre(0, 1)
        finish_pre(0, range(1, steps))
        loads[8].wait()

    for t in range(1, last):
        for h in halves:
            step(t, 1, h)
        if t == 1:
            for h in halves:
                for c in pieces(steps, 0, h):
                    send_on(0, 0, h, c)
        finish_gs(t, 1)
    for h in halves[:-1]:
        step(last, 1, h)
    def end_products(v):
        products(v, ORDER[:3])
        for j in ORDER[3:]:
            take(last, v, PARTS - 1, j)
        back(last, v, PARTS - 1)
        with scope(f"gout{v}"):
            finish_gs(last, v)
            for j in ORDER[3:]:
                product(("out", v, j))
            for j in rest("in", v):
                product(("in", v, j))

    end_products(1)

    def first_middles():
        middle(("out", 1, 2))

    for t in range(1, last):
        for h in halves:
            ending = t == last - 1
            step(t, 0, h, first_middles if ending and h == 0 else None)
            if ending and h == 0:
                with scope("wgat1"):
                    wait_gathered(1)
                with scope("gin1"):
                    grad_in(1, rest("out", 1))
                    middle(("out", 1, 3))
        finish_gs(t, 0)
    with scope("mid1"):
        middle(("out", 1, 0))
        middle(("out", 1, 1))
    for h in halves[:-1]:
        step(last, 0, h)
    end_products(0)
    with scope("midi1"):
        for j in rest("in", 1):
            middle(("in", 1, j))
    with scope("wgat0"):
        wait_gathered(0)
    with scope("gin0"):
        grad_in(0, rest("out", 0))
    with scope("final1a"):
        for j in (2, 3, 0, 1):
            final(("out", 1, j))
        for j in rest("out", 1):
            final_in(1, j)
    with scope("mid0_3"):
        middle(("out", 0, 3))
    with scope("mid0_0"):
        middle(("out", 0, 0))
    with scope("mid0_2"):
        middle(("out", 0, 2))

    @pl.when(me_p < npipe - 1)
    def _():
        for item in stat_copies("h"):
            item.wait_recv()

    with scope("drain"):
        for item in stat_copies("l") + stat_copies("h"):
            item.wait_send()
        take_bytes(sqr, sq_s)
        take_bytes(pr, pre_s)
        take_bytes(br, back_s)

        @pl.when(me_p > 0)
        def _():
            take_bytes(ob, pipe_s)

        @pl.when(me_p == 0)
        def _():
            take_bytes(ob.at[:, 1], pipe_s)

        for v in range(vs):
            take_bytes(xr[v], xg_s.at[v])
            take_bytes(gsr[v].at[:, share_of(v)], gt_s.at[v])
            for item in pass_copies(v):
                item.wait_send()

    with scope("mid0_1"):
        middle(("out", 0, 1))
    with scope("midi0"):
        for j in rest("in", 0):
            middle(("in", 0, j))
    with scope("final0i"):
        for j in rest("out", 0):
            final_in(0, j)
    with scope("final1b"):
        for j in rest("in", 1):
            final(("in", 1, j))
    for v in range(vs):
        take_bytes(r2i.at[v, pl.ds(0, GATHERED[v]), pl.ds(0, count_of[split_kind[v]] - 1)], ri_s.at[v])

    def drain_split(copies, whole, sem):
        if na == nb:
            take_bytes(whole, sem)
        else:
            for job in jobs:
                for item in copies(job):
                    item.wait_send()

    drain_split(split_copies, r1, r1_s)
    for j in (3, 0, 1, 2):
        with scope(f"fin0_{j}"):
            final(("out", 0, j))
    with scope("fini0"):
        for j in rest("in", 0):
            final(("in", 0, j))
    with scope("tail"):
        drain_split(join_copies, r2, r2_s)


def store(a, b, c, a_out, b_out, c_out, sem):
    copies = [pltpu.make_async_copy(*pair, sem.at[k]) for k, pair in enumerate(((a, a_out), (b, b_out), (c, c_out)))]
    for item in copies:
        item.start()
    for item in copies:
        item.wait()


def shards(
    saved_inputs, proj_in, proj_out, norm_gain, arriving, logp_grad, rewards, seq_lengths, group_ids
):
    nt = lax.axis_size("tensor")
    npipe = lax.axis_size("pipe")
    ndp = lax.axis_size("dp")
    steps, vs, _, tok, wid = saved_inputs.shape
    rank = proj_in.shape[2]
    new_count = logp_grad.shape[0]
    group_count = new_count * ndp * rewards.shape[2] // 8
    lanes = -(-(group_count + 1) // 128) * 128
    na, nb = factors(ndp)
    rc = rank // ndp
    cc = wid // CHUNKS
    jobs = len(reductions())
    pipe_count = len(pipe_slots(steps, vs))
    hm, lm = max(na - 1, 1), max(nb - 1, 1)
    dims = (steps, vs, tok, wid, rank, nt, npipe, ndp)
    peers = max(nt - 1, 1)
    any_spec = pl.BlockSpec(memory_space=pl.ANY)
    vmem = pl.BlockSpec(memory_space=pltpu.VMEM)
    V = pltpu.VMEM
    DMA = pltpu.SemaphoreType.DMA
    pmax = max(na, nb)
    less = max(pmax - 1, 1)
    scratch = [
        V((steps, vs, tok, wid), BF16),
        V((vs, steps * tok, wid), BF16),
        V((vs, steps, tok, wid), BF16),
        V((vs, rank, wid), BF16),
        V((vs, rank, wid), BF16),
        V((new_count, tok, wid), BF16),
        V((vs, steps * tok, rank), BF16),
        V((peers, vs, steps * tok, rank), BF16),
        V((vs, steps * tok, rank), F32),
        V((vs, steps * tok, rank), F32),
        V((vs, rank, steps * tok), BF16),
        V((vs, steps * tok, rank), BF16),
        V((vs, na, nb, rc, steps * tok), BF16),
        V((hm, nb, rc, steps * tok), BF16),
        V((lm, na, rc, steps * tok), BF16),
        V((hm, steps, tok, GATHERED[0] * cc), BF16),
        V((lm, steps, tok, GATHERED[1] * cc), BF16),
        V((vs, steps, tok, rank), BF16),
        V((peers, vs, steps, tok, rank), BF16),
        V((steps - 1, vs, tok, wid), BF16),
        V((vs, 2, tok, 128), F32),
        V((peers, vs, 2, tok, 128), F32),
        V((vs, 2, tok, 128), F32),
        V((2, 8, lanes), F32),
        V((lm, 8, lanes), F32),
        V((jobs, na, nb, rc, cc), BF16),
        V((jobs, less, pmax, rc, cc), BF16),
        V((jobs, pmax, rc, cc), BF16),
        V((jobs, less, rc, cc), BF16),
        V((vs, CHUNKS, pmax, rc, cc), BF16),
        V((vs, CHUNKS, less, rc, cc), BF16),
        V(norm_gain.shape, F32),
        pltpu.SMEM(rewards.shape, F32),
        pltpu.SMEM(seq_lengths.shape, jnp.int32),
        pltpu.SMEM(group_ids.shape, jnp.int32),
        V((hm, 8, lanes), F32),
        pltpu.SemaphoreType.REGULAR,
        DMA((13,)),
        DMA,
        DMA((2 * vs, peers)),
        DMA((4, less)),
        DMA,
        DMA((2 * vs, peers)),
        DMA,
        DMA((vs * (1 + (steps - 1) * PARTS), peers)),
        DMA,
        DMA((pipe_count,)),
        DMA((vs,)),
        DMA((vs,)),
        DMA((vs,)),
        DMA((vs,)),
        DMA((vs, less, peers)),
        DMA((vs, less, peers)),
        DMA,
        DMA((jobs, less)),
        DMA,
        DMA((jobs, less)),
        DMA((vs,)),
        DMA((vs * CHUNKS, less)),
    ]
    grad_in, grad_out, leaving = pl.pallas_call(
        functools.partial(kernel, dims),
        out_shape=(
            V((vs, rc, wid), F32),
            V((vs, rc, wid), F32),
            V((vs, tok, wid), BF16),
        ),
        in_specs=[any_spec] * 9,
        out_specs=(vmem, vmem, vmem),
        scratch_shapes=scratch,
        compiler_params=pltpu.CompilerParams(
            collective_id=0, has_side_effects=True, vmem_limit_bytes=58 * 1024 * 1024
        ),
    )(
        saved_inputs[:, :, 0], proj_in[:, 0], proj_out[:, 0], norm_gain, arriving[:, 0], logp_grad,
        rewards, seq_lengths, group_ids,
    )
    grad_in, grad_out, leaving = pl.pallas_call(
        store,
        out_shape=tuple(jax.ShapeDtypeStruct(a.shape, a.dtype) for a in (grad_in, grad_out, leaving)),
        in_specs=[vmem] * 3,
        out_specs=[any_spec] * 3,
        scratch_shapes=[DMA((3,))],
        compiler_params=pltpu.CompilerParams(vmem_limit_bytes=1024 * 1024),
    )(grad_in, grad_out, leaving)
    return grad_in[:, None], grad_out[:, None], leaving[:, None]


def solution(mesh):
    return jax.shard_map(
        shards,
        mesh=mesh,
        in_specs=(
            P(None, None, "pipe", "dp", "tensor"),
            P(None, "pipe", None, "tensor"),
            P(None, "pipe", None, "tensor"),
            P(None, "pipe", "tensor"),
            P(None, "pipe", "dp", "tensor"),
            P(None, "dp", "tensor"),
            P(None, "dp", None),
            P(None, "dp", None),
            P(None, "dp", None),
        ),
        out_specs=(
            P(None, "pipe", "dp", "tensor"),
            P(None, "pipe", "dp", "tensor"),
            P(None, "pipe", "dp", "tensor"),
        ),
        check_vma=False,
    )
```

```python
import functools

import jax
import jax.numpy as jnp
from jax import lax
from jax.experimental import pallas as pl
from jax.experimental.pallas import tpu as pltpu
from jax.sharding import PartitionSpec as P

EPS = 1e-05
MESH = pl.DeviceIdType.MESH
F32 = jnp.float32
BF16 = jnp.bfloat16


def dot_nt(a, b):
    return lax.dot_general(a, b, (((1,), (1,)), ((), ())), preferred_element_type=F32)


def factors(n):
    low = 1
    for k in range(1, n + 1):
        if n % k == 0 and k * k <= n:
            low = k
    return low, n // low


CHUNKS = 4
GATHERED = (3, 3)
PARTS = 2
FIRST_AXIS = ("hhll", "hllh")
IN_AXIS = ("h", "l")
ORDER = (3, 2, 0, 1)
scope = jax.named_scope


def reductions():
    jobs = [("out", v, j) for v in (1, 0) for j in range(CHUNKS)]
    jobs += [("in", v, j) for v in (1, 0) for j in range(GATHERED[v], CHUNKS)]
    return {job: e for e, job in enumerate(jobs)}


def pieces(steps, t, h):
    return ORDER if (t, h) in ((0, 0), (steps - 2, PARTS - 1)) else (None,)


def pipe_slots(steps, vs):
    keys = [(t, v, h, c) for t in range(steps - 1) for v in range(vs) for h in range(PARTS) for c in pieces(steps, t, h)]
    return {key: k for k, key in enumerate(keys)}


def kernel(
    dims,
    x_hbm, wi_hbm, wo_hbm, gn_hbm, ar_hbm, lp_hbm, rew_hbm, len_hbm, ids_hbm,
    fi, fo, lv,
    xs, gd, ca, wi, wo, lp, ps, pr, presum, slope, hid_t, gs, gs_t, gsr0, gsr1, xr0, xr1, bs, br, ob,
    sqs, sqr, inv_t, stl, str_, gb, r1, p2, r2, p2i, r2i,
    gn_ref, rew_ref, len_ref, ids_ref, str2, wrap_sem,
    in_sem, sq_s, sq_r, st_sem, pre_s, pre_r, back_s, back_r, pipe_s, pipe_r, xg_s, xg_r, gt_s, gt_r, gf_s, gf_r,
    r1_s, r1_r, r2_s, r2_r, ri_s, ri_r,
):
    steps, vs, tok, wid, rank, nt, npipe, ndp = dims
    na, nb = factors(ndp)
    rc = rank // ndp
    full = wid * nt
    tile = min(512, wid // 2)
    rtile = min(512, rank)
    cc = wid // CHUNKS
    part_tok = tok // PARTS
    lanes = stl.shape[2]
    new_count, _, seq_count = rew_ref.shape
    unit_lane = new_count * ndp * seq_count // 8
    me_t = lax.axis_index("tensor")
    me_p = lax.axis_index("pipe")
    me_d = lax.axis_index("dp")
    me_h = me_d // nb
    me_l = me_d % nb
    prev_p = lax.rem(me_p + npipe - 1, npipe)
    next_p = lax.rem(me_p + 1, npipe)

    def load(src, dst, k):
        return pltpu.make_async_copy(src, dst, in_sem.at[k])

    loads = [
        load(ar_hbm.at[1], ca.at[1, 0], 0),
        load(wo_hbm.at[1], wo.at[1], 1),
        load(x_hbm.at[:, 1], xs.at[:, 1], 2),
        load(wi_hbm.at[1], wi.at[1], 3),
        load(x_hbm.at[:, 0], xs.at[:, 0], 4),
        load(ar_hbm.at[0], ca.at[0, 0], 5),
        load(wo_hbm.at[0], wo.at[0], 6),
        load(wi_hbm.at[0], wi.at[0], 7),
        load(lp_hbm, lp, 8),
    ]
    small = [
        load(gn_hbm, gn_ref, 9),
        load(rew_hbm, rew_ref, 10),
        load(len_hbm, len_ref, 11),
        load(ids_hbm, ids_ref, 12),
    ]

    barrier = pltpu.get_barrier_semaphore()
    for k in range(1, nt):
        pl.semaphore_signal(barrier, inc=1, device_id={"tensor": lax.rem(me_t + k, nt)}, device_id_type=MESH)
    for k in range(1, na):
        peer = lax.rem(me_h + k, na) * nb + me_l
        pl.semaphore_signal(barrier, inc=1, device_id={"dp": peer}, device_id_type=MESH)
    for k in range(1, nb):
        peer = me_h * nb + lax.rem(me_l + k, nb)
        pl.semaphore_signal(barrier, inc=1, device_id={"dp": peer}, device_id_type=MESH)

    @pl.when(me_p < npipe - 1)
    def _():
        pl.semaphore_signal(barrier, inc=1, device_id={"pipe": next_p}, device_id_type=MESH)

    @pl.when(me_p == 0)
    def _():
        pl.semaphore_signal(barrier, inc=1, device_id={"pipe": prev_p}, device_id_type=MESH)


    for item in small + loads:
        item.start()

    with scope("barrier"):
        along_pipe = jnp.where(me_p == 0, 0, jnp.where(me_p == npipe - 1, 2, 1))
        pl.semaphore_wait(barrier, nt - 1 + na - 1 + nb - 1 + along_pipe)

    @pl.when(me_p == npipe - 1)
    def _():
        pl.semaphore_signal(wrap_sem, inc=1, device_id={"pipe": next_p}, device_id_type=MESH)

    def to_tensor(src, dst_of, send_of, recv_of):
        return [
            pltpu.make_async_remote_copy(
                src_ref=src, dst_ref=dst_of(k - 1), send_sem=send_of(k - 1), recv_sem=recv_of(k - 1),
                device_id={"tensor": lax.rem(me_t + k, nt)}, device_id_type=MESH,
            )
            for k in range(1, nt)
        ]

    def to_dp(src_of, dst_of, send_of, recv_of, kind):
        out = []
        count = {"h": na, "l": nb}[kind]
        for k in range(1, count):
            if kind == "h":
                part = lax.rem(me_h + k, na)
                who = part * nb + me_l
            else:
                part = lax.rem(me_l + k, nb)
                who = me_h * nb + part
            out.append(
                pltpu.make_async_remote_copy(
                    src_ref=src_of(part), dst_ref=dst_of(k - 1), send_sem=send_of(k - 1), recv_sem=recv_of(k - 1),
                    device_id={"dp": who}, device_id_type=MESH,
                )
            )
        return out

    gather_kind = ("h", "l")
    split_kind = ("l", "h")
    count_of = {"h": na, "l": nb}
    xr = (xr0, xr1)
    gsr = (gsr0, gsr1)

    def x_copies(t, v):
        cols = pl.ds(0, GATHERED[v] * cc)
        return to_dp(
            lambda part: x_hbm.at[t, v, :, cols], lambda k: xr[v].at[k, t],
            lambda k: xg_s.at[v], lambda k: xg_r.at[v], gather_kind[v],
        )


    def stat_copies(kind):
        if kind == "l":
            return to_dp(lambda part: stl.at[0], lambda k: str_.at[k], lambda k: st_sem.at[0, k], lambda k: st_sem.at[1, k], kind)
        return to_dp(lambda part: stl.at[1], lambda k: str2.at[k], lambda k: st_sem.at[2, k], lambda k: st_sem.at[3, k], kind)

    def stats_first():
        lane8 = lax.broadcasted_iota(jnp.int32, (8, lanes), 1)
        row8 = lax.broadcasted_iota(jnp.int32, (8, lanes), 0)
        stats_own = jnp.where((row8 == 2) & (lane8 == unit_lane), 1.0, 0.0)
        for n in range(new_count):
            for k in range(seq_count):
                value = jnp.where(row8 == 0, rew_ref[n, 0, k], jnp.where(row8 == 1, 1.0, 0.0))
                stats_own = stats_own + jnp.where(lane8 == ids_ref[n, 0, k], value, 0.0)
        stl[0] = stats_own
        for item in stat_copies("l"):
            item.start()

    def stats_second():
        for item in stat_copies("l"):
            item.wait_recv()
        total = stl[0]
        for k in range(nb - 1):
            total = total + str_[k]
        stl[1] = total
        for item in stat_copies("h"):
            item.start()

    def start_gather(v, which):
        for t in which:
            for item in x_copies(t, v):
                item.start()

    lane = lax.broadcasted_iota(jnp.int32, (tok, 128), 1)

    groups = ((0, 1), (1, steps))

    def group_of(t):
        return 0 if t == 0 else 1

    def sq_copies(v, g):
        base = 2 * v + g
        return to_tensor(
            sqs.at[v, g], lambda k: sqr.at[k, v, g], lambda k: sq_s, lambda k: sq_r.at[base, k]
        )

    def prep(v, g):
        def body(t, squares_all):
            row = xs[t, v].astype(F32)
            gd[v, pl.ds(pl.multiple_of(t * tok, tok), tok), :] = (row * gn_ref[v]).astype(BF16)
            squares = jnp.sum(row * row, axis=-1, keepdims=True)
            return jnp.where(lane == t, squares, squares_all)

        sqs[v, g] = lax.fori_loop(*groups[g], body, jnp.zeros((tok, 128), F32))
        for item in sq_copies(v, g):
            item.start()

    def finish_sq(v, g):
        for item in sq_copies(v, g):
            item.wait_recv()
        total = sqs[v, g]
        for k in range(nt - 1):
            total = total + sqr[k, v, g]
        inv_t[v, g] = 1.0 / jnp.sqrt(total * (1.0 / full) + EPS)

    def share_of(v):
        count = count_of[split_kind[v]]
        if count % nt:
            return pl.ds(0, count)
        return pl.ds(me_t * (count // nt), count // nt)

    def gs_copies(t, v):
        cols = pl.ds(t * tok, tok)
        mine = share_of(v)
        source = (lambda part: gs_t.at[v, part, mine, :, cols]) if v == 0 else (lambda part: gs_t.at[v, mine, part, :, cols])
        return to_dp(
            source, lambda k: gsr[v].at[k, mine, :, cols],
            lambda k: gt_s.at[v], lambda k: gt_r.at[v], gather_kind[v],
        )

    def pass_copies(v):
        if count_of[split_kind[v]] % nt:
            return []
        out = []
        for k in range(count_of[gather_kind[v]] - 1):
            piece = gsr[v].at[k, share_of(v)]
            out += to_tensor(piece, lambda i: piece, lambda i: gf_s.at[v, k, i], lambda i: gf_r.at[v, k, i])
        return out

    def take_bytes(ref, sem):
        pltpu.make_async_copy(ref, ref, sem).wait()

    pre_copies = {}
    back_copies = {}

    def pre_part(v, g):
        low, high = groups[g]
        rows = pl.ds(low * tok, (high - low) * tok)

        def body(j, carry):
            cols = pl.ds(pl.multiple_of(j * rtile, rtile), rtile)
            ps[v, rows, cols] = dot_nt(gd[v, rows, :], wi[v, cols, :]).astype(BF16)
            return carry

        lax.fori_loop(0, rank // rtile, body, 0)
        base = 2 * v + g
        pre_copies[v, g] = to_tensor(
            ps.at[v, rows], lambda k: pr.at[k, v, rows], lambda k: pre_s, lambda k: pre_r.at[base, k]
        )
        for item in pre_copies[v, g]:
            item.start()

    def wait_pre(v, g):
        finish_sq(v, g)
        for item in pre_copies[v, g]:
            item.wait_recv()

    def cols_of(j):
        return pl.ds(j * cc, cc)

    def rows_of(h):
        return pl.ds(h * part_tok, part_tok)

    def back_part(t, v, h=None):
        rows = pl.ds(0, tok) if h is None else rows_of(h)

        def body(j, carry):
            cols = pl.ds(pl.multiple_of(j * rtile, rtile), rtile)
            bs[v, t, rows, cols] = dot_nt(ca[v, t, rows, :], wo[v, cols, :]).astype(BF16)
            return carry

        lax.fori_loop(0, rank // rtile, body, 0)
        base = v * (1 + (steps - 1) * PARTS) + (0 if h is None else 1 + (t - 1) * PARTS + h)
        back_copies[t, v, h] = to_tensor(
            bs.at[v, t, rows], lambda k: br.at[k, v, t, rows],
            lambda k: back_s, lambda k: back_r.at[base, k],
        )
        for item in back_copies[t, v, h]:
            item.start()

    def finish_pre(v, which_steps):
        for t in which_steps:
            rows = pl.ds(t * tok, tok)
            total = ps[v, rows, :].astype(F32)
            for k in range(nt - 1):
                total = total + pr[k, v, rows, :].astype(F32)
            pre = inv_t[v, group_of(t), :, t:t + 1] * total
            sigma = jax.nn.sigmoid(pre)
            presum[v, rows, :] = total
            hid_t[v, :, rows] = jnp.transpose(pre * sigma).astype(BF16)
            slope[v, rows, :] = sigma * (1.0 + pre * (1.0 - sigma))

    def wait_back(t, v, h=None):
        for item in back_copies[t, v, h]:
            item.wait_recv()

    def finish_back(t, v, h, send=True):
        own = rows_of(h)
        rows = pl.ds(t * tok + h * part_tok, part_tok)
        inv = inv_t[v, group_of(t), own, t:t + 1]
        total = bs[v, t, own, :].astype(F32)
        for k in range(nt - 1):
            total = total + br[k, v, t, own, :].astype(F32)
        grad_pre = total * slope[v, rows, :]
        gs[v, rows, :] = (inv * grad_pre).astype(BF16)
        radial = jnp.sum(grad_pre * presum[v, rows, :], axis=-1, keepdims=True)
        coef = inv * inv * inv * radial * (1.0 / full)

        def part(cols):
            lifted = jnp.dot(gs[v, rows, :], wi[v, :, cols], preferred_element_type=F32)
            out = (
                ca[v, t, own, cols].astype(F32)
                + gn_ref[v, :, cols] * lifted
                - xs[t, v, own, cols].astype(F32) * coef
            ).astype(BF16)
            if t < steps - 1:
                ob[t, v, own, cols] = out
            else:
                lv[v, own, cols] = out

        def body(j, carry):
            part(pl.ds(pl.multiple_of(j * tile, tile), tile))
            return carry

        if t < steps - 1 and len(pieces(steps, t, h)) > 1:
            for c in pieces(steps, t, h):
                part(cols_of(c))
                if send:
                    send_on(t, v, h, c)
        else:
            lax.fori_loop(0, wid // tile, body, 0)
            if t < steps - 1 and send:
                send_on(t, v, h, None)

    halves = range(PARTS)
    slots = pipe_slots(steps, vs)

    def finish_gs(t, v):
        rows = pl.ds(t * tok, tok)
        flipped = jnp.transpose(gs[v, rows, :].astype(F32)).astype(BF16)
        gs_t[v, :, :, :, rows] = flipped.reshape(na, nb, rc, tok)
        for item in gs_copies(t, v):
            item.start()

    def pipe_copy(t, v, slot, h, c):
        where = (rows_of(h),) if c is None else (rows_of(h), cols_of(c))
        return pltpu.make_async_remote_copy(
            src_ref=ob.at[(t, v) + where], dst_ref=ca.at[(slot, t + 1) + where],
            send_sem=pipe_s, recv_sem=pipe_r.at[slots[t, slot, h, c]],
            device_id={"pipe": prev_p}, device_id_type=MESH,
        )

    def send_on(t, v, h, c):
        @pl.when(me_p > 0)
        def _():
            pipe_copy(t, v, v, h, c).start()

        if v == 1:
            @pl.when(me_p == 0)
            def _():
                if t == 0 and h == 0 and c == pieces(steps, t, h)[0]:
                    pl.semaphore_wait(wrap_sem, 1)
                pipe_copy(t, 1, 0, h, c).start()

    def take(t, v, h, only=None):
        want = pieces(steps, t - 1, h)
        first = only is None or only == want[0]
        if only is not None:
            want = (only,)
        if v == 0:
            for c in want:
                pipe_copy(t - 1, v, v, h, c).wait_recv()
            return

        @pl.when(me_p < npipe - 1)
        def _():
            for c in want:
                pipe_copy(t - 1, v, v, h, c).wait_recv()

        if first:
            @pl.when(me_p == npipe - 1)
            def _():
                if t == 1 and h == 0:
                    for item in stat_copies("h"):
                        item.wait_recv()
                stats = stl[1]
                for k in range(na - 1):
                    stats = stats + str2[k]
                means = stats[0:1] / jnp.maximum(stats[1:2], 1.0) + stats[2:3] * (1.0 / ndp)
                tok_row = lax.broadcasted_iota(jnp.int32, (part_tok, lanes), 0) + h * part_tok
                tok_lane = lax.broadcasted_iota(jnp.int32, (part_tok, lanes), 1)
                hot = jnp.zeros((part_tok, lanes), F32)
                begin = 0
                for k in range(seq_count):
                    finish = begin + len_ref[t - 1, 0, k]
                    inside = (tok_row >= begin) & (tok_row < finish)
                    value = jnp.where(tok_lane == ids_ref[t - 1, 0, k], 1.0, 0.0)
                    value = value - jnp.where(tok_lane == unit_lane, rew_ref[t - 1, 0, k], 0.0)
                    hot = hot + jnp.where(inside, value, 0.0)
                    begin = finish
                weight = jnp.sum(hot * means, axis=-1, keepdims=True)
                ca[1, t, rows_of(h), :] = (weight * lp[t - 1, rows_of(h), :].astype(F32)).astype(BF16)

    jobs = reductions()

    def axes_of(job):
        what, v, j = job
        first = FIRST_AXIS[v][j] if what == "out" else IN_AXIS[v]
        return ("l", "h") if first == "l" else ("h", "l")

    def split_copies(job):
        e = jobs[job]
        first, second = axes_of(job)
        count = count_of[second]
        source = (lambda part: gb.at[e, :, part]) if first == "l" else (lambda part: gb.at[e, part])
        return to_dp(
            source, lambda k: r1.at[e, k, pl.ds(0, count)], lambda k: r1_s, lambda k: r1_r.at[e, k], first
        )

    def join_copies(job):
        e = jobs[job]
        return to_dp(
            lambda part: p2.at[e, part], lambda k: r2.at[e, k], lambda k: r2_s, lambda k: r2_r.at[e, k],
            axes_of(job)[1],
        )

    def product(job):
        what, v, j = job
        e = jobs[job]
        if what == "out":
            value = jnp.dot(
                hid_t[v], ca[v, :, :, cols_of(j)].reshape(steps * tok, cc), preferred_element_type=F32
            )
        else:
            value = jnp.dot(
                gs_t[v].reshape(rank, steps * tok), xs[:, v, :, cols_of(j)].reshape(steps * tok, cc),
                preferred_element_type=F32,
            ) * gn_ref[v, :, cols_of(j)]
        gb[e] = value.astype(BF16).reshape(na, nb, rc, cc)
        for item in split_copies(job):
            item.start()

    def middle(job):
        e = jobs[job]
        first, second = axes_of(job)
        count = count_of[second]
        for item in split_copies(job):
            item.wait_recv()
        own = gb[e, :, me_l] if first == "l" else gb[e, me_h]
        total = own.astype(F32)
        for k in range(count_of[first] - 1):
            total = total + r1[e, k, :count].astype(F32)
        p2[e, :count] = total.astype(BF16)
        for item in join_copies(job):
            item.start()

    scale = 1.0 / (ndp * tok)

    def final(job):
        what, v, j = job
        e = jobs[job]
        kind = axes_of(job)[1]
        for item in join_copies(job):
            item.wait_recv()
        total = p2[e, me_h if kind == "h" else me_l].astype(F32)
        for k in range(count_of[kind] - 1):
            total = total + r2[e, k].astype(F32)
        dest = fo if what == "out" else fi
        dest[v, :, cols_of(j)] = total * scale

    def in_bytes(v):
        return r2i.at[v, pl.ds(0, GATHERED[v]), pl.ds(0, count_of[split_kind[v]] - 1)]

    def in_copies(v, j):
        return to_dp(
            lambda part: p2i.at[v, j, part], lambda k: r2i.at[v, j, k],
            lambda k: ri_s.at[v], lambda k: ri_r.at[v], split_kind[v],
        )

    def wait_gathered(v):
        take_bytes(gsr[v].at[:, share_of(v)], gt_r.at[v])
        for item in pass_copies(v):
            item.start()
        take_bytes(xr[v], xg_r.at[v])
        for item in pass_copies(v):
            item.wait_recv()

    def grad_in(v, which):
        width = count_of[split_kind[v]]
        own = gs_t[v, me_h] if v == 0 else gs_t[v, :, me_l]
        own = own.reshape(width * rc, steps * tok)
        for j in which:
            value = jnp.dot(
                own, xs[:, v, :, cols_of(j)].reshape(steps * tok, cc), preferred_element_type=F32
            )
            for k in range(count_of[gather_kind[v]] - 1):
                left = gsr[v][k].reshape(width * rc, steps * tok)
                value = value + jnp.dot(
                    left, xr[v][k, :, :, cols_of(j)].reshape(steps * tok, cc), preferred_element_type=F32
                )
            value = value * gn_ref[v, :, cols_of(j)]
            p2i[v, j, :width] = value.astype(BF16).reshape(width, rc, cc)
            for item in in_copies(v, j):
                item.start()

    def final_in(v):
        take_bytes(in_bytes(v), ri_r.at[v])
        along_h = split_kind[v] == "h"
        for j in range(GATHERED[v]):
            total = p2i[v, j, me_h if along_h else me_l].astype(F32)
            for k in range(count_of[split_kind[v]] - 1):
                total = total + r2i[v, j, k].astype(F32)
            fi[v, :, cols_of(j)] = total * scale

    last = steps - 1

    def back(t, v, h, during=None):
        with scope(f"back_{t}{v}{h}"):
            back_part(t, v, h)
            if during is not None:
                during()
            wait_back(t, v, h)
        with scope(f"fin_{t}{v}{h}"):
            finish_back(t, v, h)

    def step(t, v, h, during=None):
        with scope(f"take_{t}{v}{h}"):
            take(t, v, h)
        back(t, v, h, during)

    def products(v, which):
        for j in which:
            with scope(f"prod_{v}{j}"):
                take(last, v, PARTS - 1, j)
                product(("out", v, j))

    def rest(what, v):
        return range(GATHERED[v], CHUNKS) if what == "in" else range(GATHERED[v])

    with scope("stats"):
        for item in small:
            item.wait()
        start_gather(0, [0])
        stats_first()
        start_gather(1, range(steps))
    with scope("ld01"):
        loads[0].wait()
        loads[1].wait()
    with scope("first1"):
        back_part(0, 1)
        loads[2].wait()
        prep(1, 0)
        loads[3].wait()
        pre_part(1, 0)
        prep(1, 1)
        loads[4].wait()
        prep(0, 0)
    with scope("wpre1"):
        wait_pre(1, 0)
    with scope("fin1"):
        finish_pre(1, [0])
        wait_back(0, 1)
        for h in halves:
            finish_back(0, 1, h)
    with scope("first0"):
        finish_gs(0, 1)
        stats_second()
        start_gather(0, range(1, steps))
        pre_part(1, 1)
        prep(0, 1)
        loads[5].wait()
        loads[6].wait()
        back_part(0, 0)
        loads[7].wait()
        pre_part(0, 0)
        pre_part(0, 1)
        wait_pre(1, 1)
        finish_pre(1, range(1, steps))
    with scope("wpre0"):
        wait_pre(0, 0)
    with scope("fin0"):
        finish_pre(0, [0])
        wait_back(0, 0)
        for h in halves:
            finish_back(0, 0, h, send=False)
        finish_gs(0, 0)
        wait_pre(0, 1)
        finish_pre(0, range(1, steps))
        loads[8].wait()

    for t in range(1, last):
        for h in halves:
            step(t, 1, h)
        if t == 1:
            for h in halves:
                for c in pieces(steps, 0, h):
                    send_on(0, 0, h, c)
        finish_gs(t, 1)
    for h in halves[:-1]:
        step(last, 1, h)
    def end_products(v):
        products(v, ORDER[:3])
        for j in ORDER[3:]:
            take(last, v, PARTS - 1, j)
        back(last, v, PARTS - 1)
        with scope(f"gout{v}"):
            finish_gs(last, v)
            for j in ORDER[3:]:
                product(("out", v, j))
            for j in rest("in", v):
                product(("in", v, j))

    end_products(1)

    def first_middles():
        middle(("out", 1, 2))

    for t in range(1, last):
        for h in halves:
            ending = t == last - 1
            step(t, 0, h, first_middles if ending and h == 0 else None)
            if ending and h == 0:
                with scope("wgat1"):
                    wait_gathered(1)
                with scope("gin1"):
                    grad_in(1, rest("out", 1))
                    middle(("out", 1, 3))
        finish_gs(t, 0)
    with scope("mid1"):
        middle(("out", 1, 0))
        middle(("out", 1, 1))
    for h in halves[:-1]:
        step(last, 0, h)
    end_products(0)
    with scope("midi1"):
        for j in rest("in", 1):
            middle(("in", 1, j))
    with scope("mid0_3"):
        middle(("out", 0, 3))
    with scope("mid0_0"):
        middle(("out", 0, 0))
    with scope("wgat0"):
        wait_gathered(0)
    with scope("gin0"):
        grad_in(0, rest("out", 0))
    with scope("final1a"):
        for j in (2, 3, 0, 1):
            final(("out", 1, j))
        final_in(1)
    with scope("mid0_2"):
        middle(("out", 0, 2))

    @pl.when(me_p < npipe - 1)
    def _():
        for item in stat_copies("h"):
            item.wait_recv()

    with scope("drain"):
        for item in stat_copies("l") + stat_copies("h"):
            item.wait_send()
        take_bytes(sqr, sq_s)
        take_bytes(pr, pre_s)
        take_bytes(br, back_s)

        @pl.when(me_p > 0)
        def _():
            take_bytes(ob, pipe_s)

        @pl.when(me_p == 0)
        def _():
            take_bytes(ob.at[:, 1], pipe_s)

        for v in range(vs):
            take_bytes(xr[v], xg_s.at[v])
            take_bytes(gsr[v].at[:, share_of(v)], gt_s.at[v])
            for item in pass_copies(v):
                item.wait_send()

    with scope("mid0_1"):
        middle(("out", 0, 1))
    with scope("midi0"):
        for j in rest("in", 0):
            middle(("in", 0, j))
    with scope("final0i"):
        final_in(0)
    with scope("final1b"):
        for j in rest("in", 1):
            final(("in", 1, j))
    for v in range(vs):
        take_bytes(in_bytes(v), ri_s.at[v])

    def drain_split(copies, whole, sem):
        if na == nb:
            take_bytes(whole, sem)
        else:
            for job in jobs:
                for item in copies(job):
                    item.wait_send()

    drain_split(split_copies, r1, r1_s)
    for j in (3, 0, 1, 2):
        with scope(f"fin0_{j}"):
            final(("out", 0, j))
    with scope("fini0"):
        for j in rest("in", 0):
            final(("in", 0, j))
    with scope("tail"):
        drain_split(join_copies, r2, r2_s)


def store(a, b, c, a_out, b_out, c_out, sem):
    pairs = ((a, a_out), (b, b_out), (c, c_out))
    for k, (src, dst) in enumerate(pairs):
        rows = src.shape[1] // 2
        for v in range(src.shape[0]):
            for r in range(2):
                where = (v, pl.ds(r * rows, rows))
                pltpu.make_async_copy(src.at[where], dst.at[where], sem.at[k]).start()
    for k, pair in enumerate(pairs):
        pltpu.make_async_copy(*pair, sem.at[k]).wait()


def shards(
    saved_inputs, proj_in, proj_out, norm_gain, arriving, logp_grad, rewards, seq_lengths, group_ids
):
    nt = lax.axis_size("tensor")
    npipe = lax.axis_size("pipe")
    ndp = lax.axis_size("dp")
    steps, vs, _, tok, wid = saved_inputs.shape
    rank = proj_in.shape[2]
    new_count = logp_grad.shape[0]
    group_count = new_count * ndp * rewards.shape[2] // 8
    lanes = -(-(group_count + 1) // 128) * 128
    na, nb = factors(ndp)
    rc = rank // ndp
    cc = wid // CHUNKS
    jobs = len(reductions())
    pipe_count = len(pipe_slots(steps, vs))
    hm, lm = max(na - 1, 1), max(nb - 1, 1)
    dims = (steps, vs, tok, wid, rank, nt, npipe, ndp)
    peers = max(nt - 1, 1)
    any_spec = pl.BlockSpec(memory_space=pl.ANY)
    vmem = pl.BlockSpec(memory_space=pltpu.VMEM)
    V = pltpu.VMEM
    DMA = pltpu.SemaphoreType.DMA
    pmax = max(na, nb)
    less = max(pmax - 1, 1)
    scratch = [
        V((steps, vs, tok, wid), BF16),
        V((vs, steps * tok, wid), BF16),
        V((vs, steps, tok, wid), BF16),
        V((vs, rank, wid), BF16),
        V((vs, rank, wid), BF16),
        V((new_count, tok, wid), BF16),
        V((vs, steps * tok, rank), BF16),
        V((peers, vs, steps * tok, rank), BF16),
        V((vs, steps * tok, rank), F32),
        V((vs, steps * tok, rank), F32),
        V((vs, rank, steps * tok), BF16),
        V((vs, steps * tok, rank), BF16),
        V((vs, na, nb, rc, steps * tok), BF16),
        V((hm, nb, rc, steps * tok), BF16),
        V((lm, na, rc, steps * tok), BF16),
        V((hm, steps, tok, GATHERED[0] * cc), BF16),
        V((lm, steps, tok, GATHERED[1] * cc), BF16),
        V((vs, steps, tok, rank), BF16),
        V((peers, vs, steps, tok, rank), BF16),
        V((steps - 1, vs, tok, wid), BF16),
        V((vs, 2, tok, 128), F32),
        V((peers, vs, 2, tok, 128), F32),
        V((vs, 2, tok, 128), F32),
        V((2, 8, lanes), F32),
        V((lm, 8, lanes), F32),
        V((jobs, na, nb, rc, cc), BF16),
        V((jobs, less, pmax, rc, cc), BF16),
        V((jobs, pmax, rc, cc), BF16),
        V((jobs, less, rc, cc), BF16),
        V((vs, CHUNKS, pmax, rc, cc), BF16),
        V((vs, CHUNKS, less, rc, cc), BF16),
        V(norm_gain.shape, F32),
        pltpu.SMEM(rewards.shape, F32),
        pltpu.SMEM(seq_lengths.shape, jnp.int32),
        pltpu.SMEM(group_ids.shape, jnp.int32),
        V((hm, 8, lanes), F32),
        pltpu.SemaphoreType.REGULAR,
        DMA((13,)),
        DMA,
        DMA((2 * vs, peers)),
        DMA((4, less)),
        DMA,
        DMA((2 * vs, peers)),
        DMA,
        DMA((vs * (1 + (steps - 1) * PARTS), peers)),
        DMA,
        DMA((pipe_count,)),
        DMA((vs,)),
        DMA((vs,)),
        DMA((vs,)),
        DMA((vs,)),
        DMA((vs, less, peers)),
        DMA((vs, less, peers)),
        DMA,
        DMA((jobs, less)),
        DMA,
        DMA((jobs, less)),
        DMA((vs,)),
        DMA((vs,)),
    ]
    grad_in, grad_out, leaving = pl.pallas_call(
        functools.partial(kernel, dims),
        out_shape=(
            V((vs, rc, wid), F32),
            V((vs, rc, wid), F32),
            V((vs, tok, wid), BF16),
        ),
        in_specs=[any_spec] * 9,
        out_specs=(vmem, vmem, vmem),
        scratch_shapes=scratch,
        compiler_params=pltpu.CompilerParams(
            collective_id=0, has_side_effects=True, vmem_limit_bytes=58 * 1024 * 1024
        ),
    )(
        saved_inputs[:, :, 0], proj_in[:, 0], proj_out[:, 0], norm_gain, arriving[:, 0], logp_grad,
        rewards, seq_lengths, group_ids,
    )
    grad_in, grad_out, leaving = pl.pallas_call(
        store,
        out_shape=tuple(jax.ShapeDtypeStruct(a.shape, a.dtype) for a in (grad_in, grad_out, leaving)),
        in_specs=[vmem] * 3,
        out_specs=[any_spec] * 3,
        scratch_shapes=[DMA((3,))],
        compiler_params=pltpu.CompilerParams(vmem_limit_bytes=1024 * 1024),
    )(grad_in, grad_out, leaving)
    return grad_in[:, None], grad_out[:, None], leaving[:, None]


def solution(mesh):
    return jax.shard_map(
        shards,
        mesh=mesh,
        in_specs=(
            P(None, None, "pipe", "dp", "tensor"),
            P(None, "pipe", None, "tensor"),
            P(None, "pipe", None, "tensor"),
            P(None, "pipe", "tensor"),
            P(None, "pipe", "dp", "tensor"),
            P(None, "dp", "tensor"),
            P(None, "dp", None),
            P(None, "dp", None),
            P(None, "dp", None),
        ),
        out_specs=(
            P(None, "pipe", "dp", "tensor"),
            P(None, "pipe", "dp", "tensor"),
            P(None, "pipe", "dp", "tensor"),
        ),
        check_vma=False,
    )
```

```python
import functools

import jax
import jax.numpy as jnp
from jax import lax
from jax.experimental import pallas as pl
from jax.experimental.pallas import tpu as pltpu
from jax.sharding import PartitionSpec as P

EPS = 1e-05
MESH = pl.DeviceIdType.MESH
F32 = jnp.float32
BF16 = jnp.bfloat16


def dot_nt(a, b):
    return lax.dot_general(a, b, (((1,), (1,)), ((), ())), preferred_element_type=F32)


def factors(n):
    low = 1
    for k in range(1, n + 1):
        if n % k == 0 and k * k <= n:
            low = k
    return low, n // low


CHUNKS = 4
GATHERED = (3, 3)
EXTRA = -128
PARTS = 2
FIRST_AXIS = ("hhll", "hllh")
IN_AXIS = ("h", "l")
ORDER = (3, 2, 0, 1)
scope = jax.named_scope


def reductions():
    jobs = [("out", v, j) for v in (1, 0) for j in range(CHUNKS)]
    jobs += [("in", v, j) for v in (1, 0) for j in range(GATHERED[v], CHUNKS)]
    return {job: e for e, job in enumerate(jobs)}


def pieces(steps, t, h):
    return ORDER if (t, h) in ((0, 0), (steps - 2, PARTS - 1)) else (None,)


def pipe_slots(steps, vs):
    keys = [(t, v, h, c) for t in range(steps - 1) for v in range(vs) for h in range(PARTS) for c in pieces(steps, t, h)]
    return {key: k for k, key in enumerate(keys)}


def kernel(
    dims,
    x_hbm, wi_hbm, wo_hbm, gn_hbm, ar_hbm, lp_hbm, rew_hbm, len_hbm, ids_hbm,
    fi, fo, lv,
    xs, gd, ca, wi, wo, lp, ps, pr, presum, slope, hid_t, gs, gs_t, gsr0, gsr1, xr0, xr1, bs, br, ob,
    sqs, sqr, inv_t, stl, str_, gb, r1, p2, r2, p2i, r2i,
    gn_ref, rew_ref, len_ref, ids_ref, str2, wrap_sem,
    in_sem, sq_s, sq_r, st_sem, pre_s, pre_r, back_s, back_r, pipe_s, pipe_r, xg_s, xg_r, gt_s, gt_r, gf_s, gf_r,
    r1_s, r1_r, r2_s, r2_r, ri_s, ri_r,
):
    steps, vs, tok, wid, rank, nt, npipe, ndp = dims
    na, nb = factors(ndp)
    rc = rank // ndp
    full = wid * nt
    tile = min(512, wid // 2)
    rtile = min(512, rank)
    cc = wid // CHUNKS
    part_tok = tok // PARTS
    lanes = stl.shape[2]
    new_count, _, seq_count = rew_ref.shape
    unit_lane = new_count * ndp * seq_count // 8
    me_t = lax.axis_index("tensor")
    me_p = lax.axis_index("pipe")
    me_d = lax.axis_index("dp")
    me_h = me_d // nb
    me_l = me_d % nb
    prev_p = lax.rem(me_p + npipe - 1, npipe)
    next_p = lax.rem(me_p + 1, npipe)

    def load(src, dst, k):
        return pltpu.make_async_copy(src, dst, in_sem.at[k])

    loads = [
        load(ar_hbm.at[1], ca.at[1, 0], 0),
        load(wo_hbm.at[1], wo.at[1], 1),
        load(x_hbm.at[:, 1], xs.at[:, 1], 2),
        load(wi_hbm.at[1], wi.at[1], 3),
        load(x_hbm.at[:, 0], xs.at[:, 0], 4),
        load(ar_hbm.at[0], ca.at[0, 0], 5),
        load(wo_hbm.at[0], wo.at[0], 6),
        load(wi_hbm.at[0], wi.at[0], 7),
        load(lp_hbm, lp, 8),
    ]
    small = [
        load(gn_hbm, gn_ref, 9),
        load(rew_hbm, rew_ref, 10),
        load(len_hbm, len_ref, 11),
        load(ids_hbm, ids_ref, 12),
    ]

    barrier = pltpu.get_barrier_semaphore()
    for k in range(1, nt):
        pl.semaphore_signal(barrier, inc=1, device_id={"tensor": lax.rem(me_t + k, nt)}, device_id_type=MESH)
    for k in range(1, na):
        peer = lax.rem(me_h + k, na) * nb + me_l
        pl.semaphore_signal(barrier, inc=1, device_id={"dp": peer}, device_id_type=MESH)
    for k in range(1, nb):
        peer = me_h * nb + lax.rem(me_l + k, nb)
        pl.semaphore_signal(barrier, inc=1, device_id={"dp": peer}, device_id_type=MESH)

    @pl.when(me_p < npipe - 1)
    def _():
        pl.semaphore_signal(barrier, inc=1, device_id={"pipe": next_p}, device_id_type=MESH)

    @pl.when(me_p == 0)
    def _():
        pl.semaphore_signal(barrier, inc=1, device_id={"pipe": prev_p}, device_id_type=MESH)


    for item in small + loads:
        item.start()

    with scope("barrier"):
        along_pipe = jnp.where(me_p == 0, 0, jnp.where(me_p == npipe - 1, 2, 1))
        pl.semaphore_wait(barrier, nt - 1 + na - 1 + nb - 1 + along_pipe)

    @pl.when(me_p == npipe - 1)
    def _():
        pl.semaphore_signal(wrap_sem, inc=1, device_id={"pipe": next_p}, device_id_type=MESH)

    def to_tensor(src, dst_of, send_of, recv_of):
        return [
            pltpu.make_async_remote_copy(
                src_ref=src, dst_ref=dst_of(k - 1), send_sem=send_of(k - 1), recv_sem=recv_of(k - 1),
                device_id={"tensor": lax.rem(me_t + k, nt)}, device_id_type=MESH,
            )
            for k in range(1, nt)
        ]

    def to_dp(src_of, dst_of, send_of, recv_of, kind):
        out = []
        count = {"h": na, "l": nb}[kind]
        for k in range(1, count):
            if kind == "h":
                part = lax.rem(me_h + k, na)
                who = part * nb + me_l
            else:
                part = lax.rem(me_l + k, nb)
                who = me_h * nb + part
            out.append(
                pltpu.make_async_remote_copy(
                    src_ref=src_of(part), dst_ref=dst_of(k - 1), send_sem=send_of(k - 1), recv_sem=recv_of(k - 1),
                    device_id={"dp": who}, device_id_type=MESH,
                )
            )
        return out

    gather_kind = ("h", "l")
    split_kind = ("l", "h")
    count_of = {"h": na, "l": nb}
    xr = (xr0, xr1)
    gsr = (gsr0, gsr1)

    def x_copies(t, v):
        cols = pl.ds(0, GATHERED[v] * cc - EXTRA)
        return to_dp(
            lambda part: x_hbm.at[t, v, :, cols], lambda k: xr[v].at[k, t],
            lambda k: xg_s.at[v], lambda k: xg_r.at[v], gather_kind[v],
        )


    def stat_copies(kind):
        if kind == "l":
            return to_dp(lambda part: stl.at[0], lambda k: str_.at[k], lambda k: st_sem.at[0, k], lambda k: st_sem.at[1, k], kind)
        return to_dp(lambda part: stl.at[1], lambda k: str2.at[k], lambda k: st_sem.at[2, k], lambda k: st_sem.at[3, k], kind)

    def stats_first():
        lane8 = lax.broadcasted_iota(jnp.int32, (8, lanes), 1)
        row8 = lax.broadcasted_iota(jnp.int32, (8, lanes), 0)
        stats_own = jnp.where((row8 == 2) & (lane8 == unit_lane), 1.0, 0.0)
        for n in range(new_count):
            for k in range(seq_count):
                value = jnp.where(row8 == 0, rew_ref[n, 0, k], jnp.where(row8 == 1, 1.0, 0.0))
                stats_own = stats_own + jnp.where(lane8 == ids_ref[n, 0, k], value, 0.0)
        stl[0] = stats_own
        for item in stat_copies("l"):
            item.start()

    def stats_second():
        for item in stat_copies("l"):
            item.wait_recv()
        total = stl[0]
        for k in range(nb - 1):
            total = total + str_[k]
        stl[1] = total
        for item in stat_copies("h"):
            item.start()

    def start_gather(v, which):
        for t in which:
            for item in x_copies(t, v):
                item.start()

    lane = lax.broadcasted_iota(jnp.int32, (tok, 128), 1)

    groups = ((0, 1), (1, steps))

    def group_of(t):
        return 0 if t == 0 else 1

    def sq_copies(v, g):
        base = 2 * v + g
        return to_tensor(
            sqs.at[v, g], lambda k: sqr.at[k, v, g], lambda k: sq_s, lambda k: sq_r.at[base, k]
        )

    def prep(v, g):
        def body(t, squares_all):
            row = xs[t, v].astype(F32)
            gd[v, pl.ds(pl.multiple_of(t * tok, tok), tok), :] = (row * gn_ref[v]).astype(BF16)
            squares = jnp.sum(row * row, axis=-1, keepdims=True)
            return jnp.where(lane == t, squares, squares_all)

        sqs[v, g] = lax.fori_loop(*groups[g], body, jnp.zeros((tok, 128), F32))
        for item in sq_copies(v, g):
            item.start()

    def finish_sq(v, g):
        for item in sq_copies(v, g):
            item.wait_recv()
        total = sqs[v, g]
        for k in range(nt - 1):
            total = total + sqr[k, v, g]
        inv_t[v, g] = 1.0 / jnp.sqrt(total * (1.0 / full) + EPS)

    def share_of(v):
        count = count_of[split_kind[v]]
        if count % nt:
            return pl.ds(0, count)
        return pl.ds(me_t * (count // nt), count // nt)

    def gs_copies(t, v):
        cols = pl.ds(t * tok, tok)
        mine = share_of(v)
        source = (lambda part: gs_t.at[v, part, mine, :, cols]) if v == 0 else (lambda part: gs_t.at[v, mine, part, :, cols])
        return to_dp(
            source, lambda k: gsr[v].at[k, mine, :, cols],
            lambda k: gt_s.at[v], lambda k: gt_r.at[v], gather_kind[v],
        )

    def pass_copies(v):
        if count_of[split_kind[v]] % nt:
            return []
        out = []
        for k in range(count_of[gather_kind[v]] - 1):
            piece = gsr[v].at[k, share_of(v)]
            out += to_tensor(piece, lambda i: piece, lambda i: gf_s.at[v, k, i], lambda i: gf_r.at[v, k, i])
        return out

    def take_bytes(ref, sem):
        pltpu.make_async_copy(ref, ref, sem).wait()

    pre_copies = {}
    back_copies = {}

    def pre_part(v, g):
        low, high = groups[g]
        rows = pl.ds(low * tok, (high - low) * tok)

        def body(j, carry):
            cols = pl.ds(pl.multiple_of(j * rtile, rtile), rtile)
            ps[v, rows, cols] = dot_nt(gd[v, rows, :], wi[v, cols, :]).astype(BF16)
            return carry

        lax.fori_loop(0, rank // rtile, body, 0)
        base = 2 * v + g
        pre_copies[v, g] = to_tensor(
            ps.at[v, rows], lambda k: pr.at[k, v, rows], lambda k: pre_s, lambda k: pre_r.at[base, k]
        )
        for item in pre_copies[v, g]:
            item.start()

    def wait_pre(v, g):
        finish_sq(v, g)
        for item in pre_copies[v, g]:
            item.wait_recv()

    def cols_of(j):
        return pl.ds(j * cc, cc)

    def rows_of(h):
        return pl.ds(h * part_tok, part_tok)

    def back_part(t, v, h=None):
        rows = pl.ds(0, tok) if h is None else rows_of(h)

        def body(j, carry):
            cols = pl.ds(pl.multiple_of(j * rtile, rtile), rtile)
            bs[v, t, rows, cols] = dot_nt(ca[v, t, rows, :], wo[v, cols, :]).astype(BF16)
            return carry

        lax.fori_loop(0, rank // rtile, body, 0)
        base = v * (1 + (steps - 1) * PARTS) + (0 if h is None else 1 + (t - 1) * PARTS + h)
        back_copies[t, v, h] = to_tensor(
            bs.at[v, t, rows], lambda k: br.at[k, v, t, rows],
            lambda k: back_s, lambda k: back_r.at[base, k],
        )
        for item in back_copies[t, v, h]:
            item.start()

    def finish_pre(v, which_steps):
        for t in which_steps:
            rows = pl.ds(t * tok, tok)
            total = ps[v, rows, :].astype(F32)
            for k in range(nt - 1):
                total = total + pr[k, v, rows, :].astype(F32)
            pre = inv_t[v, group_of(t), :, t:t + 1] * total
            sigma = jax.nn.sigmoid(pre)
            presum[v, rows, :] = total
            hid_t[v, :, rows] = jnp.transpose(pre * sigma).astype(BF16)
            slope[v, rows, :] = sigma * (1.0 + pre * (1.0 - sigma))

    def wait_back(t, v, h=None):
        for item in back_copies[t, v, h]:
            item.wait_recv()

    def finish_back(t, v, h, send=True):
        own = rows_of(h)
        rows = pl.ds(t * tok + h * part_tok, part_tok)
        inv = inv_t[v, group_of(t), own, t:t + 1]
        total = bs[v, t, own, :].astype(F32)
        for k in range(nt - 1):
            total = total + br[k, v, t, own, :].astype(F32)
        grad_pre = total * slope[v, rows, :]
        gs[v, rows, :] = (inv * grad_pre).astype(BF16)
        radial = jnp.sum(grad_pre * presum[v, rows, :], axis=-1, keepdims=True)
        coef = inv * inv * inv * radial * (1.0 / full)

        def part(cols):
            lifted = jnp.dot(gs[v, rows, :], wi[v, :, cols], preferred_element_type=F32)
            out = (
                ca[v, t, own, cols].astype(F32)
                + gn_ref[v, :, cols] * lifted
                - xs[t, v, own, cols].astype(F32) * coef
            ).astype(BF16)
            if t < steps - 1:
                ob[t, v, own, cols] = out
            else:
                lv[v, own, cols] = out

        def body(j, carry):
            part(pl.ds(pl.multiple_of(j * tile, tile), tile))
            return carry

        if t < steps - 1 and len(pieces(steps, t, h)) > 1:
            for c in pieces(steps, t, h):
                part(cols_of(c))
                if send:
                    send_on(t, v, h, c)
        else:
            lax.fori_loop(0, wid // tile, body, 0)
            if t < steps - 1 and send:
                send_on(t, v, h, None)

    halves = range(PARTS)
    slots = pipe_slots(steps, vs)

    def finish_gs(t, v):
        rows = pl.ds(t * tok, tok)
        flipped = jnp.transpose(gs[v, rows, :].astype(F32)).astype(BF16)
        gs_t[v, :, :, :, rows] = flipped.reshape(na, nb, rc, tok)
        for item in gs_copies(t, v):
            item.start()

    def pipe_copy(t, v, slot, h, c):
        where = (rows_of(h),) if c is None else (rows_of(h), cols_of(c))
        return pltpu.make_async_remote_copy(
            src_ref=ob.at[(t, v) + where], dst_ref=ca.at[(slot, t + 1) + where],
            send_sem=pipe_s, recv_sem=pipe_r.at[slots[t, slot, h, c]],
            device_id={"pipe": prev_p}, device_id_type=MESH,
        )

    def send_on(t, v, h, c):
        @pl.when(me_p > 0)
        def _():
            pipe_copy(t, v, v, h, c).start()

        if v == 1:
            @pl.when(me_p == 0)
            def _():
                if t == 0 and h == 0 and c == pieces(steps, t, h)[0]:
                    pl.semaphore_wait(wrap_sem, 1)
                pipe_copy(t, 1, 0, h, c).start()

    def take(t, v, h, only=None):
        want = pieces(steps, t - 1, h)
        first = only is None or only == want[0]
        if only is not None:
            want = (only,)
        if v == 0:
            for c in want:
                pipe_copy(t - 1, v, v, h, c).wait_recv()
            return

        @pl.when(me_p < npipe - 1)
        def _():
            for c in want:
                pipe_copy(t - 1, v, v, h, c).wait_recv()

        if first:
            @pl.when(me_p == npipe - 1)
            def _():
                if t == 1 and h == 0:
                    for item in stat_copies("h"):
                        item.wait_recv()
                stats = stl[1]
                for k in range(na - 1):
                    stats = stats + str2[k]
                means = stats[0:1] / jnp.maximum(stats[1:2], 1.0) + stats[2:3] * (1.0 / ndp)
                tok_row = lax.broadcasted_iota(jnp.int32, (part_tok, lanes), 0) + h * part_tok
                tok_lane = lax.broadcasted_iota(jnp.int32, (part_tok, lanes), 1)
                hot = jnp.zeros((part_tok, lanes), F32)
                begin = 0
                for k in range(seq_count):
                    finish = begin + len_ref[t - 1, 0, k]
                    inside = (tok_row >= begin) & (tok_row < finish)
                    value = jnp.where(tok_lane == ids_ref[t - 1, 0, k], 1.0, 0.0)
                    value = value - jnp.where(tok_lane == unit_lane, rew_ref[t - 1, 0, k], 0.0)
                    hot = hot + jnp.where(inside, value, 0.0)
                    begin = finish
                weight = jnp.sum(hot * means, axis=-1, keepdims=True)
                ca[1, t, rows_of(h), :] = (weight * lp[t - 1, rows_of(h), :].astype(F32)).astype(BF16)

    jobs = reductions()

    def axes_of(job):
        what, v, j = job
        first = FIRST_AXIS[v][j] if what == "out" else IN_AXIS[v]
        return ("l", "h") if first == "l" else ("h", "l")

    def width_of(job):
        return cc if job[0] == "out" else cc + EXTRA

    def span_of(job):
        return cols_of(job[2]) if job[0] == "out" else pl.ds(wid - cc - EXTRA, cc + EXTRA)

    def split_copies(job):
        e = jobs[job]
        first, second = axes_of(job)
        count = count_of[second]
        lanes_of = pl.ds(0, width_of(job))
        kind = 0 if job[0] == "out" else 1
        source = (lambda part: gb.at[e, :, part, :, lanes_of]) if first == "l" else (lambda part: gb.at[e, part, :, :, lanes_of])
        return to_dp(
            source, lambda k: r1.at[e, k, pl.ds(0, count), :, lanes_of],
            lambda k: r1_s.at[kind], lambda k: r1_r.at[e, k], first,
        )

    def join_copies(job):
        e = jobs[job]
        lanes_of = pl.ds(0, width_of(job))
        kind = 0 if job[0] == "out" else 1
        return to_dp(
            lambda part: p2.at[e, part, :, lanes_of], lambda k: r2.at[e, k, :, lanes_of],
            lambda k: r2_s.at[kind], lambda k: r2_r.at[e, k], axes_of(job)[1],
        )

    def product(job):
        what, v, j = job
        e = jobs[job]
        if what == "out":
            value = jnp.dot(
                hid_t[v], ca[v, :, :, cols_of(j)].reshape(steps * tok, cc), preferred_element_type=F32
            )
        else:
            value = jnp.dot(
                gs_t[v].reshape(rank, steps * tok), xs[:, v, :, span_of(job)].reshape(steps * tok, width_of(job)),
                preferred_element_type=F32,
            ) * gn_ref[v, :, span_of(job)]
        gb[e, :, :, :, :width_of(job)] = value.astype(BF16).reshape(na, nb, rc, width_of(job))
        for item in split_copies(job):
            item.start()

    def middle(job):
        e = jobs[job]
        first, second = axes_of(job)
        count = count_of[second]
        for item in split_copies(job):
            item.wait_recv()
        w = width_of(job)
        own = gb[e, :, me_l, :, :w] if first == "l" else gb[e, me_h, :, :, :w]
        total = own.astype(F32)
        for k in range(count_of[first] - 1):
            total = total + r1[e, k, :count, :, :w].astype(F32)
        p2[e, :count, :, :w] = total.astype(BF16)
        for item in join_copies(job):
            item.start()

    scale = 1.0 / (ndp * tok)

    def final(job):
        what, v, j = job
        e = jobs[job]
        kind = axes_of(job)[1]
        for item in join_copies(job):
            item.wait_recv()
        w = width_of(job)
        total = p2[e, me_h if kind == "h" else me_l, :, :w].astype(F32)
        for k in range(count_of[kind] - 1):
            total = total + r2[e, k, :, :w].astype(F32)
        dest = fo if what == "out" else fi
        dest[v, :, span_of(job)] = total * scale

    def in_bytes(v):
        return r2i.at[v, pl.ds(0, count_of[split_kind[v]] - 1)]

    def in_cols(v, j):
        return pl.ds(j * cc, cc - EXTRA if j == GATHERED[v] - 1 else cc)

    def in_copies(v, j):
        cols = in_cols(v, j)
        return to_dp(
            lambda part: p2i.at[v, part, :, cols], lambda k: r2i.at[v, k, :, cols],
            lambda k: ri_s.at[v], lambda k: ri_r.at[v], split_kind[v],
        )

    def wait_gathered(v):
        take_bytes(gsr[v].at[:, share_of(v)], gt_r.at[v])
        for item in pass_copies(v):
            item.start()
        take_bytes(xr[v], xg_r.at[v])
        for item in pass_copies(v):
            item.wait_recv()

    def grad_in(v, which):
        width = count_of[split_kind[v]]
        own = gs_t[v, me_h] if v == 0 else gs_t[v, :, me_l]
        own = own.reshape(width * rc, steps * tok)
        for j in which:
            cols = in_cols(v, j)
            w = cols.size
            value = jnp.dot(own, xs[:, v, :, cols].reshape(steps * tok, w), preferred_element_type=F32)
            for k in range(count_of[gather_kind[v]] - 1):
                left = gsr[v][k].reshape(width * rc, steps * tok)
                value = value + jnp.dot(
                    left, xr[v][k, :, :, cols].reshape(steps * tok, w), preferred_element_type=F32
                )
            value = value * gn_ref[v, :, cols]
            p2i[v, :width, :, cols] = value.astype(BF16).reshape(width, rc, w)
            for item in in_copies(v, j):
                item.start()

    def final_in(v):
        take_bytes(in_bytes(v), ri_r.at[v])
        along_h = split_kind[v] == "h"
        for j in range(GATHERED[v]):
            cols = in_cols(v, j)
            total = p2i[v, me_h if along_h else me_l, :, cols].astype(F32)
            for k in range(count_of[split_kind[v]] - 1):
                total = total + r2i[v, k, :, cols].astype(F32)
            fi[v, :, cols] = total * scale

    last = steps - 1

    def back(t, v, h, during=None):
        with scope(f"back_{t}{v}{h}"):
            back_part(t, v, h)
            if during is not None:
                during()
            wait_back(t, v, h)
        with scope(f"fin_{t}{v}{h}"):
            finish_back(t, v, h)

    def step(t, v, h, during=None):
        with scope(f"take_{t}{v}{h}"):
            take(t, v, h)
        back(t, v, h, during)

    def products(v, which):
        for j in which:
            with scope(f"prod_{v}{j}"):
                take(last, v, PARTS - 1, j)
                product(("out", v, j))

    def rest(what, v):
        return range(GATHERED[v], CHUNKS) if what == "in" else range(GATHERED[v])

    with scope("stats"):
        for item in small:
            item.wait()
        start_gather(0, [0])
        stats_first()
        start_gather(1, range(steps))
    with scope("ld01"):
        loads[0].wait()
        loads[1].wait()
    with scope("first1"):
        back_part(0, 1)
        loads[2].wait()
        prep(1, 0)
        loads[3].wait()
        pre_part(1, 0)
        prep(1, 1)
        loads[4].wait()
        prep(0, 0)
    with scope("wpre1"):
        wait_pre(1, 0)
    with scope("fin1"):
        finish_pre(1, [0])
        wait_back(0, 1)
        for h in halves:
            finish_back(0, 1, h)
    with scope("first0"):
        finish_gs(0, 1)
        stats_second()
        start_gather(0, range(1, steps))
        pre_part(1, 1)
        prep(0, 1)
        loads[5].wait()
        loads[6].wait()
        back_part(0, 0)
        loads[7].wait()
        pre_part(0, 0)
        pre_part(0, 1)
        wait_pre(1, 1)
        finish_pre(1, range(1, steps))
    with scope("wpre0"):
        wait_pre(0, 0)
    with scope("fin0"):
        finish_pre(0, [0])
        wait_back(0, 0)
        for h in halves:
            finish_back(0, 0, h, send=False)
        finish_gs(0, 0)
        wait_pre(0, 1)
        finish_pre(0, range(1, steps))
        loads[8].wait()

    for t in range(1, last):
        for h in halves:
            step(t, 1, h)
        if t == 1:
            for h in halves:
                for c in pieces(steps, 0, h):
                    send_on(0, 0, h, c)
        finish_gs(t, 1)
    for h in halves[:-1]:
        step(last, 1, h)
    def end_products(v):
        ahead = 2 + v
        products(v, ORDER[:ahead])
        for j in ORDER[ahead:]:
            take(last, v, PARTS - 1, j)
        back(last, v, PARTS - 1)
        with scope(f"gout{v}"):
            finish_gs(last, v)
            for j in ORDER[ahead:]:
                product(("out", v, j))
            for j in rest("in", v):
                product(("in", v, j))

    end_products(1)

    def first_middles():
        middle(("out", 1, 2))

    for t in range(1, last):
        for h in halves:
            ending = t == last - 1
            step(t, 0, h, first_middles if ending and h == 0 else None)
            if ending and h == 0:
                with scope("wgat1"):
                    wait_gathered(1)
                with scope("gin1"):
                    grad_in(1, rest("out", 1))
                    middle(("out", 1, 3))
        finish_gs(t, 0)
    with scope("mid1"):
        middle(("out", 1, 0))
        middle(("out", 1, 1))
    for h in halves[:-1]:
        step(last, 0, h)
    end_products(0)
    with scope("midi1"):
        for j in rest("in", 1):
            middle(("in", 1, j))
    with scope("mid0_3"):
        middle(("out", 0, 3))
    with scope("wgat0"):
        wait_gathered(0)
    with scope("gin0"):
        grad_in(0, rest("out", 0))
    with scope("final1a"):
        for j in (2, 3, 0, 1):
            final(("out", 1, j))
        final_in(1)
    with scope("mid0_0"):
        middle(("out", 0, 0))
    with scope("mid0_2"):
        middle(("out", 0, 2))

    @pl.when(me_p < npipe - 1)
    def _():
        for item in stat_copies("h"):
            item.wait_recv()

    with scope("drain"):
        for item in stat_copies("l") + stat_copies("h"):
            item.wait_send()
        take_bytes(sqr, sq_s)
        take_bytes(pr, pre_s)
        take_bytes(br, back_s)

        @pl.when(me_p > 0)
        def _():
            take_bytes(ob, pipe_s)

        @pl.when(me_p == 0)
        def _():
            take_bytes(ob.at[:, 1], pipe_s)

        for v in range(vs):
            take_bytes(xr[v], xg_s.at[v])
            take_bytes(gsr[v].at[:, share_of(v)], gt_s.at[v])
            for item in pass_copies(v):
                item.wait_send()

    with scope("mid0_1"):
        middle(("out", 0, 1))
    with scope("midi0"):
        for j in rest("in", 0):
            middle(("in", 0, j))
    with scope("final0i"):
        final_in(0)
    with scope("final1b"):
        for j in rest("in", 1):
            final(("in", 1, j))
    for v in range(vs):
        take_bytes(in_bytes(v), ri_s.at[v])

    outs = vs * CHUNKS

    def drain_split(copies, landed, sem):
        if na == nb:
            rows = (slice(None),) * (len(landed.shape) - 2)
            take_bytes(landed.at[(pl.ds(0, outs),) + rows + (pl.ds(0, cc),)], sem.at[0])
            take_bytes(landed.at[(pl.ds(outs, len(jobs) - outs),) + rows + (pl.ds(0, cc + EXTRA),)], sem.at[1])
        else:
            for job in jobs:
                for item in copies(job):
                    item.wait_send()

    drain_split(split_copies, r1, r1_s)
    for j in (3, 0, 1, 2):
        with scope(f"fin0_{j}"):
            final(("out", 0, j))
    with scope("fini0"):
        for j in rest("in", 0):
            final(("in", 0, j))
    with scope("tail"):
        drain_split(join_copies, r2, r2_s)


def store(a, b, c, a_out, b_out, c_out, sem):
    pairs = ((a, a_out), (b, b_out), (c, c_out))
    for k, (src, dst) in enumerate(pairs):
        rows = src.shape[1] // 2
        for v in range(src.shape[0]):
            for r in range(2):
                where = (v, pl.ds(r * rows, rows))
                pltpu.make_async_copy(src.at[where], dst.at[where], sem.at[k]).start()
    for k, pair in enumerate(pairs):
        pltpu.make_async_copy(*pair, sem.at[k]).wait()


def shards(
    saved_inputs, proj_in, proj_out, norm_gain, arriving, logp_grad, rewards, seq_lengths, group_ids
):
    nt = lax.axis_size("tensor")
    npipe = lax.axis_size("pipe")
    ndp = lax.axis_size("dp")
    steps, vs, _, tok, wid = saved_inputs.shape
    rank = proj_in.shape[2]
    new_count = logp_grad.shape[0]
    group_count = new_count * ndp * rewards.shape[2] // 8
    lanes = -(-(group_count + 1) // 128) * 128
    na, nb = factors(ndp)
    rc = rank // ndp
    cc = wid // CHUNKS
    jobs = len(reductions())
    pipe_count = len(pipe_slots(steps, vs))
    hm, lm = max(na - 1, 1), max(nb - 1, 1)
    dims = (steps, vs, tok, wid, rank, nt, npipe, ndp)
    peers = max(nt - 1, 1)
    any_spec = pl.BlockSpec(memory_space=pl.ANY)
    vmem = pl.BlockSpec(memory_space=pltpu.VMEM)
    V = pltpu.VMEM
    DMA = pltpu.SemaphoreType.DMA
    pmax = max(na, nb)
    less = max(pmax - 1, 1)
    scratch = [
        V((steps, vs, tok, wid), BF16),
        V((vs, steps * tok, wid), BF16),
        V((vs, steps, tok, wid), BF16),
        V((vs, rank, wid), BF16),
        V((vs, rank, wid), BF16),
        V((new_count, tok, wid), BF16),
        V((vs, steps * tok, rank), BF16),
        V((peers, vs, steps * tok, rank), BF16),
        V((vs, steps * tok, rank), F32),
        V((vs, steps * tok, rank), F32),
        V((vs, rank, steps * tok), BF16),
        V((vs, steps * tok, rank), BF16),
        V((vs, na, nb, rc, steps * tok), BF16),
        V((hm, nb, rc, steps * tok), BF16),
        V((lm, na, rc, steps * tok), BF16),
        V((hm, steps, tok, GATHERED[0] * cc - EXTRA), BF16),
        V((lm, steps, tok, GATHERED[1] * cc - EXTRA), BF16),
        V((vs, steps, tok, rank), BF16),
        V((peers, vs, steps, tok, rank), BF16),
        V((steps - 1, vs, tok, wid), BF16),
        V((vs, 2, tok, 128), F32),
        V((peers, vs, 2, tok, 128), F32),
        V((vs, 2, tok, 128), F32),
        V((2, 8, lanes), F32),
        V((lm, 8, lanes), F32),
        V((jobs, na, nb, rc, cc + max(EXTRA, 0)), BF16),
        V((jobs, less, pmax, rc, cc + max(EXTRA, 0)), BF16),
        V((jobs, pmax, rc, cc + max(EXTRA, 0)), BF16),
        V((jobs, less, rc, cc + max(EXTRA, 0)), BF16),
        V((vs, pmax, rc, wid - cc - EXTRA), BF16),
        V((vs, less, rc, wid - cc - EXTRA), BF16),
        V(norm_gain.shape, F32),
        pltpu.SMEM(rewards.shape, F32),
        pltpu.SMEM(seq_lengths.shape, jnp.int32),
        pltpu.SMEM(group_ids.shape, jnp.int32),
        V((hm, 8, lanes), F32),
        pltpu.SemaphoreType.REGULAR,
        DMA((13,)),
        DMA,
        DMA((2 * vs, peers)),
        DMA((4, less)),
        DMA,
        DMA((2 * vs, peers)),
        DMA,
        DMA((vs * (1 + (steps - 1) * PARTS), peers)),
        DMA,
        DMA((pipe_count,)),
        DMA((vs,)),
        DMA((vs,)),
        DMA((vs,)),
        DMA((vs,)),
        DMA((vs, less, peers)),
        DMA((vs, less, peers)),
        DMA((2,)),
        DMA((jobs, less)),
        DMA((2,)),
        DMA((jobs, less)),
        DMA((vs,)),
        DMA((vs,)),
    ]
    grad_in, grad_out, leaving = pl.pallas_call(
        functools.partial(kernel, dims),
        out_shape=(
            V((vs, rc, wid), F32),
            V((vs, rc, wid), F32),
            V((vs, tok, wid), BF16),
        ),
        in_specs=[any_spec] * 9,
        out_specs=(vmem, vmem, vmem),
        scratch_shapes=scratch,
        compiler_params=pltpu.CompilerParams(
            collective_id=0, has_side_effects=True, vmem_limit_bytes=58 * 1024 * 1024
        ),
    )(
        saved_inputs[:, :, 0], proj_in[:, 0], proj_out[:, 0], norm_gain, arriving[:, 0], logp_grad,
        rewards, seq_lengths, group_ids,
    )
    grad_in, grad_out, leaving = pl.pallas_call(
        store,
        out_shape=tuple(jax.ShapeDtypeStruct(a.shape, a.dtype) for a in (grad_in, grad_out, leaving)),
        in_specs=[vmem] * 3,
        out_specs=[any_spec] * 3,
        scratch_shapes=[DMA((3,))],
        compiler_params=pltpu.CompilerParams(vmem_limit_bytes=1024 * 1024),
    )(grad_in, grad_out, leaving)
    return grad_in[:, None], grad_out[:, None], leaving[:, None]


def solution(mesh):
    return jax.shard_map(
        shards,
        mesh=mesh,
        in_specs=(
            P(None, None, "pipe", "dp", "tensor"),
            P(None, "pipe", None, "tensor"),
            P(None, "pipe", None, "tensor"),
            P(None, "pipe", "tensor"),
            P(None, "pipe", "dp", "tensor"),
            P(None, "dp", "tensor"),
            P(None, "dp", None),
            P(None, "dp", None),
            P(None, "dp", None),
        ),
        out_specs=(
            P(None, "pipe", "dp", "tensor"),
            P(None, "pipe", "dp", "tensor"),
            P(None, "pipe", "dp", "tensor"),
        ),
        check_vma=False,
    )
```

```python
import functools

import jax
import jax.numpy as jnp
from jax import lax
from jax.experimental import pallas as pl
from jax.experimental.pallas import tpu as pltpu
from jax.sharding import PartitionSpec as P

EPS = 1e-05
MESH = pl.DeviceIdType.MESH
F32 = jnp.float32
BF16 = jnp.bfloat16


def dot_nt(a, b):
    return lax.dot_general(a, b, (((1,), (1,)), ((), ())), preferred_element_type=F32)


def factors(n):
    low = 1
    for k in range(1, n + 1):
        if n % k == 0 and k * k <= n:
            low = k
    return low, n // low


CHUNKS = 4
GATHERED = (3, 3)
EXTRA = -128
PARTS = 2
FIRST_AXIS = ("hhll", "hllh")
IN_AXIS = ("h", "l")
ORDER = (3, 2, 0, 1)
scope = jax.named_scope


def reductions():
    jobs = [("out", v, j) for v in (1, 0) for j in range(CHUNKS)]
    jobs += [("in", v, j) for v in (1, 0) for j in range(GATHERED[v], CHUNKS)]
    return {job: e for e, job in enumerate(jobs)}


def pieces(steps, t, h):
    return ORDER if (t, h) in ((0, 0), (steps - 2, PARTS - 1)) else (None,)


def pipe_slots(steps, vs):
    keys = [(t, v, h, c) for t in range(steps - 1) for v in range(vs) for h in range(PARTS) for c in pieces(steps, t, h)]
    names = list(dict.fromkeys(shared_key(steps, key) for key in keys))
    return {key: names.index(shared_key(steps, key)) for key in keys}


def shared_key(steps, key):
    t, v, h, c = key
    return key if (t, h) == (steps - 2, PARTS - 1) else (t, v, h, None)


def kernel(
    dims,
    x_hbm, wi_hbm, wo_hbm, gn_hbm, ar_hbm, lp_hbm, rew_hbm, len_hbm, ids_hbm,
    fi, fo, lv,
    xs, gd, ca, wi, wo, lp, ps, pr, presum, slope, hid_t, gs, gs_t, gsr0, gsr1, xr0, xr1, bs, br, ob,
    sqs, sqr, inv_t, stl, str_, gb, r1, p2, r2, p2i, r2i,
    gn_ref, rew_ref, len_ref, ids_ref, str2, wrap_sem,
    in_sem, sq_s, sq_r, st_sem, pre_s, pre_r, back_s, back_r, pipe_s, pipe_r, xg_s, xg_r, gt_s, gt_r, gf_s, gf_r,
    r1_s, r1_r, r2_s, r2_r, ri_s, ri_r,
):
    steps, vs, tok, wid, rank, nt, npipe, ndp = dims
    na, nb = factors(ndp)
    rc = rank // ndp
    full = wid * nt
    tile = min(512, wid // 2)
    rtile = min(512, rank)
    cc = wid // CHUNKS
    part_tok = tok // PARTS
    lanes = stl.shape[2]
    new_count, _, seq_count = rew_ref.shape
    unit_lane = new_count * ndp * seq_count // 8
    me_t = lax.axis_index("tensor")
    me_p = lax.axis_index("pipe")
    me_d = lax.axis_index("dp")
    me_h = me_d // nb
    me_l = me_d % nb
    prev_p = lax.rem(me_p + npipe - 1, npipe)
    next_p = lax.rem(me_p + 1, npipe)

    def load(src, dst, k):
        return pltpu.make_async_copy(src, dst, in_sem.at[k])

    loads = [
        load(ar_hbm.at[1], ca.at[1, 0], 0),
        load(wo_hbm.at[1], wo.at[1], 1),
        load(x_hbm.at[:, 1], xs.at[:, 1], 2),
        load(wi_hbm.at[1], wi.at[1], 3),
        load(x_hbm.at[:, 0], xs.at[:, 0], 4),
        load(ar_hbm.at[0], ca.at[0, 0], 5),
        load(wo_hbm.at[0], wo.at[0], 6),
        load(wi_hbm.at[0], wi.at[0], 7),
        load(lp_hbm, lp, 8),
    ]
    small = [
        load(gn_hbm, gn_ref, 9),
        load(rew_hbm, rew_ref, 10),
        load(len_hbm, len_ref, 11),
        load(ids_hbm, ids_ref, 12),
    ]

    barrier = pltpu.get_barrier_semaphore()
    for k in range(1, nt):
        pl.semaphore_signal(barrier, inc=1, device_id={"tensor": lax.rem(me_t + k, nt)}, device_id_type=MESH)
    for k in range(1, na):
        peer = lax.rem(me_h + k, na) * nb + me_l
        pl.semaphore_signal(barrier, inc=1, device_id={"dp": peer}, device_id_type=MESH)
    for k in range(1, nb):
        peer = me_h * nb + lax.rem(me_l + k, nb)
        pl.semaphore_signal(barrier, inc=1, device_id={"dp": peer}, device_id_type=MESH)

    @pl.when(me_p < npipe - 1)
    def _():
        pl.semaphore_signal(barrier, inc=1, device_id={"pipe": next_p}, device_id_type=MESH)

    @pl.when(me_p == 0)
    def _():
        pl.semaphore_signal(barrier, inc=1, device_id={"pipe": prev_p}, device_id_type=MESH)


    for item in small + loads:
        item.start()

    with scope("barrier"):
        along_pipe = jnp.where(me_p == 0, 0, jnp.where(me_p == npipe - 1, 2, 1))
        pl.semaphore_wait(barrier, nt - 1 + na - 1 + nb - 1 + along_pipe)

    @pl.when(me_p == npipe - 1)
    def _():
        pl.semaphore_signal(wrap_sem, inc=1, device_id={"pipe": next_p}, device_id_type=MESH)

    def to_tensor(src, dst_of, send_of, recv_of):
        return [
            pltpu.make_async_remote_copy(
                src_ref=src, dst_ref=dst_of(k - 1), send_sem=send_of(k - 1), recv_sem=recv_of(k - 1),
                device_id={"tensor": lax.rem(me_t + k, nt)}, device_id_type=MESH,
            )
            for k in range(1, nt)
        ]

    def to_dp(src_of, dst_of, send_of, recv_of, kind):
        out = []
        count = {"h": na, "l": nb}[kind]
        for k in range(1, count):
            if kind == "h":
                part = lax.rem(me_h + k, na)
                who = part * nb + me_l
            else:
                part = lax.rem(me_l + k, nb)
                who = me_h * nb + part
            out.append(
                pltpu.make_async_remote_copy(
                    src_ref=src_of(part), dst_ref=dst_of(k - 1), send_sem=send_of(k - 1), recv_sem=recv_of(k - 1),
                    device_id={"dp": who}, device_id_type=MESH,
                )
            )
        return out

    gather_kind = ("h", "l")
    split_kind = ("l", "h")
    count_of = {"h": na, "l": nb}
    xr = (xr0, xr1)
    gsr = (gsr0, gsr1)

    def x_copies(t, v):
        cols = pl.ds(0, GATHERED[v] * cc - EXTRA)
        return to_dp(
            lambda part: x_hbm.at[t, v, :, cols], lambda k: xr[v].at[k, t],
            lambda k: xg_s.at[v], lambda k: xg_r.at[v], gather_kind[v],
        )


    def stat_copies(kind):
        if kind == "l":
            return to_dp(lambda part: stl.at[0], lambda k: str_.at[k], lambda k: st_sem.at[0, k], lambda k: st_sem.at[1, k], kind)
        return to_dp(lambda part: stl.at[1], lambda k: str2.at[k], lambda k: st_sem.at[2, k], lambda k: st_sem.at[3, k], kind)

    def stats_first():
        lane8 = lax.broadcasted_iota(jnp.int32, (8, lanes), 1)
        row8 = lax.broadcasted_iota(jnp.int32, (8, lanes), 0)
        stats_own = jnp.where((row8 == 2) & (lane8 == unit_lane), 1.0, 0.0)
        for n in range(new_count):
            for k in range(seq_count):
                value = jnp.where(row8 == 0, rew_ref[n, 0, k], jnp.where(row8 == 1, 1.0, 0.0))
                stats_own = stats_own + jnp.where(lane8 == ids_ref[n, 0, k], value, 0.0)
        stl[0] = stats_own
        for item in stat_copies("l"):
            item.start()

    def stats_second():
        for item in stat_copies("l"):
            item.wait_recv()
        total = stl[0]
        for k in range(nb - 1):
            total = total + str_[k]
        stl[1] = total
        for item in stat_copies("h"):
            item.start()

    def start_gather(v, which):
        for t in which:
            for item in x_copies(t, v):
                item.start()

    lane = lax.broadcasted_iota(jnp.int32, (tok, 128), 1)

    groups = ((0, 1), (1, steps))

    def group_of(t):
        return 0 if t == 0 else 1

    def sq_copies(v, g):
        base = 2 * v + g
        return to_tensor(
            sqs.at[v, g], lambda k: sqr.at[k, v, g], lambda k: sq_s, lambda k: sq_r.at[base, k]
        )

    def prep(v, g):
        def body(t, squares_all):
            row = xs[t, v].astype(F32)
            gd[v, pl.ds(pl.multiple_of(t * tok, tok), tok), :] = (row * gn_ref[v]).astype(BF16)
            squares = jnp.sum(row * row, axis=-1, keepdims=True)
            return jnp.where(lane == t, squares, squares_all)

        sqs[v, g] = lax.fori_loop(*groups[g], body, jnp.zeros((tok, 128), F32))
        for item in sq_copies(v, g):
            item.start()

    def finish_sq(v, g):
        for item in sq_copies(v, g):
            item.wait_recv()
        total = sqs[v, g]
        for k in range(nt - 1):
            total = total + sqr[k, v, g]
        inv_t[v, g] = 1.0 / jnp.sqrt(total * (1.0 / full) + EPS)

    def share_of(v):
        count = count_of[split_kind[v]]
        if count % nt:
            return pl.ds(0, count)
        return pl.ds(me_t * (count // nt), count // nt)

    def gs_copies(t, v):
        cols = pl.ds(t * tok, tok)
        mine = share_of(v)
        source = (lambda part: gs_t.at[v, part, mine, :, cols]) if v == 0 else (lambda part: gs_t.at[v, mine, part, :, cols])
        return to_dp(
            source, lambda k: gsr[v].at[k, mine, :, cols],
            lambda k: gt_s.at[v], lambda k: gt_r.at[v], gather_kind[v],
        )

    def pass_copies(v):
        if count_of[split_kind[v]] % nt:
            return []
        out = []
        for k in range(count_of[gather_kind[v]] - 1):
            piece = gsr[v].at[k, share_of(v)]
            out += to_tensor(piece, lambda i: piece, lambda i: gf_s.at[v, k, i], lambda i: gf_r.at[v, k, i])
        return out

    def take_bytes(ref, sem):
        pltpu.make_async_copy(ref, ref, sem).wait()

    pre_copies = {}
    back_copies = {}

    def pre_part(v, g):
        low, high = groups[g]
        rows = pl.ds(low * tok, (high - low) * tok)

        def body(j, carry):
            cols = pl.ds(pl.multiple_of(j * rtile, rtile), rtile)
            ps[v, rows, cols] = dot_nt(gd[v, rows, :], wi[v, cols, :]).astype(BF16)
            return carry

        lax.fori_loop(0, rank // rtile, body, 0)
        base = 2 * v + g
        pre_copies[v, g] = to_tensor(
            ps.at[v, rows], lambda k: pr.at[k, v, rows], lambda k: pre_s, lambda k: pre_r.at[base, k]
        )
        for item in pre_copies[v, g]:
            item.start()

    def wait_pre(v, g):
        finish_sq(v, g)
        for item in pre_copies[v, g]:
            item.wait_recv()

    def cols_of(j):
        return pl.ds(j * cc, cc)

    def rows_of(h):
        return pl.ds(h * part_tok, part_tok)

    def back_part(t, v, h=None):
        rows = pl.ds(0, tok) if h is None else rows_of(h)

        def body(j, carry):
            cols = pl.ds(pl.multiple_of(j * rtile, rtile), rtile)
            bs[v, t, rows, cols] = dot_nt(ca[v, t, rows, :], wo[v, cols, :]).astype(BF16)
            return carry

        lax.fori_loop(0, rank // rtile, body, 0)
        base = v * (1 + (steps - 1) * PARTS) + (0 if h is None else 1 + (t - 1) * PARTS + h)
        back_copies[t, v, h] = to_tensor(
            bs.at[v, t, rows], lambda k: br.at[k, v, t, rows],
            lambda k: back_s, lambda k: back_r.at[base, k],
        )
        for item in back_copies[t, v, h]:
            item.start()

    def finish_pre(v, which_steps):
        for t in which_steps:
            rows = pl.ds(t * tok, tok)
            total = ps[v, rows, :].astype(F32)
            for k in range(nt - 1):
                total = total + pr[k, v, rows, :].astype(F32)
            pre = inv_t[v, group_of(t), :, t:t + 1] * total
            sigma = jax.nn.sigmoid(pre)
            presum[v, rows, :] = total
            hid_t[v, :, rows] = jnp.transpose(pre * sigma).astype(BF16)
            slope[v, rows, :] = sigma * (1.0 + pre * (1.0 - sigma))

    def wait_back(t, v, h=None):
        for item in back_copies[t, v, h]:
            item.wait_recv()

    def finish_back(t, v, h, send=True):
        own = rows_of(h)
        rows = pl.ds(t * tok + h * part_tok, part_tok)
        inv = inv_t[v, group_of(t), own, t:t + 1]
        total = bs[v, t, own, :].astype(F32)
        for k in range(nt - 1):
            total = total + br[k, v, t, own, :].astype(F32)
        grad_pre = total * slope[v, rows, :]
        gs[v, rows, :] = (inv * grad_pre).astype(BF16)
        radial = jnp.sum(grad_pre * presum[v, rows, :], axis=-1, keepdims=True)
        coef = inv * inv * inv * radial * (1.0 / full)

        def part(cols):
            lifted = jnp.dot(gs[v, rows, :], wi[v, :, cols], preferred_element_type=F32)
            out = (
                ca[v, t, own, cols].astype(F32)
                + gn_ref[v, :, cols] * lifted
                - xs[t, v, own, cols].astype(F32) * coef
            ).astype(BF16)
            if t < steps - 1:
                ob[t, v, own, cols] = out
            else:
                lv[v, own, cols] = out

        def body(j, carry):
            part(pl.ds(pl.multiple_of(j * tile, tile), tile))
            return carry

        if t < steps - 1 and len(pieces(steps, t, h)) > 1:
            for c in pieces(steps, t, h):
                part(cols_of(c))
                if send:
                    send_on(t, v, h, c)
        else:
            lax.fori_loop(0, wid // tile, body, 0)
            if t < steps - 1 and send:
                send_on(t, v, h, None)

    halves = range(PARTS)
    slots = pipe_slots(steps, vs)

    def finish_gs(t, v):
        rows = pl.ds(t * tok, tok)
        flipped = jnp.transpose(gs[v, rows, :].astype(F32)).astype(BF16)
        gs_t[v, :, :, :, rows] = flipped.reshape(na, nb, rc, tok)
        for item in gs_copies(t, v):
            item.start()

    def pipe_copy(t, v, slot, h, c):
        where = (rows_of(h),) if c is None else (rows_of(h), cols_of(c))
        return pltpu.make_async_remote_copy(
            src_ref=ob.at[(t, v) + where], dst_ref=ca.at[(slot, t + 1) + where],
            send_sem=pipe_s, recv_sem=pipe_r.at[slots[t, slot, h, c]],
            device_id={"pipe": prev_p}, device_id_type=MESH,
        )

    def send_on(t, v, h, c):
        @pl.when(me_p > 0)
        def _():
            pipe_copy(t, v, v, h, c).start()

        if v == 1:
            @pl.when(me_p == 0)
            def _():
                if t == 0 and h == 0 and c == pieces(steps, t, h)[0]:
                    pl.semaphore_wait(wrap_sem, 1)
                pipe_copy(t, 1, 0, h, c).start()

    def take(t, v, h, only=None):
        want = pieces(steps, t - 1, h)
        first = only is None or only == want[0]
        if only is not None:
            want = (only,)
        together = (t - 1, h) != (steps - 2, PARTS - 1)

        def arrive():
            if together:
                take_bytes(ca.at[v, t, rows_of(h)], pipe_r.at[slots[t - 1, v, h, want[0]]])
            else:
                for c in want:
                    pipe_copy(t - 1, v, v, h, c).wait_recv()

        if v == 0:
            arrive()
            return

        @pl.when(me_p < npipe - 1)
        def _():
            arrive()

        if first:
            @pl.when(me_p == npipe - 1)
            def _():
                if t == 1 and h == 0:
                    for item in stat_copies("h"):
                        item.wait_recv()
                stats = stl[1]
                for k in range(na - 1):
                    stats = stats + str2[k]
                means = stats[0:1] / jnp.maximum(stats[1:2], 1.0) + stats[2:3] * (1.0 / ndp)
                tok_row = lax.broadcasted_iota(jnp.int32, (part_tok, lanes), 0) + h * part_tok
                tok_lane = lax.broadcasted_iota(jnp.int32, (part_tok, lanes), 1)
                hot = jnp.zeros((part_tok, lanes), F32)
                begin = 0
                for k in range(seq_count):
                    finish = begin + len_ref[t - 1, 0, k]
                    inside = (tok_row >= begin) & (tok_row < finish)
                    value = jnp.where(tok_lane == ids_ref[t - 1, 0, k], 1.0, 0.0)
                    value = value - jnp.where(tok_lane == unit_lane, rew_ref[t - 1, 0, k], 0.0)
                    hot = hot + jnp.where(inside, value, 0.0)
                    begin = finish
                weight = jnp.sum(hot * means, axis=-1, keepdims=True)
                ca[1, t, rows_of(h), :] = (weight * lp[t - 1, rows_of(h), :].astype(F32)).astype(BF16)

    jobs = reductions()

    def axes_of(job):
        what, v, j = job
        first = FIRST_AXIS[v][j] if what == "out" else IN_AXIS[v]
        return ("l", "h") if first == "l" else ("h", "l")

    def width_of(job):
        return cc if job[0] == "out" else cc + EXTRA

    def span_of(job):
        return cols_of(job[2]) if job[0] == "out" else pl.ds(wid - cc - EXTRA, cc + EXTRA)

    def split_copies(job):
        e = jobs[job]
        first, second = axes_of(job)
        count = count_of[second]
        lanes_of = pl.ds(0, width_of(job))
        kind = 0 if job[0] == "out" else 1
        source = (lambda part: gb.at[e, :, part, :, lanes_of]) if first == "l" else (lambda part: gb.at[e, part, :, :, lanes_of])
        return to_dp(
            source, lambda k: r1.at[e, k, pl.ds(0, count), :, lanes_of],
            lambda k: r1_s.at[kind], lambda k: r1_r.at[e, k], first,
        )

    def join_copies(job):
        e = jobs[job]
        lanes_of = pl.ds(0, width_of(job))
        kind = 0 if job[0] == "out" else 1
        return to_dp(
            lambda part: p2.at[e, part, :, lanes_of], lambda k: r2.at[e, k, :, lanes_of],
            lambda k: r2_s.at[kind], lambda k: r2_r.at[e, k], axes_of(job)[1],
        )

    def product(job):
        what, v, j = job
        e = jobs[job]
        if what == "out":
            value = jnp.dot(
                hid_t[v], ca[v, :, :, cols_of(j)].reshape(steps * tok, cc), preferred_element_type=F32
            )
        else:
            value = jnp.dot(
                gs_t[v].reshape(rank, steps * tok), xs[:, v, :, span_of(job)].reshape(steps * tok, width_of(job)),
                preferred_element_type=F32,
            ) * gn_ref[v, :, span_of(job)]
        gb[e, :, :, :, :width_of(job)] = value.astype(BF16).reshape(na, nb, rc, width_of(job))
        for item in split_copies(job):
            item.start()

    def middle(job):
        e = jobs[job]
        first, second = axes_of(job)
        count = count_of[second]
        for item in split_copies(job):
            item.wait_recv()
        w = width_of(job)
        own = gb[e, :, me_l, :, :w] if first == "l" else gb[e, me_h, :, :, :w]
        total = own.astype(F32)
        for k in range(count_of[first] - 1):
            total = total + r1[e, k, :count, :, :w].astype(F32)
        p2[e, :count, :, :w] = total.astype(BF16)
        for item in join_copies(job):
            item.start()

    scale = 1.0 / (ndp * tok)

    def final(job):
        what, v, j = job
        e = jobs[job]
        kind = axes_of(job)[1]
        for item in join_copies(job):
            item.wait_recv()
        w = width_of(job)
        total = p2[e, me_h if kind == "h" else me_l, :, :w].astype(F32)
        for k in range(count_of[kind] - 1):
            total = total + r2[e, k, :, :w].astype(F32)
        dest = fo if what == "out" else fi
        dest[v, :, span_of(job)] = total * scale

    def in_bytes(v):
        return r2i.at[v, pl.ds(0, count_of[split_kind[v]] - 1)]

    def in_cols(v, j):
        return pl.ds(j * cc, cc - EXTRA if j == GATHERED[v] - 1 else cc)

    def in_copies(v, j):
        cols = in_cols(v, j)
        return to_dp(
            lambda part: p2i.at[v, part, :, cols], lambda k: r2i.at[v, k, :, cols],
            lambda k: ri_s.at[v], lambda k: ri_r.at[v], split_kind[v],
        )

    def wait_gathered(v):
        take_bytes(gsr[v].at[:, share_of(v)], gt_r.at[v])
        for item in pass_copies(v):
            item.start()
        take_bytes(xr[v], xg_r.at[v])
        for item in pass_copies(v):
            item.wait_recv()

    def grad_in(v, which):
        width = count_of[split_kind[v]]
        own = gs_t[v, me_h] if v == 0 else gs_t[v, :, me_l]
        own = own.reshape(width * rc, steps * tok)
        for j in which:
            cols = in_cols(v, j)
            w = cols.size
            value = jnp.dot(own, xs[:, v, :, cols].reshape(steps * tok, w), preferred_element_type=F32)
            for k in range(count_of[gather_kind[v]] - 1):
                left = gsr[v][k].reshape(width * rc, steps * tok)
                value = value + jnp.dot(
                    left, xr[v][k, :, :, cols].reshape(steps * tok, w), preferred_element_type=F32
                )
            value = value * gn_ref[v, :, cols]
            p2i[v, :width, :, cols] = value.astype(BF16).reshape(width, rc, w)
            for item in in_copies(v, j):
                item.start()

    def final_in(v):
        take_bytes(in_bytes(v), ri_r.at[v])
        along_h = split_kind[v] == "h"
        for j in range(GATHERED[v]):
            cols = in_cols(v, j)
            total = p2i[v, me_h if along_h else me_l, :, cols].astype(F32)
            for k in range(count_of[split_kind[v]] - 1):
                total = total + r2i[v, k, :, cols].astype(F32)
            fi[v, :, cols] = total * scale

    last = steps - 1

    def back(t, v, h, during=None):
        with scope(f"back_{t}{v}{h}"):
            back_part(t, v, h)
            if during is not None:
                during()
            wait_back(t, v, h)
        with scope(f"fin_{t}{v}{h}"):
            finish_back(t, v, h)

    def step(t, v, h, during=None):
        with scope(f"take_{t}{v}{h}"):
            take(t, v, h)
        back(t, v, h, during)

    def products(v, which):
        for j in which:
            with scope(f"prod_{v}{j}"):
                take(last, v, PARTS - 1, j)
                product(("out", v, j))

    def rest(what, v):
        return range(GATHERED[v], CHUNKS) if what == "in" else range(GATHERED[v])

    with scope("stats"):
        for item in small:
            item.wait()
        start_gather(0, [0])
        stats_first()
        start_gather(1, range(steps))
    with scope("ld01"):
        loads[0].wait()
        loads[1].wait()
    with scope("first1"):
        back_part(0, 1)
        loads[2].wait()
        prep(1, 0)
        loads[3].wait()
        pre_part(1, 0)
        prep(1, 1)
        loads[4].wait()
        prep(0, 0)
    with scope("wpre1"):
        wait_pre(1, 0)
    with scope("fin1"):
        finish_pre(1, [0])
        wait_back(0, 1)
        for h in halves:
            finish_back(0, 1, h)
    with scope("first0"):
        finish_gs(0, 1)
        stats_second()
        start_gather(0, range(1, steps))
        pre_part(1, 1)
        prep(0, 1)
        loads[5].wait()
        loads[6].wait()
        back_part(0, 0)
        loads[7].wait()
        pre_part(0, 0)
        pre_part(0, 1)
        wait_pre(1, 1)
        finish_pre(1, range(1, steps))
    with scope("wpre0"):
        wait_pre(0, 0)
    with scope("fin0"):
        finish_pre(0, [0])
        wait_back(0, 0)
        for h in halves:
            finish_back(0, 0, h, send=False)
        finish_gs(0, 0)
        wait_pre(0, 1)
        finish_pre(0, range(1, steps))
        loads[8].wait()

    for t in range(1, last):
        for h in halves:
            step(t, 1, h)
        if t == 1:
            for h in halves:
                for c in pieces(steps, 0, h):
                    send_on(0, 0, h, c)
        finish_gs(t, 1)
    for h in halves[:-1]:
        step(last, 1, h)
    def end_products(v):
        ahead = 2 + v
        products(v, ORDER[:ahead])
        for j in ORDER[ahead:]:
            take(last, v, PARTS - 1, j)
        back(last, v, PARTS - 1)
        with scope(f"gout{v}"):
            finish_gs(last, v)
            for j in ORDER[ahead:]:
                product(("out", v, j))
            for j in rest("in", v):
                product(("in", v, j))

    end_products(1)

    def first_middles():
        middle(("out", 1, 2))

    for t in range(1, last):
        for h in halves:
            ending = t == last - 1
            step(t, 0, h, first_middles if ending and h == 0 else None)
            if ending and h == 0:
                with scope("wgat1"):
                    wait_gathered(1)
                with scope("gin1"):
                    grad_in(1, rest("out", 1))
                    middle(("out", 1, 3))
        finish_gs(t, 0)
    with scope("mid1"):
        middle(("out", 1, 0))
        middle(("out", 1, 1))
    for h in halves[:-1]:
        step(last, 0, h)
    end_products(0)
    with scope("midi1"):
        for j in rest("in", 1):
            middle(("in", 1, j))
    with scope("mid0_3"):
        middle(("out", 0, 3))
    with scope("wgat0"):
        wait_gathered(0)
    with scope("gin0"):
        grad_in(0, rest("out", 0))
    with scope("final1a"):
        for j in (2, 3, 0, 1):
            final(("out", 1, j))
        final_in(1)
    with scope("mid0_0"):
        middle(("out", 0, 0))
    with scope("mid0_2"):
        middle(("out", 0, 2))

    @pl.when(me_p < npipe - 1)
    def _():
        for item in stat_copies("h"):
            item.wait_recv()

    with scope("drain"):
        for item in stat_copies("l") + stat_copies("h"):
            item.wait_send()
        take_bytes(sqr, sq_s)
        take_bytes(pr, pre_s)
        take_bytes(br, back_s)

        @pl.when(me_p > 0)
        def _():
            take_bytes(ob, pipe_s)

        @pl.when(me_p == 0)
        def _():
            take_bytes(ob.at[:, 1], pipe_s)

        for v in range(vs):
            take_bytes(xr[v], xg_s.at[v])
            take_bytes(gsr[v].at[:, share_of(v)], gt_s.at[v])
            for item in pass_copies(v):
                item.wait_send()

    with scope("mid0_1"):
        middle(("out", 0, 1))
    with scope("midi0"):
        for j in rest("in", 0):
            middle(("in", 0, j))
    with scope("final0i"):
        final_in(0)
    with scope("final1b"):
        for j in rest("in", 1):
            final(("in", 1, j))
    for v in range(vs):
        take_bytes(in_bytes(v), ri_s.at[v])

    outs = vs * CHUNKS

    def drain_split(copies, landed, sem):
        if na == nb:
            rows = (slice(None),) * (len(landed.shape) - 2)
            take_bytes(landed.at[(pl.ds(0, outs),) + rows + (pl.ds(0, cc),)], sem.at[0])
            take_bytes(landed.at[(pl.ds(outs, len(jobs) - outs),) + rows + (pl.ds(0, cc + EXTRA),)], sem.at[1])
        else:
            for job in jobs:
                for item in copies(job):
                    item.wait_send()

    drain_split(split_copies, r1, r1_s)
    for j in (3, 0, 1, 2):
        with scope(f"fin0_{j}"):
            final(("out", 0, j))
    with scope("fini0"):
        for j in rest("in", 0):
            final(("in", 0, j))
    with scope("tail"):
        drain_split(join_copies, r2, r2_s)


def store(a, b, c, a_out, b_out, c_out, sem):
    pairs = ((a, a_out), (b, b_out), (c, c_out))
    for k, (src, dst) in enumerate(pairs):
        rows = src.shape[1] // 2
        for v in range(src.shape[0]):
            for r in range(2):
                where = (v, pl.ds(r * rows, rows))
                pltpu.make_async_copy(src.at[where], dst.at[where], sem.at[k]).start()
    for k, pair in enumerate(pairs):
        pltpu.make_async_copy(*pair, sem.at[k]).wait()


def shards(
    saved_inputs, proj_in, proj_out, norm_gain, arriving, logp_grad, rewards, seq_lengths, group_ids
):
    nt = lax.axis_size("tensor")
    npipe = lax.axis_size("pipe")
    ndp = lax.axis_size("dp")
    steps, vs, _, tok, wid = saved_inputs.shape
    rank = proj_in.shape[2]
    new_count = logp_grad.shape[0]
    group_count = new_count * ndp * rewards.shape[2] // 8
    lanes = -(-(group_count + 1) // 128) * 128
    na, nb = factors(ndp)
    rc = rank // ndp
    cc = wid // CHUNKS
    jobs = len(reductions())
    pipe_count = len(set(pipe_slots(steps, vs).values()))
    hm, lm = max(na - 1, 1), max(nb - 1, 1)
    dims = (steps, vs, tok, wid, rank, nt, npipe, ndp)
    peers = max(nt - 1, 1)
    any_spec = pl.BlockSpec(memory_space=pl.ANY)
    vmem = pl.BlockSpec(memory_space=pltpu.VMEM)
    V = pltpu.VMEM
    DMA = pltpu.SemaphoreType.DMA
    pmax = max(na, nb)
    less = max(pmax - 1, 1)
    scratch = [
        V((steps, vs, tok, wid), BF16),
        V((vs, steps * tok, wid), BF16),
        V((vs, steps, tok, wid), BF16),
        V((vs, rank, wid), BF16),
        V((vs, rank, wid), BF16),
        V((new_count, tok, wid), BF16),
        V((vs, steps * tok, rank), BF16),
        V((peers, vs, steps * tok, rank), BF16),
        V((vs, steps * tok, rank), F32),
        V((vs, steps * tok, rank), F32),
        V((vs, rank, steps * tok), BF16),
        V((vs, steps * tok, rank), BF16),
        V((vs, na, nb, rc, steps * tok), BF16),
        V((hm, nb, rc, steps * tok), BF16),
        V((lm, na, rc, steps * tok), BF16),
        V((hm, steps, tok, GATHERED[0] * cc - EXTRA), BF16),
        V((lm, steps, tok, GATHERED[1] * cc - EXTRA), BF16),
        V((vs, steps, tok, rank), BF16),
        V((peers, vs, steps, tok, rank), BF16),
        V((steps - 1, vs, tok, wid), BF16),
        V((vs, 2, tok, 128), F32),
        V((peers, vs, 2, tok, 128), F32),
        V((vs, 2, tok, 128), F32),
        V((2, 8, lanes), F32),
        V((lm, 8, lanes), F32),
        V((jobs, na, nb, rc, cc + max(EXTRA, 0)), BF16),
        V((jobs, less, pmax, rc, cc + max(EXTRA, 0)), BF16),
        V((jobs, pmax, rc, cc + max(EXTRA, 0)), BF16),
        V((jobs, less, rc, cc + max(EXTRA, 0)), BF16),
        V((vs, pmax, rc, wid - cc - EXTRA), BF16),
        V((vs, less, rc, wid - cc - EXTRA), BF16),
        V(norm_gain.shape, F32),
        pltpu.SMEM(rewards.shape, F32),
        pltpu.SMEM(seq_lengths.shape, jnp.int32),
        pltpu.SMEM(group_ids.shape, jnp.int32),
        V((hm, 8, lanes), F32),
        pltpu.SemaphoreType.REGULAR,
        DMA((13,)),
        DMA,
        DMA((2 * vs, peers)),
        DMA((4, less)),
        DMA,
        DMA((2 * vs, peers)),
        DMA,
        DMA((vs * (1 + (steps - 1) * PARTS), peers)),
        DMA,
        DMA((pipe_count,)),
        DMA((vs,)),
        DMA((vs,)),
        DMA((vs,)),
        DMA((vs,)),
        DMA((vs, less, peers)),
        DMA((vs, less, peers)),
        DMA((2,)),
        DMA((jobs, less)),
        DMA((2,)),
        DMA((jobs, less)),
        DMA((vs,)),
        DMA((vs,)),
    ]
    grad_in, grad_out, leaving = pl.pallas_call(
        functools.partial(kernel, dims),
        out_shape=(
            V((vs, rc, wid), F32),
            V((vs, rc, wid), F32),
            V((vs, tok, wid), BF16),
        ),
        in_specs=[any_spec] * 9,
        out_specs=(vmem, vmem, vmem),
        scratch_shapes=scratch,
        compiler_params=pltpu.CompilerParams(
            collective_id=0, has_side_effects=True, vmem_limit_bytes=58 * 1024 * 1024
        ),
    )(
        saved_inputs[:, :, 0], proj_in[:, 0], proj_out[:, 0], norm_gain, arriving[:, 0], logp_grad,
        rewards, seq_lengths, group_ids,
    )
    grad_in, grad_out, leaving = pl.pallas_call(
        store,
        out_shape=tuple(jax.ShapeDtypeStruct(a.shape, a.dtype) for a in (grad_in, grad_out, leaving)),
        in_specs=[vmem] * 3,
        out_specs=[any_spec] * 3,
        scratch_shapes=[DMA((3,))],
        compiler_params=pltpu.CompilerParams(vmem_limit_bytes=1024 * 1024),
    )(grad_in, grad_out, leaving)
    return grad_in[:, None], grad_out[:, None], leaving[:, None]


def solution(mesh):
    return jax.shard_map(
        shards,
        mesh=mesh,
        in_specs=(
            P(None, None, "pipe", "dp", "tensor"),
            P(None, "pipe", None, "tensor"),
            P(None, "pipe", None, "tensor"),
            P(None, "pipe", "tensor"),
            P(None, "pipe", "dp", "tensor"),
            P(None, "dp", "tensor"),
            P(None, "dp", None),
            P(None, "dp", None),
            P(None, "dp", None),
        ),
        out_specs=(
            P(None, "pipe", "dp", "tensor"),
            P(None, "pipe", "dp", "tensor"),
            P(None, "pipe", "dp", "tensor"),
        ),
        check_vma=False,
    )
```
